128 devices in a mesh: dap: 64 (over y, z_lo, x, core), dp: 2 (over z_hi).
Axes of the slice: x: 4, y: 4, z: 4 (z_hi: 2, z_lo: 2; z = z_hi * 2 + z_lo), core: 2. Of those that a mesh axis runs over, the one named last changes fastest.
Arguments:
- edge_embedding: bfloat16 [768, 384, 128], P(('dp', 'dap')), parts along dimension 0, may hold values from -6 to 6
- alignment_embedding: bfloat16 [128, 384, 256], P('dp', 'dap'), parts along dimension 0, may hold values from -6 to 6
- tensor_flank_matrix: bfloat16 [256, 64], replicated, may hold values from -0.375 to 0.375
- tensor_final_matrix: bfloat16 [1024, 128], replicated, may hold values from -0.75 to 0.75
- outward_sigmoid_matrix: bfloat16 [128, 640], replicated, may hold values from -0.5 to 0.5
- outward_final_matrix: bfloat16 [128, 128], replicated, may hold values from -0.5 to 0.5
- inward_sigmoid_matrix: bfloat16 [128, 640], replicated, may hold values from -0.5 to 0.5
- inward_final_matrix: bfloat16 [128, 128], replicated, may hold values from -0.5 to 0.5
- adjoint_seed: bfloat16 [768, 384, 128], P(('dp', 'dap')), parts along dimension 0, may hold values from -16 to 16
Outputs:
- edge_embedding_updated: bfloat16 [768, 384, 128], P(('dp', 'dap')), parts along dimension 0
- edge_embedding_adjoint: bfloat16 [768, 384, 128], P(('dp', 'dap')), parts along dimension 0
- alignment_adjoint: bfloat16 [128, 384, 256], P('dp', 'dap'), parts along dimension 0
- outer_proj_grad: float32 [512, 64], P('dp'), parts along dimension 0
- outer_final_grad: float32 [2048, 128], P('dp'), parts along dimension 0
- outgoing_proj_grad: float32 [256, 640], P('dp'), parts along dimension 0
- outgoing_final_grad: float32 [256, 128], P('dp'), parts along dimension 0
- incoming_proj_grad: float32 [256, 640], P('dp'), parts along dimension 0
- incoming_final_grad: float32 [256, 128], P('dp'), parts along dimension 0
The draws below stay inside these ranges and needn't reach their ends.
There are 2 independent parts, one for each index of `dp`. The reference program is written for one: setup_inputs(seed, part) draws one part's arguments, and reference() takes and returns one part's arrays. A program takes and returns all parts, laid end to end along the dimension named above; an argument that names none is the same for every part. Nothing has to cross between parts.
All inputs are finite; a program needn't handle non-finite values.
Results may differ from the reference program's by a relative error of at most 0.02.
Values may be sent and summed in bfloat16 or wider, within the bound.
A program may use at most 128 MiB of HBM per device.

```python
import jax
import jax.numpy as jnp
from jax import lax

ALIGN_FEATURES = 256
EDGE_FEATURES = 128
CH = 128
HIDDEN_WIDTH = 32
ALIGN_ROWS = 64
AMINO_TOTAL = 384


def strengthened(array, rng, source, target, blocks, factor):
    def block_of(axis_at):
        return (jnp.arange(array.shape[axis_at]) // (array.shape[axis_at] // blocks)).reshape((-1,) + (1,) * (array.ndim - 1 - axis_at))

    one_side = jax.random.permutation(rng, blocks)[block_of(target)]
    second = (block_of(target) + blocks // 2) % blocks
    return jnp.where((block_of(source) == one_side) | (block_of(source) == second), factor * array, array)


def block_levels(rng, dims, cuts, low, largest):
    def one(dim, parts):
        draws = jax.random.uniform(jax.random.fold_in(jax.random.fold_in(rng, 6), dim), (parts,), jnp.float32, low / len(cuts), largest / len(cuts))
        return jnp.repeat(jnp.exp(draws), dims[dim] // parts).reshape((-1,) + (1,) * (len(dims) - dim - 1))

    loudness = one(*cuts[0])
    for cut in cuts[1:]:
        loudness = loudness * one(*cut)
    return loudness


def scatter_about(stream_key, dims, spread, bound, shards=(), dtype=jnp.bfloat16):
    factor_of = block_levels(stream_key, dims, shards, -0.22, 0.18) if shards else 1.0
    drawn = jax.random.normal(stream_key, dims, jnp.float32) * spread * factor_of
    return jnp.minimum(jnp.maximum(drawn, -bound), bound).astype(dtype)


def gaussian_with(key, dims, width, bound, split, heavy, dtype=jnp.bfloat16):
    entries = width * jax.random.normal(key, dims, jnp.float32)
    if split:
        entries = entries * block_levels(key, dims, split, -0.22, 0.18)
    return jnp.clip(strengthened(entries, jax.random.fold_in(key, 3), *heavy), -bound, bound).astype(dtype)


def setup_inputs(seed: int = 0, part: int = 0) -> dict:
    seeds = jax.random.split(jax.random.key(seed), 10)
    part_splits = jax.random.split(jax.random.fold_in(seeds[9], part), 10)
    edge_embedding = scatter_about(part_splits[0], (AMINO_TOTAL, AMINO_TOTAL, EDGE_FEATURES), 1.0, 6.0, ((0, 64),))
    alignment_embedding = scatter_about(part_splits[1], (ALIGN_ROWS, AMINO_TOTAL, ALIGN_FEATURES), 1.0, 6.0, ((1, 64),))
    tensor_flank_matrix = scatter_about(seeds[2], (ALIGN_FEATURES, 2 * HIDDEN_WIDTH), ALIGN_FEATURES ** -0.5, 0.375)
    tensor_final_matrix = scatter_about(seeds[3], (HIDDEN_WIDTH * HIDDEN_WIDTH, EDGE_FEATURES), (HIDDEN_WIDTH * HIDDEN_WIDTH // 16) ** -0.5, 0.75)
    outward_sigmoid_matrix = scatter_about(seeds[4], (EDGE_FEATURES, 4 * CH + EDGE_FEATURES), EDGE_FEATURES ** -0.5, 0.5)
    outward_final_matrix = scatter_about(seeds[5], (CH, EDGE_FEATURES), CH ** -0.5, 0.5)
    inward_sigmoid_matrix = scatter_about(seeds[6], (EDGE_FEATURES, 4 * CH + EDGE_FEATURES), EDGE_FEATURES ** -0.5, 0.5)
    inward_final_matrix = scatter_about(seeds[7], (CH, EDGE_FEATURES), CH ** -0.5, 0.5)
    adjoint_seed = gaussian_with(part_splits[8], (AMINO_TOTAL, AMINO_TOTAL, EDGE_FEATURES), 1.0, 16.0, ((0, 64),), (0, 1, 64, 4.0))
    return dict(edge_embedding=edge_embedding, alignment_embedding=alignment_embedding, tensor_flank_matrix=tensor_flank_matrix, tensor_final_matrix=tensor_final_matrix, outward_sigmoid_matrix=outward_sigmoid_matrix, outward_final_matrix=outward_final_matrix, inward_sigmoid_matrix=inward_sigmoid_matrix, inward_final_matrix=inward_final_matrix, adjoint_seed=adjoint_seed)


EPSILON = 1e-05

def truncated_numbers(values):
    return lax.optimization_barrier(values.astype(jnp.bfloat16))

def edge_standardized(values, which_axis):
    average = lax.optimization_barrier(jnp.mean(values, axis=which_axis, keepdims=True))
    centred = values - average
    factor = lax.rsqrt(lax.optimization_barrier(jnp.mean(centred * centred, axis=which_axis, keepdims=True)) + EPSILON)
    return centred * factor

def standardizer_adjoint(values, gradient, which_axis):
    average = lax.optimization_barrier(jnp.mean(values, axis=which_axis, keepdims=True))
    centred = values - average
    factor = lax.rsqrt(lax.optimization_barrier(jnp.mean(centred * centred, axis=which_axis, keepdims=True)) + EPSILON)
    hatted = centred * factor
    return factor * (gradient - lax.optimization_barrier(jnp.mean(gradient, axis=which_axis, keepdims=True)) - hatted * lax.optimization_barrier(jnp.mean(gradient * hatted, axis=which_axis, keepdims=True)))

def sigmoid_pieces(edge_entry, linear_mapping, latent_tensor):
    standardized_edges = truncated_numbers(edge_standardized(edge_entry.astype(jnp.float32), -1))
    alignment_mapped = jnp.dot(standardized_edges, linear_mapping, preferred_element_type=jnp.float32)
    source_masked = truncated_numbers(jax.nn.sigmoid(alignment_mapped[..., :latent_tensor]) * alignment_mapped[..., latent_tensor:2 * latent_tensor])
    target_masked = truncated_numbers(jax.nn.sigmoid(alignment_mapped[..., 2 * latent_tensor:3 * latent_tensor]) * alignment_mapped[..., 3 * latent_tensor:4 * latent_tensor])
    sigmoid_factor = jax.nn.sigmoid(alignment_mapped[..., 4 * latent_tensor:])
    return (standardized_edges, alignment_mapped, source_masked, target_masked, sigmoid_factor)

def contract(source_masked, target_masked, outgoing):
    left_wide = source_masked.astype(jnp.float32)
    target_broad = target_masked.astype(jnp.float32)
    if outgoing:
        triangle_contraction = jnp.einsum('ikc,jkc->ijc', left_wide, target_broad)
    else:
        triangle_contraction = jnp.einsum('kic,kjc->ijc', left_wide, target_broad)
    return truncated_numbers(triangle_contraction)

def triangle_update(edge_entry, linear_mapping, final, outgoing):
    latent_tensor = final.shape[0]
    standardized_edges, alignment_mapped, source_masked, target_masked, sigmoid_factor = sigmoid_pieces(edge_entry, linear_mapping, latent_tensor)
    triangle = contract(source_masked, target_masked, outgoing)
    unit_norm = truncated_numbers(edge_standardized(triangle.astype(jnp.float32), -1))
    values = jnp.dot(unit_norm, final, preferred_element_type=jnp.float32)
    return truncated_numbers(edge_entry.astype(jnp.float32) + sigmoid_factor * values)

def triangle_back(edge_entry, linear_mapping, final, outgoing, gradient):
    latent_tensor = final.shape[0]
    standardized_edges, alignment_mapped, source_masked, target_masked, sigmoid_factor = sigmoid_pieces(edge_entry, linear_mapping, latent_tensor)
    triangle = contract(source_masked, target_masked, outgoing)
    tri_wide = triangle.astype(jnp.float32)
    unit_norm = truncated_numbers(edge_standardized(tri_wide, -1))
    values = jnp.dot(unit_norm, final, preferred_element_type=jnp.float32)
    scaled = truncated_numbers(gradient * sigmoid_factor)
    final_sum = jnp.einsum('ijc,ijz->cz', unit_norm.astype(jnp.float32), scaled.astype(jnp.float32))
    grad_unit = jnp.dot(scaled, final.T, preferred_element_type=jnp.float32)
    adjoint_sigmoid = gradient * values * sigmoid_factor * (1.0 - sigmoid_factor)
    grad_triangle = truncated_numbers(standardizer_adjoint(tri_wide, grad_unit, -1)).astype(jnp.float32)
    left_wide = source_masked.astype(jnp.float32)
    target_broad = target_masked.astype(jnp.float32)
    if outgoing:
        source_adjoint = jnp.einsum('ijc,jkc->ikc', grad_triangle, target_broad)
        target_adjoint = jnp.einsum('ijc,ikc->jkc', grad_triangle, left_wide)
    else:
        source_adjoint = jnp.einsum('ijc,kjc->kic', grad_triangle, target_broad)
        target_adjoint = jnp.einsum('ijc,kic->kjc', grad_triangle, left_wide)
    source_adjoint = truncated_numbers(source_adjoint).astype(jnp.float32)
    target_adjoint = truncated_numbers(target_adjoint).astype(jnp.float32)
    logistic_primary = jax.nn.sigmoid(alignment_mapped[..., :latent_tensor])
    logistic_tertiary = jax.nn.sigmoid(alignment_mapped[..., 2 * latent_tensor:3 * latent_tensor])
    adjoint_linear_input = truncated_numbers(jnp.concatenate([source_adjoint * alignment_mapped[..., latent_tensor:2 * latent_tensor] * logistic_primary * (1.0 - logistic_primary), source_adjoint * logistic_primary, target_adjoint * alignment_mapped[..., 3 * latent_tensor:4 * latent_tensor] * logistic_tertiary * (1.0 - logistic_tertiary), target_adjoint * logistic_tertiary, adjoint_sigmoid], axis=-1))
    proj_sum = jnp.einsum('ijz,ijc->zc', standardized_edges.astype(jnp.float32), adjoint_linear_input.astype(jnp.float32))
    grad_norm = jnp.dot(adjoint_linear_input, linear_mapping.T, preferred_element_type=jnp.float32)
    grad_pair = gradient + standardizer_adjoint(edge_entry.astype(jnp.float32), grad_norm, -1)
    return (grad_pair, proj_sum, final_sum)

def reference(edge_embedding, alignment_embedding, tensor_flank_matrix, tensor_final_matrix, outward_sigmoid_matrix, outward_final_matrix, inward_sigmoid_matrix, inward_final_matrix, adjoint_seed):
    alignment_standardized = truncated_numbers(edge_standardized(alignment_embedding.astype(jnp.float32), -1))
    alignment_mapped = jnp.dot(alignment_standardized, tensor_flank_matrix, preferred_element_type=jnp.float32)
    tensor_source_factor = truncated_numbers(alignment_mapped[..., :HIDDEN_WIDTH])
    tensor_target_factor = truncated_numbers(alignment_mapped[..., HIDDEN_WIDTH:])
    tile_lines = 64 if AMINO_TOTAL % 64 == 0 else AMINO_TOTAL
    tile_number = AMINO_TOTAL // tile_lines
    source_tiles = jnp.transpose(tensor_source_factor.reshape(ALIGN_ROWS, tile_number, tile_lines, HIDDEN_WIDTH), (1, 0, 2, 3))
    pair_blocks = edge_embedding.reshape(tile_number, tile_lines, AMINO_TOTAL, EDGE_FEATURES)
    target_broad = tensor_target_factor.astype(jnp.float32)

    def outer_rows(source_lines):
        triangle_contraction = jnp.einsum('sic,sjd->ijcd', source_lines.astype(jnp.float32), target_broad)
        return truncated_numbers(triangle_contraction.reshape(tile_lines, AMINO_TOTAL, HIDDEN_WIDTH * HIDDEN_WIDTH) / ALIGN_ROWS)

    def forward_block(pieces):
        source_lines, pair_rows = pieces
        update = jnp.dot(outer_rows(source_lines), tensor_final_matrix, preferred_element_type=jnp.float32)
        return truncated_numbers(pair_rows.astype(jnp.float32) + update)
    pair_one = lax.map(forward_block, (source_tiles, pair_blocks)).reshape(AMINO_TOTAL, AMINO_TOTAL, EDGE_FEATURES)
    pair_two = triangle_update(pair_one, outward_sigmoid_matrix, outward_final_matrix, True)
    edge_embedding_updated = triangle_update(pair_two, inward_sigmoid_matrix, inward_final_matrix, False)
    grad_two, inward_sigmoid_accrual, inward_final_accrual = triangle_back(pair_two, inward_sigmoid_matrix, inward_final_matrix, False, adjoint_seed.astype(jnp.float32))
    grad_one, outward_sigmoid_accrual, outward_final_accrual = triangle_back(pair_one, outward_sigmoid_matrix, outward_final_matrix, True, grad_two)
    edge_embedding_adjoint = truncated_numbers(grad_one)
    grad_blocks = edge_embedding_adjoint.reshape(tile_number, tile_lines, AMINO_TOTAL, EDGE_FEATURES)

    def backward_block(running, pieces):
        final_sum, target_accrual = running
        source_lines, grad_rows = pieces
        outer_block = outer_rows(source_lines)
        final_sum = final_sum + jnp.einsum('ijk,ijz->kz', outer_block.astype(jnp.float32), grad_rows.astype(jnp.float32))
        adjoint_tensor_mean = truncated_numbers(jnp.dot(grad_rows, tensor_final_matrix.T, preferred_element_type=jnp.float32))
        adjoint_tensor_mean = adjoint_tensor_mean.astype(jnp.float32).reshape(tile_lines, AMINO_TOTAL, HIDDEN_WIDTH, HIDDEN_WIDTH)
        source_piece = jnp.einsum('mopz,loz->lmp', adjoint_tensor_mean, target_broad) / ALIGN_ROWS
        target_accrual = target_accrual + jnp.einsum('gxqp,vgq->vxp', adjoint_tensor_mean, source_lines.astype(jnp.float32)) / ALIGN_ROWS
        return ((final_sum, target_accrual), source_piece)
    starting_tensor = (jnp.zeros((HIDDEN_WIDTH * HIDDEN_WIDTH, EDGE_FEATURES), jnp.float32), jnp.zeros((ALIGN_ROWS, AMINO_TOTAL, HIDDEN_WIDTH), jnp.float32))
    (tensor_final_accrual, target_adjoint), source_pieces = lax.scan(backward_block, starting_tensor, (source_tiles, grad_blocks))
    source_adjoint = jnp.transpose(source_pieces, (1, 0, 2, 3)).reshape(ALIGN_ROWS, AMINO_TOTAL, HIDDEN_WIDTH)
    alignment_mapped_adjoint = truncated_numbers(jnp.concatenate([source_adjoint, target_adjoint], axis=-1))
    tensor_flank_accrual = jnp.einsum('ctm,ctg->mg', alignment_standardized.astype(jnp.float32), alignment_mapped_adjoint.astype(jnp.float32))
    alignment_standard_adjoint = jnp.dot(alignment_mapped_adjoint, tensor_flank_matrix.T, preferred_element_type=jnp.float32)
    alignment_adjoint = truncated_numbers(standardizer_adjoint(alignment_embedding.astype(jnp.float32), alignment_standard_adjoint, -1))
    return (edge_embedding_updated, edge_embedding_adjoint, alignment_adjoint, tensor_flank_accrual / AMINO_TOTAL, tensor_final_accrual / AMINO_TOTAL, outward_sigmoid_accrual / AMINO_TOTAL, outward_final_accrual / AMINO_TOTAL, inward_sigmoid_accrual / AMINO_TOTAL, inward_final_accrual / AMINO_TOTAL)
```

```python
import functools

import jax
import jax.numpy as jnp
from jax import lax
from jax.experimental import pallas as pl
from jax.experimental.pallas import tpu as pltpu
from jax.sharding import PartitionSpec as P

EPSILON = 1e-05
F32, BF16 = jnp.float32, jnp.bfloat16
MESH = pl.DeviceIdType.MESH
N = 64
ROWS = 6
RES = 384
CELLS = ROWS * RES
CH = 128
GROUPS = CELLS // 128
TILE = 256
TILES = CELLS // TILE
VMEM_LIMIT = 60 * 1024 * 1024


def nn(a, b):
    return lax.dot_general(a, b, (((1,), (0,)), ((), ())), preferred_element_type=F32)


def nt(a, b):
    return lax.dot_general(a, b, (((1,), (1,)), ((), ())), preferred_element_type=F32)


def one_hot(rows, columns, pick, dtype=BF16):
    row = lax.broadcasted_iota(jnp.int32, (rows, columns), 0)
    column = lax.broadcasted_iota(jnp.int32, (rows, columns), 1)
    return jnp.where(pick(row) == column, 1.0, 0.0).astype(dtype)


def identity(size):
    return one_hot(size, size, lambda r: r)


def hidden_order(dtype=BF16):
    return one_hot(CH, CH, lambda r: jnp.where(r < N, 2 * r, 2 * r - (CH - 1)), dtype)


def sigmoid(v):
    return 1.0 / (1.0 + jnp.exp(-v))


def ln0(v):
    centred = v - jnp.mean(v, axis=0, keepdims=True)
    factor = lax.rsqrt(jnp.mean(centred * centred, axis=0, keepdims=True) + EPSILON)
    return centred * factor, factor


def ln0_adjoint(hatted, factor, g):
    return factor * (
        g
        - jnp.mean(g, axis=0, keepdims=True)
        - hatted * jnp.mean(g * hatted, axis=0, keepdims=True)
    )


def loop(count, body, start=0):
    def step(k, carry):
        body(k)
        return carry

    lax.fori_loop(start, count, step, 0)


def me_index():
    return lax.axis_index("dap")


def greet():
    me = me_index()
    sem = pltpu.get_barrier_semaphore()
    loop(
        N,
        lambda k: pl.semaphore_signal(
            sem, inc=1, device_id={"dap": lax.rem(me + k, N)}, device_id_type=MESH
        ),
        1,
    )


def all_here():
    pl.semaphore_wait(pltpu.get_barrier_semaphore(), N - 1)


def remote(src, dst, send_sem, recv_sem, to):
    return pltpu.make_async_remote_copy(
        src_ref=src,
        dst_ref=dst,
        send_sem=send_sem,
        recv_sem=recv_sem,
        device_id={"dap": to},
        device_id_type=MESH,
    )


class Exchange:
    def __init__(self, out, into, sent, got):
        self.out, self.into, self.sent, self.got = out, into, sent, got

    def send(self, d):
        me = me_index()
        remote(self.out.at[d], self.into.at[me], self.sent.at[d], self.got.at[me], d).start()

    def pack_and_send(self, rows_of):
        me = me_index()
        self.into[me] = rows_of(me)

        def first(d):
            self.out[d] = rows_of(d)

        first(lax.rem(me + 1, N))

        def step(k):
            first(lax.rem(me + k + 1, N))
            self.send(lax.rem(me + k, N))

        loop(N - 1, step, 1)
        self.send(lax.rem(me + N - 1, N))

    def receive(self, use):
        me = me_index()
        use(me)

        def step(k):
            s = lax.rem(me + N - k, N)
            remote(
                self.out.at[s], self.into.at[s], self.sent.at[s], self.got.at[s], s
            ).wait_recv()
            use(s)

        loop(N, step, 1)

    def close(self):
        me = me_index()

        def step(k):
            d = lax.rem(me + k, N)
            remote(
                self.out.at[d], self.into.at[d], self.sent.at[d], self.got.at[d], d
            ).wait_send()

        loop(N, step, 1)


def strided(ref, start, size, stride):
    return ref[pl.ds(start, size, stride=stride), :]


def widen_into(wide, into, rows, pitch):
    def use(s):
        wide[pl.ds(pl.multiple_of(s * pitch, 8), rows), :] = into[s].astype(F32)

    return use


def proj_weights(p_ref, pt):
    order = hidden_order()
    for b in range(4):
        pt[b * CH : (b + 1) * CH, :] = nt(order, p_ref[:, b * CH : (b + 1) * CH]).astype(BF16)
    pt[4 * CH :, :] = nt(identity(CH), p_ref[:, 4 * CH :]).astype(BF16)


def lanes_of(t):
    return pl.ds(pl.multiple_of(t * TILE, TILE), TILE)


def scatter_hidden(flat, value, piece, t):
    for m in range(2):
        for q in range(TILE // 128):
            g = t * (TILE // 128) + q
            at = pl.multiple_of(((piece * 2 + m) * GROUPS + g) * N, N)
            flat[pl.ds(at, N), :] = value[m * N : (m + 1) * N, q * 128 : (q + 1) * 128]


def gather_hidden(wide, pitch, base, t):
    parts = []
    for m in range(2):
        row = []
        for q in range(TILE // 128):
            g = t * (TILE // 128) + q
            row.append(strided(wide, base + m * GROUPS + g, N, pitch))
        parts.append(jnp.concatenate(row, axis=1))
    return jnp.concatenate(parts, axis=0)


def scatter_rows(flat, value, piece):
    for r in range(ROWS):
        for jg in range(3):
            at = ((piece * ROWS + r) * 3 + jg) * N
            flat[at : at + N, :] = value[r * N : (r + 1) * N, jg * 128 : (jg + 1) * 128]


def gather_matrix(out, wide, pitch, base):
    for r in range(ROWS):
        for jg in range(3):
            out[r * N : (r + 1) * N, jg * 128 : (jg + 1) * 128] = strided(
                wide, base + r * 3 + jg, N, pitch
            ).astype(BF16)


def update_kernel(
    outgoing, x_ref, p_ref, f_ref,
    new_ref, tri_ref, kept_ref,
    pt, ft, nrm, gate, flat, wide, out1, in1, out2, in2, sent1, got1, sent2, got2,
):
    greet()
    proj_weights(p_ref, pt)
    turned = nn(hidden_order(), f_ref[...]).astype(BF16)
    ft[...] = nt(identity(CH), turned).astype(BF16)

    def rows_in(t):
        at = lanes_of(t)
        hatted, _ = ln0(x_ref[:, at].astype(F32))
        norm = hatted.astype(BF16)
        nrm[:, at] = norm
        pre = nn(pt[: 4 * CH, :], norm)
        scatter_hidden(flat, sigmoid(pre[:CH]) * pre[CH : 2 * CH], 0, t)
        scatter_hidden(flat, sigmoid(pre[2 * CH : 3 * CH]) * pre[3 * CH :], 1, t)

    loop(TILES, rows_in)
    all_here()
    one = Exchange(out1, in1, sent1, got1)
    one.pack_and_send(lambda d: strided(flat, d, 72, N).astype(BF16))

    def gates(t):
        at = lanes_of(t)
        gate[:, at] = sigmoid(nn(pt[4 * CH :, :], nrm[:, at]))

    loop(TILES, gates)
    one.receive(widen_into(wide, in1, 72, 72))
    for piece in range(4):
        gather_matrix(kept_ref.at[piece], wide, 72, piece * GROUPS)
    for m in range(2):
        left, right = kept_ref[m], kept_ref[2 + m]
        if outgoing:
            product = nt(left, right)
        else:
            product = nn(left.T, right)
        scatter_rows(flat, product, m)
    two = Exchange(out2, in2, sent2, got2)
    two.pack_and_send(lambda d: strided(flat, d, 36, N).astype(BF16))
    one.close()
    two.receive(widen_into(wide, in2, 36, 40))

    def rows_out(t):
        at = lanes_of(t)
        tri = gather_hidden(wide, 40, 0, t)
        tri_ref[:, at] = tri.astype(BF16)
        unit, _ = ln0(tri)
        values = nn(ft[...], unit.astype(BF16))
        new_ref[:, at] = (x_ref[:, at].astype(F32) + gate[:, at] * values).astype(BF16)

    loop(TILES, rows_out)
    two.close()


def vmem(count):
    return [pl.BlockSpec(memory_space=pltpu.VMEM)] * count


def shaped(shape, dtype):
    return jax.ShapeDtypeStruct(shape, dtype)


def params(collective_id):
    return pltpu.CompilerParams(
        collective_id=collective_id, has_side_effects=True, vmem_limit_bytes=VMEM_LIMIT
    )


def sems(count):
    return [pltpu.SemaphoreType.DMA((N,))] * count


def triangle_update(x, proj, final, outgoing, collective_id):
    return pl.pallas_call(
        functools.partial(update_kernel, outgoing),
        out_shape=(
            shaped((CH, CELLS), BF16),
            shaped((CH, CELLS), BF16),
            shaped((4, RES, RES), BF16),
        ),
        in_specs=vmem(3),
        out_specs=tuple(vmem(3)),
        scratch_shapes=[
            pltpu.VMEM((5 * CH, CH), BF16),
            pltpu.VMEM((CH, CH), BF16),
            pltpu.VMEM((CH, CELLS), BF16),
            pltpu.VMEM((CH, CELLS), F32),
            pltpu.VMEM((72 * N, 128), F32),
            pltpu.VMEM((72 * N, 128), F32),
            pltpu.VMEM((N, 72, 128), BF16),
            pltpu.VMEM((N, 72, 128), BF16),
            pltpu.VMEM((N, 36, 128), BF16),
            pltpu.VMEM((N, 36, 128), BF16),
            *sems(4),
        ],
        compiler_params=params(collective_id),
        name="update_out" if outgoing else "update_in",
    )(x, proj, final)


def back_kernel(
    outgoing, x_ref, p_ref, f_ref, tri_ref, kept_ref, gz_ref,
    gnew_ref, psum_ref,
    pt, pp, fh, ft, nrm, unit_s, scaled_s, coef, gp, flat, wide, grad_m,
    out1, in1, out2, in2, sent1, got1, sent2, got2,
):
    greet()
    proj_weights(p_ref, pt)
    order = hidden_order()
    for b in range(4):
        pp[:, b * CH : (b + 1) * CH] = nt(p_ref[:, b * CH : (b + 1) * CH], order).astype(BF16)
    pp[:, 4 * CH :] = p_ref[:, 4 * CH :]
    fh[...] = nn(order, f_ref[...]).astype(BF16)
    ft[...] = nt(identity(CH), fh[...]).astype(BF16)

    def rows_in(t):
        at = lanes_of(t)
        hatted, _ = ln0(x_ref[:, at].astype(F32))
        norm = hatted.astype(BF16)
        nrm[:, at] = norm
        gate = sigmoid(nn(pt[4 * CH :, :], norm))
        tri_hat, tri_factor = ln0(tri_ref[:, at].astype(F32))
        unit = tri_hat.astype(BF16)
        values = nn(ft[...], unit)
        gz = gz_ref[:, at].astype(F32)
        scaled_wide = gz * gate
        scaled = scaled_wide.astype(BF16)
        unit_s[:, at] = unit
        scaled_s[:, at] = scaled
        gp[4 * CH :, at] = (scaled_wide * values * (1.0 - gate)).astype(BF16)
        grad_unit = nn(fh[...], scaled)
        scatter_hidden(flat, ln0_adjoint(tri_hat, tri_factor, grad_unit), 0, t)

    loop(TILES, rows_in)
    all_here()
    one = Exchange(out1, in1, sent1, got1)
    one.pack_and_send(lambda d: strided(flat, d, 36, N).astype(BF16))

    def coefficients(t):
        at = lanes_of(t)
        pre = nn(pt[: 4 * CH, :], nrm[:, at])
        for side in range(2):
            base = 2 * side * CH
            opened = sigmoid(pre[base : base + CH])
            coef[base : base + CH, at] = pre[base + CH : base + 2 * CH] * opened * (1.0 - opened)
            coef[base + CH : base + 2 * CH, at] = opened

    loop(TILES, coefficients)
    exact = dict(preferred_element_type=F32, precision=lax.Precision.HIGHEST)
    order_wide = hidden_order(F32)
    final_sum = nt(unit_s[...], scaled_s[...])
    psum_ref[5 * CH :, :] = lax.dot_general(
        order_wide, final_sum, (((0,), (0,)), ((), ())), **exact
    ) * (1.0 / RES)

    one.receive(widen_into(wide, in1, 36, 40))
    for m in range(2):
        gather_matrix(grad_m, wide, 40, m * GROUPS)
        grad = grad_m[...]
        left, right = kept_ref[m], kept_ref[2 + m]
        if outgoing:
            grad_left = nn(grad, right)
            grad_right = nn(grad.T, left)
        else:
            grad_left = nt(right, grad)
            grad_right = nn(left, grad)
        scatter_rows(flat, grad_left, m)
        scatter_rows(flat, grad_right, 2 + m)
    two = Exchange(out2, in2, sent2, got2)
    two.pack_and_send(lambda d: strided(flat, d, 72, N).astype(BF16))
    psum_ref[4 * CH : 5 * CH, :] = nt(nrm[...], gp[4 * CH :, :]) * (1.0 / RES)
    one.close()
    two.receive(widen_into(wide, in2, 72, 72))

    def rows_out(t):
        at = lanes_of(t)
        for side in range(2):
            base = 2 * side * CH
            grad = gather_hidden(wide, 72, 2 * side * GROUPS, t).astype(BF16).astype(F32)
            for half in range(2):
                rows = pl.ds(base + half * CH, CH)
                gp[rows, at] = (grad * coef[rows, at]).astype(BF16)
        grad_norm = nn(pp[...], gp[:, at])
        hatted, factor = ln0(x_ref[:, at].astype(F32))
        gnew_ref[:, at] = (
            gz_ref[:, at].astype(F32) + ln0_adjoint(hatted, factor, grad_norm)
        ).astype(gnew_ref.dtype)

    loop(TILES, rows_out)
    for b in range(4):
        here = nt(nrm[...], gp[b * CH : (b + 1) * CH, :])
        psum_ref[b * CH : (b + 1) * CH, :] = lax.dot_general(
            here, order_wide, (((1,), (0,)), ((), ())), **exact
        ) * (1.0 / RES)
    two.close()


def triangle_back(x, proj, final, tri, kept, gz, outgoing, out_dtype, collective_id):
    return pl.pallas_call(
        functools.partial(back_kernel, outgoing),
        out_shape=(shaped((CH, CELLS), out_dtype), shaped((6 * CH, CH), F32)),
        in_specs=vmem(6),
        out_specs=tuple(vmem(2)),
        scratch_shapes=[
            pltpu.VMEM((5 * CH, CH), BF16),
            pltpu.VMEM((CH, 5 * CH), BF16),
            pltpu.VMEM((CH, CH), BF16),
            pltpu.VMEM((CH, CH), BF16),
            pltpu.VMEM((CH, CELLS), BF16),
            pltpu.VMEM((CH, CELLS), BF16),
            pltpu.VMEM((CH, CELLS), BF16),
            pltpu.VMEM((4 * CH, CELLS), F32),
            pltpu.VMEM((5 * CH, CELLS), BF16),
            pltpu.VMEM((72 * N, 128), F32),
            pltpu.VMEM((72 * N, 128), F32),
            pltpu.VMEM((RES, RES), BF16),
            pltpu.VMEM((N, 36, 128), BF16),
            pltpu.VMEM((N, 36, 128), BF16),
            pltpu.VMEM((N, 72, 128), BF16),
            pltpu.VMEM((N, 72, 128), BF16),
            *sems(4),
        ],
        compiler_params=params(collective_id),
        name="back_out" if outgoing else "back_in",
    )(x, proj, final, tri, kept, gz)


HIDDEN = 32
PAIRS = HIDDEN // 2
SEQ = 64
FEATURES = 256


class Gather:
    def __init__(self, own, into, sent, got, passed):
        self.own, self.into, self.sent, self.got, self.passed = own, into, sent, got, passed

    def partner(self):
        me = me_index()
        return me + 1 - 2 * lax.rem(me, 2)

    def across(self, k):
        me = me_index()
        d = lax.rem(me + 2 * k, N)
        return remote(self.own, self.into.at[me], self.sent.at[k], self.got.at[me], d)

    def handed(self, s):
        return remote(
            self.into.at[s], self.into.at[s], self.passed.at[s], self.got.at[s], self.partner()
        )

    def home(self):
        me = me_index()
        return remote(
            self.own, self.into.at[me], self.passed.at[me], self.got.at[me], self.partner()
        )

    def start(self):
        self.into[me_index()] = self.own[...]
        loop(N // 2, lambda k: self.across(k).start(), 1)
        self.home().start()

    def hand_on(self):
        me = me_index()

        def step(k):
            s = lax.rem(me + N - 2 * k, N)
            self.handed(s).wait_recv()
            self.handed(s).start()

        loop(N // 2, step, 1)

    def finish(self):
        me, other = me_index(), self.partner()

        def step(k):
            self.handed(lax.rem(other + N - 2 * k, N)).wait_recv()

        loop(N // 2, step)

    def close(self):
        me = me_index()
        loop(N // 2, lambda k: self.across(k).wait_send(), 1)
        self.home().wait_send()
        loop(N // 2, lambda k: self.handed(lax.rem(me + N - 2 * k, N)).wait_send(), 1)


def ln1(v):
    centred = v - jnp.mean(v, axis=1, keepdims=True)
    factor = lax.rsqrt(jnp.mean(centred * centred, axis=1, keepdims=True) + EPSILON)
    return centred * factor, factor


def spread_out(all_ref, wide, into):
    loop(N, lambda s: widen_into(wide, into, 96, 96)(s))
    for r in range(ROWS):
        for p in range(PAIRS):
            all_ref[r * N : (r + 1) * N, p * 128 : (p + 1) * 128] = strided(
                wide, r * PAIRS + p, N, 96
            ).astype(BF16)


def pair_lanes(p):
    return pl.ds(pl.multiple_of(p * 128, 128), 128)


def start_kernel(
    al_ref, flank_ref, fin_ref, edge_ref,
    x_ref, right_ref, left_ref, own_ref,
    fin_turned, wide, cells_wide, outer, fin_wide,
    out_r, in_r, out_l, in_l, sent_r, got_r, pass_r, sent_l, got_l, pass_l,
):
    greet()
    flank = flank_ref[...]
    split = lambda first: one_hot(
        HIDDEN, 2 * HIDDEN, lambda r: first + jnp.where(r < PAIRS, 2 * r, 2 * r - (HIDDEN - 1))
    )
    split_left = nt(split(0), flank).astype(BF16)
    split_right = nt(split(HIDDEN), flank).astype(BF16)
    plain_left = nt(one_hot(HIDDEN, 2 * HIDDEN, lambda r: r), flank).astype(BF16)
    none = jnp.zeros((SEQ, FEATURES), BF16)
    for r in range(ROWS):
        hatted, _ = ln1(al_ref[r].astype(F32))
        norm = hatted.astype(BF16)
        halves = (jnp.concatenate([norm, none], 0), jnp.concatenate([none, norm], 0))
        here = pl.ds(r * PAIRS, PAIRS)
        for out, weights in ((out_r, split_right), (out_l, split_left)):
            out[here, :] = (
                nt(weights[:PAIRS], halves[0]) + nt(weights[PAIRS:], halves[1])
            ).astype(BF16)
        for h in range(2):
            at = (2 * r + h) * HIDDEN
            own_ref[at : at + HIDDEN, :] = nt(plain_left, halves[h]).astype(BF16)
    all_here()
    right = Gather(out_r, in_r, sent_r, got_r, pass_r)
    left = Gather(out_l, in_l, sent_l, got_l, pass_l)
    right.start()
    left.start()
    for r in range(ROWS):
        rows = slice(r * RES, (r + 1) * RES)
        cells_wide[rows, :] = edge_ref[rows, :].astype(F32)
    for r in range(ROWS):
        parts = [strided(cells_wide, r * RES + q, N, ROWS) for q in range(ROWS)]
        x_ref[:, r * RES : (r + 1) * RES] = jnp.concatenate(parts, 0).T.astype(BF16)
    fin_wide[...] = fin_ref[...].astype(F32)
    for d in range(HIDDEN):
        rows = strided(fin_wide, d, HIDDEN, HIDDEN).astype(BF16)
        outer[0, d * HIDDEN : (d + 1) * HIDDEN, :CH] = rows
    fin_turned[...] = nt(identity(CH), outer[0, :, :CH]).astype(BF16)
    right.hand_on()
    right.finish()
    spread_out(right_ref, wide, in_r)

    def outer_pair(p):
        block = nt(own_ref[...], right_ref[:, pair_lanes(p)]) * (1.0 / SEQ)
        for r in range(ROWS):
            outer[r, pl.ds(pl.multiple_of(p * 64, 64), 64), :] = block[
                r * 64 : (r + 1) * 64
            ].astype(BF16)

    loop(PAIRS, outer_pair)
    for r in range(ROWS):
        at = slice(r * RES, (r + 1) * RES)
        x_ref[:, at] = (x_ref[:, at].astype(F32) + nn(fin_turned[...], outer[r])).astype(BF16)
    left.hand_on()
    left.finish()
    spread_out(left_ref, wide, in_l)
    right.close()
    left.close()


def start(alignment, flank, fin, edge, collective_id):
    return pl.pallas_call(
        start_kernel,
        out_shape=(
            shaped((CH, CELLS), BF16),
            shaped((RES, HIDDEN * SEQ), BF16),
            shaped((RES, HIDDEN * SEQ), BF16),
            shaped((2 * ROWS * HIDDEN, 2 * SEQ), BF16),
        ),
        in_specs=vmem(4),
        out_specs=tuple(vmem(4)),
        scratch_shapes=[
            pltpu.VMEM((CH, HIDDEN * HIDDEN), BF16),
            pltpu.VMEM((96 * N, 128), F32),
            pltpu.VMEM((CELLS, 128), F32),
            pltpu.VMEM((ROWS, HIDDEN * HIDDEN, RES), BF16),
            pltpu.VMEM((HIDDEN * HIDDEN, CH), F32),
            pltpu.VMEM((96, 128), BF16),
            pltpu.VMEM((N, 96, 128), BF16),
            pltpu.VMEM((96, 128), BF16),
            pltpu.VMEM((N, 96, 128), BF16),
            *sems(6),
        ],
        compiler_params=params(collective_id),
        name="start",
    )(alignment, flank, fin, edge)


def outer_back(weights, cells_of, all_ref, grads, acc, rows_nt):
    for r in range(ROWS):
        block = (nt if rows_nt else nn)(weights[...], cells_of(r))
        for p in range(PAIRS):
            grads[p, r * 64 : (r + 1) * 64, :] = block[p * 64 : (p + 1) * 64].astype(BF16)
    acc[...] = jnp.zeros_like(acc)

    def add(p):
        acc[...] += nn(grads[p], all_ref[:, pair_lanes(p)])

    loop(PAIRS, add)


def matched(acc, r):
    return acc[r * 64 : r * 64 + 32, :] + pltpu.roll(acc[r * 64 + 32 : (r + 1) * 64, :], 64, 1)


def end_kernel(
    adj_ref, right_ref, left_ref, own_ref, fin_ref, al_ref, flank_ref,
    pair_ref, align_ref, flank_sum_ref, fin_sum_ref,
    cells_wide, natural, fin_wide, fin_split, outer, grads, acc_l, acc_r, wide, columns,
    out1, in1, sent1, got1,
):
    greet()
    for r in range(ROWS):
        at = slice(r * RES, (r + 1) * RES)
        cells_wide[at, :] = adj_ref[:, at].astype(F32).T
    all_here()
    one = Exchange(out1, in1, sent1, got1)
    one.pack_and_send(lambda d: strided(cells_wide, d, 36, N).astype(BF16))
    fin_wide[...] = fin_ref[...].astype(F32)
    for d in range(HIDDEN):
        fin_split[d * HIDDEN : (d + 1) * HIDDEN, :] = strided(fin_wide, d, HIDDEN, HIDDEN).astype(
            BF16
        )

    def outer_pair(p):
        block = nt(own_ref[...], right_ref[:, pair_lanes(p)]) * (1.0 / SEQ)
        for r in range(ROWS):
            outer[r, pl.ds(pl.multiple_of(p * 64, 64), 64), :] = block[
                r * 64 : (r + 1) * 64
            ].astype(BF16)

    loop(PAIRS, outer_pair)
    total = None
    for r in range(ROWS):
        part = nt(outer[r], adj_ref[:, r * RES : (r + 1) * RES])
        total = part if total is None else total + part
    fin_wide[...] = total * (1.0 / RES)
    for c in range(HIDDEN):
        fin_sum_ref[c * HIDDEN : (c + 1) * HIDDEN, :] = strided(fin_wide, c, HIDDEN, HIDDEN)
    outer_back(
        fin_split, lambda r: adj_ref[:, r * RES : (r + 1) * RES], right_ref, grads, acc_l, False
    )
    for r in range(ROWS):
        for q in range(ROWS):
            natural[pl.ds(r * RES + q, N, stride=ROWS), :] = cells_wide[
                (r * ROWS + q) * N : (r * ROWS + q + 1) * N, :
            ]
    for r in range(ROWS):
        rows = slice(r * RES, (r + 1) * RES)
        pair_ref[rows, :] = natural[rows, :].astype(BF16)
    one.receive(widen_into(wide, in1, 36, 40))
    for q in range(ROWS):
        for r in range(ROWS):
            columns[q, r * N : (r + 1) * N, :] = strided(wide, r * ROWS + q, N, 40).astype(BF16)
    outer_back(fin_ref, lambda q: columns[q], left_ref, grads, acc_r, True)
    flank = flank_ref[...]
    flank_turned = nt(identity(2 * HIDDEN), flank).astype(BF16)
    lane = lax.broadcasted_iota(jnp.int32, (2 * HIDDEN, 2 * SEQ), 1)
    none = jnp.zeros((SEQ, FEATURES), BF16)
    flank_sum = jnp.zeros((2 * HIDDEN, FEATURES), F32)
    for r in range(ROWS):
        both = jnp.concatenate([matched(acc_l, r), matched(acc_r, r)], 0) * (1.0 / SEQ)
        both = jnp.where(lane < SEQ, both, 0.0)
        hatted, factor = ln1(al_ref[r].astype(F32))
        norm = jnp.concatenate([hatted.astype(BF16), none], 0)
        flank_sum = flank_sum + nn(both.astype(BF16), norm)
        grad = nn(both.T[:SEQ].astype(BF16), flank_turned)
        align_ref[r] = (
            factor
            * (
                grad
                - jnp.mean(grad, axis=1, keepdims=True)
                - hatted * jnp.mean(grad * hatted, axis=1, keepdims=True)
            )
        ).astype(BF16)
    flank_sum_ref[...] = flank_sum * (1.0 / RES)
    one.close()


def end(adj, right_all, left_all, own, fin, alignment, flank, collective_id):
    return pl.pallas_call(
        end_kernel,
        out_shape=(
            shaped((CELLS, CH), BF16),
            shaped((ROWS, SEQ, FEATURES), BF16),
            shaped((2 * HIDDEN, FEATURES), F32),
            shaped((HIDDEN * HIDDEN, CH), F32),
        ),
        in_specs=vmem(7),
        out_specs=tuple(vmem(4)),
        scratch_shapes=[
            pltpu.VMEM((CELLS, 128), F32),
            pltpu.VMEM((CELLS, 128), F32),
            pltpu.VMEM((HIDDEN * HIDDEN, CH), F32),
            pltpu.VMEM((HIDDEN * HIDDEN, CH), BF16),
            pltpu.VMEM((ROWS, HIDDEN * HIDDEN, RES), BF16),
            pltpu.VMEM((PAIRS, RES, RES), BF16),
            pltpu.VMEM((RES, 128), F32),
            pltpu.VMEM((RES, 128), F32),
            pltpu.VMEM((40 * N, 128), F32),
            pltpu.VMEM((ROWS, RES, CH), BF16),
            pltpu.VMEM((N, 36, 128), BF16),
            pltpu.VMEM((N, 36, 128), BF16),
            *sems(2),
        ],
        compiler_params=params(collective_id),
        name="end",
    )(adj, right_all, left_all, own, fin, alignment, flank)


def to_cells(pair):
    turned = pair.reshape(ROWS, N, ROWS, CH).transpose(3, 0, 2, 1)
    return lax.optimization_barrier(turned.reshape(CH, CELLS))


def from_cells(cells):
    return cells.reshape(CH, ROWS, ROWS, N).transpose(1, 3, 2, 0).reshape(ROWS, RES, CH)


HALF = 1536
SHARE = HALF // (N // 2)


def reduce_kernel(
    flank_ref, fin_ref, in_ref, out_ref,
    flank_out, fin_out, proj_out, final_out, proj_in, final_in,
    mine, theirs, blocks, landed, own, full,
    sent0, got0, sent1, got1, sent2, got2, passed,
):
    greet()
    me = me_index()
    core = lax.rem(me, 2)
    chip = me // 2
    mine[0:64, :] = flank_ref[:, :128]
    mine[64:128, :] = flank_ref[:, 128:]
    mine[128:1152, :] = fin_ref[...]
    mine[1152:1920, :] = out_ref[...]
    mine[1920:2688, :] = in_ref[...]
    mine[2688:, :] = jnp.zeros((2 * HALF - 2688, 128), F32)
    all_here()
    result = Gather(own, full, sent2, got2, passed)

    def half(c):
        return pl.ds(pl.multiple_of(c * HALF, HALF), HALF)

    swap = remote(mine.at[half(1 - core)], theirs, sent0, got0, result.partner())
    swap.start()
    swap.wait_recv()
    for j in range(N // 2):
        at = pl.ds(pl.multiple_of(core * HALF + j * SHARE, 8), SHARE)
        blocks[j] = mine[at, :] + theirs[j * SHARE : (j + 1) * SHARE, :]

    def to(k):
        j = lax.rem(chip + k, N // 2)
        return remote(blocks.at[j], landed.at[chip], sent1.at[j], got1.at[chip], 2 * j + core)

    def back(k):
        j = lax.rem(chip + N // 2 - k, N // 2)
        return remote(blocks.at[j], landed.at[j], sent1.at[j], got1.at[j], 2 * j + core)

    loop(N // 2, lambda k: to(k).start(), 1)
    landed[chip] = blocks[chip]
    loop(N // 2, lambda k: back(k).wait_recv(), 1)
    own[...] = lax.fori_loop(
        0, N // 2, lambda j, total: total + landed[j], jnp.zeros((SHARE, 128), F32)
    ).astype(BF16)
    result.start()
    result.hand_on()
    result.finish()

    def place(s):
        at = pl.multiple_of(lax.rem(s, 2) * HALF + (s // 2) * SHARE, 8)
        theirs_or_mine[pl.ds(at, SHARE), :] = full[s].astype(F32)

    theirs_or_mine = mine
    swap.wait_send()
    loop(N, place)
    flank_out[:128, :] = mine[0:64, :].T
    flank_out[128:, :] = mine[64:128, :].T
    fin_out[...] = mine[128:1152, :]
    for base, proj, final in ((1152, proj_out, final_out), (1920, proj_in, final_in)):
        for b in range(5):
            proj[:, b * CH : (b + 1) * CH] = mine[base + b * CH : base + (b + 1) * CH, :]
        final[...] = mine[base + 5 * CH : base + 6 * CH, :]
    loop(N // 2, lambda k: to(k).wait_send(), 1)
    result.close()


def reduced(flank_sum, fin_sum, in_sums, out_sums, collective_id):
    one = pltpu.SemaphoreType.DMA
    return pl.pallas_call(
        reduce_kernel,
        out_shape=(
            shaped((FEATURES, 2 * HIDDEN), F32),
            shaped((HIDDEN * HIDDEN, CH), F32),
            shaped((CH, 5 * CH), F32),
            shaped((CH, CH), F32),
            shaped((CH, 5 * CH), F32),
            shaped((CH, CH), F32),
        ),
        in_specs=vmem(4),
        out_specs=tuple(vmem(6)),
        scratch_shapes=[
            pltpu.VMEM((2 * HALF, 128), F32),
            pltpu.VMEM((HALF, 128), F32),
            pltpu.VMEM((N // 2, SHARE, 128), F32),
            pltpu.VMEM((N // 2, SHARE, 128), F32),
            pltpu.VMEM((SHARE, 128), BF16),
            pltpu.VMEM((N, SHARE, 128), BF16),
            one(()),
            one(()),
            one((N // 2,)),
            one((N // 2,)),
            *sems(3),
        ],
        compiler_params=params(collective_id),
        name="reduce",
    )(flank_sum, fin_sum, in_sums, out_sums)


def shards(
    edge_embedding,
    alignment_embedding,
    tensor_flank_matrix,
    tensor_final_matrix,
    outward_sigmoid_matrix,
    outward_final_matrix,
    inward_sigmoid_matrix,
    inward_final_matrix,
    adjoint_seed,
):
    alignment = alignment_embedding.transpose(1, 0, 2)
    pair_cells, right_all, left_all, own = start(
        alignment, tensor_flank_matrix, tensor_final_matrix, edge_embedding.reshape(CELLS, CH), 5
    )
    two_cells, triangle_out, kept_out = triangle_update(
        pair_cells, outward_sigmoid_matrix, outward_final_matrix, True, 1
    )
    new_cells, triangle_in, kept_in = triangle_update(
        two_cells, inward_sigmoid_matrix, inward_final_matrix, False, 2
    )
    edge_embedding_updated = from_cells(new_cells)
    grad_two, in_sums = triangle_back(
        two_cells, inward_sigmoid_matrix, inward_final_matrix, triangle_in, kept_in,
        to_cells(adjoint_seed), False, F32, 3,
    )
    grad_one, out_sums = triangle_back(
        pair_cells, outward_sigmoid_matrix, outward_final_matrix, triangle_out, kept_out,
        grad_two, True, BF16, 4,
    )
    pair_adjoint, alignment_adjoint, flank_sum, fin_sum = end(
        grad_one, right_all, left_all, own, tensor_final_matrix, alignment,
        tensor_flank_matrix, 6,
    )
    sums = reduced(flank_sum, fin_sum, in_sums, out_sums, 7)
    return (
        edge_embedding_updated,
        pair_adjoint.reshape(ROWS, RES, CH),
        alignment_adjoint.transpose(1, 0, 2),
        *sums,
    )


def solution(mesh):
    placed = (
        P(("dp", "dap"), None, None),
        P("dp", "dap", None),
        P(),
        P(),
        P(),
        P(),
        P(),
        P(),
        P(("dp", "dap"), None, None),
    )
    return jax.shard_map(
        shards,
        mesh=mesh,
        in_specs=placed,
        out_specs=(
            P(("dp", "dap"), None, None),
            P(("dp", "dap"), None, None),
            P("dp", "dap", None),
            P("dp", None),
            P("dp", None),
            P("dp", None),
            P("dp", None),
            P("dp", None),
            P("dp", None),
        ),
        check_vma=False,
    )
```

```python
from types import SimpleNamespace

import jax
import jax.numpy as jnp
from jax import lax
from jax.experimental import pallas as pl
from jax.experimental.pallas import tpu as pltpu
from jax.sharding import PartitionSpec as P

EPSILON = 1e-05
F32, BF16 = jnp.float32, jnp.bfloat16
MESH = pl.DeviceIdType.MESH
N = 64
ROWS = 6
RES = 384
CELLS = ROWS * RES
CH = 128
GROUPS = CELLS // 128
PITCH = 72
HIDDEN = 32
PAIRS = HIDDEN // 2
SEQ = 64
FEATURES = 256
TILE = 256
TILES = CELLS // TILE
VMEM_LIMIT = 60 * 1024 * 1024


def nn(a, b):
    return lax.dot_general(a, b, (((1,), (0,)), ((), ())), preferred_element_type=F32)


def nt(a, b):
    return lax.dot_general(a, b, (((1,), (1,)), ((), ())), preferred_element_type=F32)


def one_hot(rows, columns, pick, dtype=BF16):
    row = lax.broadcasted_iota(jnp.int32, (rows, columns), 0)
    column = lax.broadcasted_iota(jnp.int32, (rows, columns), 1)
    return jnp.where(pick(row) == column, 1.0, 0.0).astype(dtype)


def identity(size):
    return one_hot(size, size, lambda r: r)


def hidden_order(dtype=BF16):
    return one_hot(CH, CH, lambda r: jnp.where(r < N, 2 * r, 2 * r - (CH - 1)), dtype)


def sigmoid(v):
    return 1.0 / (1.0 + jnp.exp(-v))


def ln0(v):
    centred = v - jnp.mean(v, axis=0, keepdims=True)
    factor = lax.rsqrt(jnp.mean(centred * centred, axis=0, keepdims=True) + EPSILON)
    return centred * factor, factor


def ln0_adjoint(hatted, factor, g):
    return factor * (
        g
        - jnp.mean(g, axis=0, keepdims=True)
        - hatted * jnp.mean(g * hatted, axis=0, keepdims=True)
    )


def loop(count, body, start=0):
    def step(k, carry):
        body(k)
        return carry

    lax.fori_loop(start, count, step, 0)


def me_index():
    return lax.axis_index("dap")


def greet():
    me = me_index()
    sem = pltpu.get_barrier_semaphore()
    loop(
        N,
        lambda k: pl.semaphore_signal(
            sem, inc=1, device_id={"dap": lax.rem(me + k, N)}, device_id_type=MESH
        ),
        1,
    )


def all_here():
    pl.semaphore_wait(pltpu.get_barrier_semaphore(), N - 1)


def remote(src, dst, send_sem, recv_sem, to):
    return pltpu.make_async_remote_copy(
        src_ref=src,
        dst_ref=dst,
        send_sem=send_sem,
        recv_sem=recv_sem,
        device_id={"dap": to},
        device_id_type=MESH,
    )


STRIDE = 37


def ahead(k):
    return lax.rem(me_index() + k * STRIDE, N)


def behind(k):
    return lax.rem(me_index() + N * STRIDE - k * STRIDE, N)


class Exchange:
    def __init__(self, out, into, sent, got, lo, hi):
        self.out, self.into, self.sent, self.got = out, into, sent, got
        self.rows = pl.ds(lo, hi - lo)

    def copy(self, d, at):
        return remote(
            self.out.at[d, self.rows], self.into.at[at, self.rows],
            self.sent.at[d], self.got.at[at], d,
        )

    def pack_and_send(self, rows_of):
        me = me_index()
        self.into[me, self.rows] = rows_of(me)

        def pack(d):
            self.out[d, self.rows] = rows_of(d)

        pack(ahead(1))

        def step(k):
            pack(ahead(k + 1))
            self.copy(ahead(k), me).start()

        loop(N - 1, step, 1)
        self.copy(ahead(N - 1), me).start()

    def receive(self, use):
        use(me_index())

        def step(k):
            s = behind(k)
            self.copy(s, s).wait_recv()
            use(s)

        loop(N, step, 1)

    def close(self):
        def step(k):
            d = ahead(k)
            self.copy(d, d).wait_send()

        loop(N, step, 1)


class Gather:
    def __init__(self, own, into, sent, got, passed):
        self.own, self.into, self.sent, self.got, self.passed = own, into, sent, got, passed

    def partner(self):
        me = me_index()
        return me + 1 - 2 * lax.rem(me, 2)

    def across(self, k):
        me = me_index()
        d = lax.rem(me + 2 * k, N)
        return remote(self.own, self.into.at[me], self.sent.at[k], self.got.at[me], d)

    def handed(self, s):
        return remote(
            self.into.at[s], self.into.at[s], self.passed.at[s], self.got.at[s], self.partner()
        )

    def home(self):
        me = me_index()
        return remote(
            self.own, self.into.at[me], self.passed.at[me], self.got.at[me], self.partner()
        )

    def start(self):
        self.into[me_index()] = self.own[...]
        loop(N // 2, lambda k: self.across(k).start(), 1)
        self.home().start()

    def hand_on(self):
        me = me_index()

        def step(k):
            s = lax.rem(me + N - 2 * k, N)
            self.handed(s).wait_recv()
            self.handed(s).start()

        loop(N // 2, step, 1)

    def finish(self):
        me, other = me_index(), self.partner()

        def step(k):
            self.handed(lax.rem(other + N - 2 * k, N)).wait_recv()

        loop(N // 2, step)

    def close(self):
        me = me_index()
        loop(N // 2, lambda k: self.across(k).wait_send(), 1)
        self.home().wait_send()
        loop(N // 2, lambda k: self.handed(lax.rem(me + N - 2 * k, N)).wait_send(), 1)


def ln1(v):
    centred = v - jnp.mean(v, axis=1, keepdims=True)
    factor = lax.rsqrt(jnp.mean(centred * centred, axis=1, keepdims=True) + EPSILON)
    return centred * factor, factor


def strided(ref, start, size, stride):
    return ref[pl.ds(start, size, stride=stride), :]


def packed(flat, lo, hi):
    return lambda d: strided(flat, lo * PITCH + d, hi - lo, PITCH).astype(BF16)


def widen_into(wide, into, lo, hi, pitch):
    def use(s):
        at = pl.multiple_of(s * pitch + lo, 8)
        wide[pl.ds(at, hi - lo), :] = into[s, pl.ds(lo, hi - lo)].astype(F32)

    return use


def lanes_of(t):
    return pl.ds(pl.multiple_of(t * TILE, TILE), TILE)


def row_lanes(r):
    return slice(r * RES, (r + 1) * RES)


def pair_lanes(p):
    return pl.ds(pl.multiple_of(p * 128, 128), 128)


def scatter_hidden(flat, value, piece, t):
    for q in range(TILE // 128):
        at = pl.multiple_of((piece * GROUPS + t * (TILE // 128) + q) * PITCH, 8)
        flat[pl.ds(at, N), :] = value[:, q * 128 : (q + 1) * 128]


def gather_hidden(wide, pitch, bases, t):
    parts = []
    for base in bases:
        row = [
            strided(wide, base + t * (TILE // 128) + q, N, pitch) for q in range(TILE // 128)
        ]
        parts.append(jnp.concatenate(row, axis=1))
    return jnp.concatenate(parts, axis=0)


def scatter_rows(flat, value, piece):
    for r in range(ROWS):
        for jg in range(3):
            at = (piece * GROUPS + r * 3 + jg) * PITCH
            flat[at : at + N, :] = value[r * N : (r + 1) * N, jg * 128 : (jg + 1) * 128]


def gather_matrix(out, wide, pitch, base):
    for r in range(ROWS):
        for jg in range(3):
            out[r * N : (r + 1) * N, jg * 128 : (jg + 1) * 128] = strided(
                wide, base + r * 3 + jg, N, pitch
            ).astype(BF16)


def prepare(w, p_ref, f_ref):
    order = hidden_order()
    for b in range(4):
        block = p_ref[:, b * CH : (b + 1) * CH]
        turned = nt(order, block).astype(BF16)
        for m in range(2):
            w.turned[m, b * N : (b + 1) * N, :] = turned[m * N : (m + 1) * N]
        w.straight[:, b * CH : (b + 1) * CH] = nt(block, order).astype(BF16)
    w.gate[...] = nt(identity(CH), p_ref[:, 4 * CH :]).astype(BF16)
    w.straight[:, 4 * CH :] = p_ref[:, 4 * CH :]
    w.final[...] = nn(order, f_ref[...]).astype(BF16)
    w.final_turned[...] = nt(identity(CH), w.final[...]).astype(BF16)


def update(c, u, w, outgoing, x_ref, new_ref):
    one_a = Exchange(c.out_two, u.in_ops, u.sent[0], u.got[0], 0, 40)
    one_b = Exchange(c.out_two, u.in_ops, u.sent[1], u.got[1], 40, 72)
    two_a = Exchange(c.out_one, u.in_tri, u.sent[2], u.got[2], 0, 16)
    two_b = Exchange(c.out_one, u.in_tri, u.sent[3], u.got[3], 16, 40)

    def gated(m, t):
        pre = nn(w.turned[m], u.norm[:, lanes_of(t)])
        scatter_hidden(c.flat, sigmoid(pre[:N]) * pre[N : 2 * N], 2 * m, t)
        scatter_hidden(c.flat, sigmoid(pre[2 * N : 3 * N]) * pre[3 * N :], 2 * m + 1, t)

    def first(t):
        at = lanes_of(t)
        hatted, _ = ln0(x_ref[:, at].astype(F32))
        u.norm[:, at] = hatted.astype(BF16)
        gated(0, t)

    loop(TILES, first)
    loop(2, lambda t: gated(1, t))
    one_a.pack_and_send(packed(c.flat, 0, 40))
    loop(TILES, lambda t: gated(1, t), 2)
    one_b.pack_and_send(packed(c.flat, 40, 72))

    def gates(t):
        at = lanes_of(t)
        u.gate[:, at] = sigmoid(nn(w.gate[...], u.norm[:, at]))

    loop(TILES, gates)
    for m in range(2):
        if m == 0:
            one_a.receive(widen_into(c.wide, u.in_ops, 0, 40, 72))
        else:
            one_b.receive(widen_into(c.wide, u.in_ops, 40, 72, 72))
        for op in range(2):
            gather_matrix(u.kept.at[2 * op + m], c.wide, 72, (2 * m + op) * GROUPS)
        left, right = u.kept[m], u.kept[2 + m]
        product = nt(left, right) if outgoing else nn(left.T, right)
        scatter_rows(c.flat_one, product, m)
        if m == 0:
            two_a.pack_and_send(packed(c.flat_one, 0, 16))
        else:
            two_b.pack_and_send(packed(c.flat_one, 16, 40))
    one_a.close()
    one_b.close()
    two_a.receive(widen_into(c.wide, u.in_tri, 0, 16, 40))
    two_b.receive(widen_into(c.wide, u.in_tri, 16, 40, 40))

    def rows_out(t):
        at = lanes_of(t)
        tri = gather_hidden(c.wide, 40, (0, GROUPS), t)
        u.tri[:, at] = tri.astype(BF16)
        unit, _ = ln0(tri)
        values = nn(w.final_turned[...], unit.astype(BF16))
        new_ref[:, at] = (x_ref[:, at].astype(F32) + u.gate[:, at] * values).astype(BF16)

    def finish():
        loop(TILES, rows_out)
        two_a.close()
        two_b.close()

    return finish


def back(c, u, w, outgoing, x_ref, gz_ref, gnew_ref, sums_at, between):
    one_a = Exchange(c.out_one, u.in_grad, u.sent[4], u.got[4], 0, 24)
    one_b = Exchange(c.out_one, u.in_grad, u.sent[5], u.got[5], 24, 40)
    two_a = Exchange(c.out_two, u.in_back, u.sent[6], u.got[6], 0, 32)
    two_b = Exchange(c.out_two, u.in_back, u.sent[7], u.got[7], 32, 72)

    def rows_in(t):
        at = lanes_of(t)
        gate = u.gate[:, at]
        tri_hat, tri_factor = ln0(u.tri[:, at].astype(F32))
        unit = tri_hat.astype(BF16)
        values = nn(w.final_turned[...], unit)
        scaled_wide = gz_ref[:, at].astype(F32) * gate
        scaled = scaled_wide.astype(BF16)
        c.unit[:, at] = unit
        c.scaled[:, at] = scaled
        c.grad_proj[4 * CH :, at] = (scaled_wide * values * (1.0 - gate)).astype(BF16)
        grad = ln0_adjoint(tri_hat, tri_factor, nn(w.final[...], scaled))
        for m in range(2):
            scatter_hidden(c.flat_one, grad[m * N : (m + 1) * N], m, t)

    loop(TILES, rows_in)
    one_a.pack_and_send(packed(c.flat_one, 0, 24))
    one_b.pack_and_send(packed(c.flat_one, 24, 40))
    between()

    def coefficients(t):
        at = lanes_of(t)
        for m in range(2):
            pre = nn(w.turned[m], u.norm[:, at])
            for side in range(2):
                opened = sigmoid(pre[2 * side * N : (2 * side + 1) * N])
                slope = pre[(2 * side + 1) * N : (2 * side + 2) * N] * opened * (1.0 - opened)
                rows = 2 * side * CH + m * N
                c.coef[rows : rows + N, at] = slope
                c.coef[rows + CH : rows + CH + N, at] = opened

    loop(TILES, coefficients)
    exact = dict(preferred_element_type=F32, precision=lax.Precision.HIGHEST)
    order_wide = hidden_order(F32)

    def keep_sum(block, value):
        at = sums_at + block * CH
        c.mine[at : at + CH, :] = value

    keep_sum(
        5,
        lax.dot_general(
            order_wide, nt(c.unit[...], c.scaled[...]), (((0,), (0,)), ((), ())), **exact
        ),
    )
    keep_sum(4, nt(u.norm[...], c.grad_proj[4 * CH :, :]))
    for m in range(2):
        if m == 0:
            one_a.receive(widen_into(c.wide, u.in_grad, 0, 24, 40))
        else:
            one_b.receive(widen_into(c.wide, u.in_grad, 24, 40, 40))
        gather_matrix(c.grad_m, c.wide, 40, m * GROUPS)
        grad = c.grad_m[...]
        left, right = u.kept[m], u.kept[2 + m]
        if outgoing:
            grad_left, grad_right = nn(grad, right), nn(grad.T, left)
        else:
            grad_left, grad_right = nt(right, grad), nn(left, grad)
        scatter_rows(c.flat, grad_left, 2 * m)
        scatter_rows(c.flat, grad_right, 2 * m + 1)
        if m == 0:
            two_a.pack_and_send(packed(c.flat, 0, 32))
        else:
            two_b.pack_and_send(packed(c.flat, 32, 72))
    one_a.close()
    one_b.close()
    two_a.receive(widen_into(c.wide, u.in_back, 0, 32, 72))
    two_b.receive(widen_into(c.wide, u.in_back, 32, 72, 72))

    def rows_out(t):
        at = lanes_of(t)
        for side in range(2):
            base = 2 * side * CH
            grad = gather_hidden(c.wide, 72, (side * GROUPS, (2 + side) * GROUPS), t)
            for half in range(2):
                rows = pl.ds(base + half * CH, CH)
                c.grad_proj[rows, at] = (grad * c.coef[rows, at]).astype(BF16)
        grad_norm = nn(w.straight[...], c.grad_proj[:, at])
        hatted, factor = ln0(x_ref[:, at].astype(F32))
        gnew_ref[:, at] = (
            gz_ref[:, at].astype(F32) + ln0_adjoint(hatted, factor, grad_norm)
        ).astype(gnew_ref.dtype)

    def finish():
        loop(TILES, rows_out)
        two_a.close()
        two_b.close()

    def sums():
        for b in range(4):
            here = nt(u.norm[...], c.grad_proj[b * CH : (b + 1) * CH, :])
            keep_sum(
                b, lax.dot_general(here, order_wide, (((1,), (0,)), ((), ())), **exact)
            )

    return finish, sums


class Total:
    def __init__(self, mine, theirs, blocks, landed, own, full, sems_of):
        self.mine, self.theirs, self.blocks, self.landed = mine, theirs, blocks, landed
        self.own, self.half = own, theirs.shape[0]
        self.share = self.half // (N // 2)
        self.sent0, self.got0, self.sent1, self.got1, *rest = sems_of
        self.gather = Gather(own, full, *rest)

    def swap(self):
        core = lax.rem(me_index(), 2)
        other = pl.ds(pl.multiple_of((1 - core) * self.half, 8), self.half)
        return remote(
            self.mine.at[other], self.theirs, self.sent0, self.got0, self.gather.partner()
        )

    def to(self, k):
        me = me_index()
        chip, core = me // 2, lax.rem(me, 2)
        j = lax.rem(chip + k, N // 2)
        return remote(
            self.blocks.at[j], self.landed.at[chip], self.sent1.at[j], self.got1.at[chip],
            2 * j + core,
        )

    def back(self, k):
        me = me_index()
        chip, core = me // 2, lax.rem(me, 2)
        j = lax.rem(chip + N // 2 - k, N // 2)
        return remote(
            self.blocks.at[j], self.landed.at[j], self.sent1.at[j], self.got1.at[j], 2 * j + core
        )

    def scatter(self):
        core, chip = lax.rem(me_index(), 2), me_index() // 2
        self.swap().wait_recv()
        mine = self.mine[pl.ds(pl.multiple_of(core * self.half, 8), self.half), :]
        for j in range(N // 2):
            at = slice(j * self.share, (j + 1) * self.share)
            self.blocks[j] = mine[at] + self.theirs[at, :]
        loop(N // 2, lambda k: self.to(k).start(), 1)
        self.landed[chip] = self.blocks[chip]

    def spread(self):
        loop(N // 2, lambda k: self.back(k).wait_recv(), 1)
        total = lax.fori_loop(
            0, N // 2, lambda j, sofar: sofar + self.landed[j],
            jnp.zeros(self.landed.shape[1:], F32),
        )
        self.own[...] = (total * (1.0 / RES)).astype(self.own.dtype)
        self.gather.start()

    def close(self):
        self.swap().wait_send()
        loop(N // 2, lambda k: self.to(k).wait_send(), 1)
        self.gather.close()


def alignment_rows(c, r):
    return jnp.concatenate([strided(c.align_wide.at[h], r, SEQ, 8) for h in range(2)], axis=1)


def spread_out(all_ref, wide, into):
    loop(N, widen_into(wide, into, 0, 96, 104))
    for r in range(ROWS):
        for p in range(PAIRS):
            all_ref[r * N : (r + 1) * N, p * 128 : (p + 1) * 128] = strided(
                wide, r * PAIRS + p, N, 104
            ).astype(BF16)


def cells_of(c, ref, out):
    for r in range(ROWS):
        c.cells_wide[:RES, :] = ref[row_lanes(r), :].astype(F32)
        parts = [strided(c.cells_wide, q, N, ROWS) for q in range(ROWS)]
        out[:, row_lanes(r)] = jnp.concatenate(parts, 0).T.astype(BF16)


def outer_sums(c, weights, of_row, all_ref, acc, by_rows):
    for r in range(ROWS):
        block = (nt if by_rows else nn)(weights[...], of_row(r))
        for p in range(PAIRS):
            c.outer_grad[p, r * 64 : (r + 1) * 64, :] = block[p * 64 : (p + 1) * 64].astype(BF16)
    acc[...] = jnp.zeros_like(acc)

    def add(p):
        acc[...] += nn(c.outer_grad[p], all_ref[:, pair_lanes(p)])

    loop(PAIRS, add)


def matched(acc, r):
    return acc[r * 64 : r * 64 + 32, :] + pltpu.roll(acc[r * 64 + 32 : (r + 1) * 64, :], 64, 1)


def whole_kernel(names, *refs):
    c = SimpleNamespace(**dict(zip(names, refs)))
    greet()
    phases = []
    for kind in ("out", "in"):
        part = lambda name: getattr(c, name + "_" + kind)
        phases.append(
            SimpleNamespace(
                norm=part("norm"), gate=part("gate"), tri=part("tri"), kept=part("kept"),
                in_ops=part("in_ops"), in_tri=part("in_tri"),
                in_grad=part("in_grad"), in_back=part("in_back"),
                sent=[part("sent%d" % i) for i in range(8)],
                got=[part("got%d" % i) for i in range(8)],
                weights=SimpleNamespace(
                    turned=part("turned"), straight=part("straight"), gate=part("w_gate"),
                    final=part("final"), final_turned=part("final_turned"),
                ),
            )
        )
    out, into = phases

    def widen_alignment(s):
        rows = c.alignment[s].astype(F32)
        at = pl.ds(pl.multiple_of(s * 8, 8), ROWS)
        for h in range(2):
            c.align_wide[h, at, :] = rows[:, h * 128 : (h + 1) * 128]

    loop(SEQ, widen_alignment)
    flank = c.flank[...]
    split = lambda first: one_hot(
        HIDDEN, 2 * HIDDEN, lambda r: first + jnp.where(r < PAIRS, 2 * r, 2 * r - (HIDDEN - 1))
    )
    split_left = nt(split(0), flank).astype(BF16)
    split_right = nt(split(HIDDEN), flank).astype(BF16)
    plain_left = nt(one_hot(HIDDEN, 2 * HIDDEN, lambda r: r), flank).astype(BF16)
    none = jnp.zeros((SEQ, FEATURES), BF16)
    for r in range(ROWS):
        hatted, _ = ln1(alignment_rows(c, r))
        norm = hatted.astype(BF16)
        halves = (jnp.concatenate([norm, none], 0), jnp.concatenate([none, norm], 0))
        here = pl.ds(r * PAIRS, PAIRS)
        for block, weights in ((c.own_right, split_right), (c.own_left, split_left)):
            block[here, :] = (
                nt(weights[:PAIRS], halves[0]) + nt(weights[PAIRS:], halves[1])
            ).astype(BF16)
        for h in range(2):
            at = (2 * r + h) * HIDDEN
            c.own_outer[at : at + HIDDEN, :] = nt(plain_left, halves[h]).astype(BF16)
    all_here()
    right = Gather(c.own_right, c.in_right, c.sent_r, c.got_r, c.pass_r)
    left = Gather(c.own_left, c.in_left, c.sent_l, c.got_l, c.pass_l)
    right.start()
    cells_of(c, c.edge, c.x_one)
    cells_of(c, c.seed, c.seed_cells)
    prepare(out.weights, c.p_out, c.f_out)
    prepare(into.weights, c.p_in, c.f_in)
    c.fin_wide[...] = c.fin[...].astype(F32)
    for d in range(HIDDEN):
        c.fin_split[d * HIDDEN : (d + 1) * HIDDEN, :] = strided(
            c.fin_wide, d, HIDDEN, HIDDEN
        ).astype(BF16)
    c.fin_turned[...] = nt(identity(CH), c.fin_split[...]).astype(BF16)
    c.flat_one[2 * GROUPS * PITCH :, :] = jnp.zeros((4 * PITCH, 128), F32)
    right.hand_on()
    right.finish()
    spread_out(c.right_all, c.wide, c.in_right)

    def outer_pair(p):
        block = nt(c.own_outer[...], c.right_all[:, pair_lanes(p)]) * (1.0 / SEQ)
        for r in range(ROWS):
            c.outer[r, pl.ds(pl.multiple_of(p * 64, 64), 64), :] = block[
                r * 64 : (r + 1) * 64
            ].astype(BF16)

    loop(PAIRS, outer_pair)
    for r in range(ROWS):
        at = row_lanes(r)
        c.x_one[:, at] = (c.x_one[:, at].astype(F32) + nn(c.fin_turned[...], c.outer[r])).astype(
            BF16
        )
    right.close()

    update(c, out, out.weights, True, c.x_one, c.x_two)()
    finish = update(c, into, into.weights, False, c.x_two, c.new_cells)
    left.start()
    finish()

    def pass_left():
        left.hand_on()

    finish, sums = back(
        c, into, into.weights, False, c.x_two, c.seed_cells, c.grad_two, 1792, pass_left
    )
    finish()
    sums()

    def take_left():
        left.finish()
        left.close()

    finish, sums = back(
        c, out, out.weights, True, c.x_one, c.grad_two, c.adjoint, 1024, take_left
    )
    finish()

    for r in range(ROWS):
        turned = c.adjoint[:, row_lanes(r)].astype(F32).T
        for q in range(ROWS):
            at = (r * ROWS + q) * PITCH
            c.flat_one[at : at + N, :] = turned[q * N : (q + 1) * N]
    pair = Exchange(c.out_one, c.in_pair, c.sent_p, c.got_p, 0, 40)
    pair.pack_and_send(packed(c.flat_one, 0, 40))
    sums()
    total = None
    for r in range(ROWS):
        part = nt(c.outer[r], c.adjoint[:, row_lanes(r)])
        total = part if total is None else total + part
    c.fin_wide[...] = total
    for k in range(HIDDEN):
        c.mine[k * HIDDEN : (k + 1) * HIDDEN, :] = strided(c.fin_wide, k, HIDDEN, HIDDEN)
    large = Total(
        c.mine, c.theirs, c.blocks, c.landed, c.own_sum, c.full,
        (c.swap_a0, c.swap_a1, c.sent_a, c.got_a, c.sent_ag, c.got_ag, c.pass_ag),
    )
    small = Total(
        c.flank_sum, c.flank_theirs, c.flank_blocks, c.flank_landed, c.flank_own, c.flank_full,
        (c.swap_b0, c.swap_b1, c.sent_b, c.got_b, c.sent_bg, c.got_bg, c.pass_bg),
    )
    large.swap().start()
    spread_out(c.left_all, c.wide, c.in_left)
    large.scatter()
    outer_sums(
        c, c.fin_split, lambda r: c.adjoint[:, row_lanes(r)], c.right_all, c.acc_left, False
    )
    pair.receive(widen_into(c.wide, c.in_pair, 0, 40, 40))
    for q in range(ROWS):
        for r in range(ROWS):
            c.columns[q, r * N : (r + 1) * N, :] = strided(c.wide, r * ROWS + q, N, 40).astype(
                BF16
            )
    large.spread()
    outer_sums(c, c.fin, lambda q: c.columns[q], c.left_all, c.acc_right, True)
    large.gather.hand_on()
    flank_turned = nt(identity(2 * HIDDEN), flank).astype(BF16)
    lane = lax.broadcasted_iota(jnp.int32, (2 * HIDDEN, 2 * SEQ), 1)
    flank_sum = jnp.zeros((2 * HIDDEN, FEATURES), F32)
    grads = []
    for r in range(ROWS):
        both = jnp.concatenate([matched(c.acc_left, r), matched(c.acc_right, r)], 0)
        both = jnp.where(lane < SEQ, both * (1.0 / SEQ), 0.0)
        c.flank_grad[r] = both
        hatted, _ = ln1(alignment_rows(c, r))
        norm = jnp.concatenate([hatted.astype(BF16), none], 0)
        flank_sum = flank_sum + nn(both.astype(BF16), norm)
    c.flank_sum[: 2 * HIDDEN, :] = flank_sum[:, :128]
    c.flank_sum[2 * HIDDEN :, :] = flank_sum[:, 128:]
    small.swap().start()
    small.scatter()
    for r in range(ROWS):
        grad = nn(c.flank_grad[r].T[:SEQ].astype(BF16), flank_turned)
        hatted, factor = ln1(alignment_rows(c, r))
        c.align_grad[r] = (
            factor
            * (
                grad
                - jnp.mean(grad, axis=1, keepdims=True)
                - hatted * jnp.mean(grad * hatted, axis=1, keepdims=True)
            )
        ).astype(BF16)
    small.spread()
    pair.close()
    small.gather.hand_on()
    large.gather.finish()
    small.gather.finish()
    large.close()
    small.close()


def vmem(count):
    return [pl.BlockSpec(memory_space=pltpu.VMEM)] * count


def shaped(shape, dtype):
    return jax.ShapeDtypeStruct(shape, dtype)


INPUTS = ("edge", "alignment", "flank", "fin", "p_out", "f_out", "p_in", "f_in", "seed")
OUTPUTS = dict(
    new_cells=((CH, CELLS), BF16),
    adjoint=((CH, CELLS), BF16),
    align_grad=((ROWS, SEQ, FEATURES), BF16),
    full=((N, 40, 128), BF16),
    flank_full=((N, 2, 128), F32),
)


def scratch():
    shapes = dict(
        x_one=((CH, CELLS), BF16),
        x_two=((CH, CELLS), BF16),
        seed_cells=((CH, CELLS), BF16),
        grad_two=((CH, CELLS), F32),
        flat=((72 * PITCH, 128), F32),
        flat_one=((40 * PITCH, 128), F32),
        wide=((104 * N, 128), F32),
        out_two=((N, 72, 128), BF16),
        out_one=((N, 40, 128), BF16),
        unit=((CH, CELLS), BF16),
        scaled=((CH, CELLS), BF16),
        coef=((4 * CH, CELLS), F32),
        grad_proj=((5 * CH, CELLS), BF16),
        grad_m=((RES, RES), BF16),
        mine=((2560, 128), F32),
        theirs=((1280, 128), F32),
        blocks=((N // 2, 40, 128), F32),
        landed=((N // 2, 40, 128), F32),
        own_sum=((40, 128), BF16),
        flank_sum=((128, 128), F32),
        flank_theirs=((64, 128), F32),
        flank_blocks=((N // 2, 2, 128), F32),
        flank_landed=((N // 2, 2, 128), F32),
        flank_own=((2, 128), F32),
        flank_grad=((ROWS, 2 * HIDDEN, 128), F32),
        align_wide=((2, SEQ * 8, 128), F32),
        own_right=((96, 128), BF16),
        own_left=((96, 128), BF16),
        own_outer=((2 * ROWS * HIDDEN, 2 * SEQ), BF16),
        in_right=((N, 96, 128), BF16),
        in_left=((N, 96, 128), BF16),
        right_all=((RES, HIDDEN * SEQ), BF16),
        left_all=((RES, HIDDEN * SEQ), BF16),
        cells_wide=((RES, 128), F32),
        fin_wide=((HIDDEN * HIDDEN, CH), F32),
        fin_split=((HIDDEN * HIDDEN, CH), BF16),
        fin_turned=((CH, HIDDEN * HIDDEN), BF16),
        outer=((ROWS, HIDDEN * HIDDEN, RES), BF16),
        outer_grad=((PAIRS, RES, RES), BF16),
        acc_left=((RES, 128), F32),
        acc_right=((RES, 128), F32),
        columns=((ROWS, RES, CH), BF16),
        in_pair=((N, 40, 128), BF16),
    )
    each = dict(
        norm=((CH, CELLS), BF16),
        gate=((CH, CELLS), F32),
        tri=((CH, CELLS), BF16),
        kept=((4, RES, RES), BF16),
        in_ops=((N, 72, 128), BF16),
        in_tri=((N, 40, 128), BF16),
        in_grad=((N, 40, 128), BF16),
        in_back=((N, 72, 128), BF16),
        turned=((2, 4 * N, CH), BF16),
        straight=((CH, 5 * CH), BF16),
        w_gate=((CH, CH), BF16),
        final=((CH, CH), BF16),
        final_turned=((CH, CH), BF16),
    )
    for kind in ("out", "in"):
        shapes.update({name + "_" + kind: value for name, value in each.items()})
    made = {name: pltpu.VMEM(*value) for name, value in shapes.items()}
    flags = {}
    for kind in ("out", "in"):
        for i in range(8):
            flags["sent%d_%s" % (i, kind)] = (N,)
            flags["got%d_%s" % (i, kind)] = (N,)
    for tail in ("r", "l", "ag", "bg"):
        for name in ("sent_", "got_", "pass_"):
            flags[name + tail] = (N,)
    flags["sent_p"] = flags["got_p"] = (N,)
    for tail in ("a", "b"):
        flags["sent_" + tail] = flags["got_" + tail] = (N // 2,)
        flags["swap_%s0" % tail] = flags["swap_%s1" % tail] = ()
    made.update({name: pltpu.SemaphoreType.DMA(shape) for name, shape in flags.items()})
    return made


def whole(*arrays):
    made = scratch()
    names = INPUTS + tuple(OUTPUTS) + tuple(made)
    return pl.pallas_call(
        lambda *refs: whole_kernel(names, *refs),
        out_shape=tuple(shaped(*value) for value in OUTPUTS.values()),
        in_specs=vmem(len(INPUTS)),
        out_specs=tuple(vmem(len(OUTPUTS))),
        scratch_shapes=list(made.values()),
        compiler_params=pltpu.CompilerParams(
            collective_id=1, has_side_effects=True, vmem_limit_bytes=67_043_328
        ),
        name="window",
    )(*arrays)


def finish_kernel(
    new_ref, adj_ref, align_ref, full_ref, flank_ref,
    new_out, adj_out, align_out, flank_out, fin_out, proj_out, final_out, proj_in, final_in,
    cells, align_wide, sums, flank_rows,
):
    for ref, out in ((new_ref, new_out), (adj_ref, adj_out)):
        for r in range(ROWS):
            turned = ref[:, row_lanes(r)].astype(F32).T
            for q in range(ROWS):
                cells[pl.ds(q, N, stride=ROWS), :] = turned[q * N : (q + 1) * N]
            out[row_lanes(r), :] = cells[...].astype(BF16)
    for r in range(ROWS):
        for h in range(2):
            align_wide[h, pl.ds(r, SEQ, stride=8), :] = align_ref[
                r, :, h * 128 : (h + 1) * 128
            ].astype(F32)

    def narrow(s):
        at = pl.ds(pl.multiple_of(s * 8, 8), ROWS)
        align_out[s] = jnp.concatenate(
            [align_wide[0, at, :], align_wide[1, at, :]], axis=1
        ).astype(BF16)

    loop(SEQ, narrow)

    def place(s):
        at = pl.multiple_of((lax.rem(s, 2) * (N // 2) + s // 2) * 40, 8)
        sums[pl.ds(at, 40), :] = full_ref[s].astype(F32)

    loop(N, place)
    fin_out[...] = sums[:1024, :]
    for base, proj, final in ((1024, proj_out, final_out), (1792, proj_in, final_in)):
        for b in range(5):
            proj[:, b * CH : (b + 1) * CH] = sums[base + b * CH : base + (b + 1) * CH, :]
        final[...] = sums[base + 5 * CH : base + 6 * CH, :]
    for j in range(N // 2):
        for core in range(2):
            flank_rows[core * 64 + 2 * j : core * 64 + 2 * j + 2, :] = flank_ref[2 * j + core]
    flank_out[:128, :] = flank_rows[:64, :].T
    flank_out[128:, :] = flank_rows[64:, :].T


def shards(
    edge_embedding,
    alignment_embedding,
    tensor_flank_matrix,
    tensor_final_matrix,
    outward_sigmoid_matrix,
    outward_final_matrix,
    inward_sigmoid_matrix,
    inward_final_matrix,
    adjoint_seed,
):
    results = whole(
        edge_embedding.reshape(CELLS, CH),
        alignment_embedding,
        tensor_flank_matrix,
        tensor_final_matrix,
        outward_sigmoid_matrix,
        outward_final_matrix,
        inward_sigmoid_matrix,
        inward_final_matrix,
        adjoint_seed.reshape(CELLS, CH),
    )
    outs = pl.pallas_call(
        finish_kernel,
        out_shape=(
            shaped((CELLS, CH), BF16),
            shaped((CELLS, CH), BF16),
            shaped((SEQ, ROWS, FEATURES), BF16),
            shaped((FEATURES, 2 * HIDDEN), F32),
            shaped((HIDDEN * HIDDEN, CH), F32),
            shaped((CH, 5 * CH), F32),
            shaped((CH, CH), F32),
            shaped((CH, 5 * CH), F32),
            shaped((CH, CH), F32),
        ),
        in_specs=vmem(5),
        out_specs=tuple(vmem(9)),
        scratch_shapes=[
            pltpu.VMEM((RES, 128), F32),
            pltpu.VMEM((2, SEQ * 8, 128), F32),
            pltpu.VMEM((2560, 128), F32),
            pltpu.VMEM((128, 128), F32),
        ],
        compiler_params=pltpu.CompilerParams(vmem_limit_bytes=VMEM_LIMIT),
        name="finish",
    )(*results)
    return (
        outs[0].reshape(ROWS, RES, CH),
        outs[1].reshape(ROWS, RES, CH),
        *outs[2:],
    )


def solution(mesh):
    placed = (
        P(("dp", "dap"), None, None),
        P("dp", "dap", None),
        P(),
        P(),
        P(),
        P(),
        P(),
        P(),
        P(("dp", "dap"), None, None),
    )
    return jax.shard_map(
        shards,
        mesh=mesh,
        in_specs=placed,
        out_specs=(
            P(("dp", "dap"), None, None),
            P(("dp", "dap"), None, None),
            P("dp", "dap", None),
            P("dp", None),
            P("dp", None),
            P("dp", None),
            P("dp", None),
            P("dp", None),
            P("dp", None),
        ),
        check_vma=False,
    )
```

```python
from types import SimpleNamespace

import jax
import jax.numpy as jnp
from jax import lax
from jax.experimental import pallas as pl
from jax.experimental.pallas import tpu as pltpu
from jax.sharding import PartitionSpec as P

EPSILON = 1e-05
F32, BF16 = jnp.float32, jnp.bfloat16
MESH = pl.DeviceIdType.MESH
N = 64
ROWS = 6
RES = 384
CELLS = ROWS * RES
CH = 128
GROUPS = CELLS // 128
PITCH = 72
HIDDEN = 32
PAIRS = HIDDEN // 2
SEQ = 64
FEATURES = 256
TILE = 256
TILES = CELLS // TILE
VMEM_LIMIT = 60 * 1024 * 1024


def nn(a, b):
    return lax.dot_general(a, b, (((1,), (0,)), ((), ())), preferred_element_type=F32)


def nt(a, b):
    return lax.dot_general(a, b, (((1,), (1,)), ((), ())), preferred_element_type=F32)


def one_hot(rows, columns, pick, dtype=BF16):
    row = lax.broadcasted_iota(jnp.int32, (rows, columns), 0)
    column = lax.broadcasted_iota(jnp.int32, (rows, columns), 1)
    return jnp.where(pick(row) == column, 1.0, 0.0).astype(dtype)


def identity(size):
    return one_hot(size, size, lambda r: r)


def hidden_order(dtype=BF16):
    return one_hot(CH, CH, lambda r: jnp.where(r < N, 2 * r, 2 * r - (CH - 1)), dtype)


def sigmoid(v):
    return 1.0 / (1.0 + jnp.exp(-v))


def ln0(v):
    centred = v - jnp.mean(v, axis=0, keepdims=True)
    factor = lax.rsqrt(jnp.mean(centred * centred, axis=0, keepdims=True) + EPSILON)
    return centred * factor, factor


def ln0_adjoint(hatted, factor, g):
    return factor * (
        g
        - jnp.mean(g, axis=0, keepdims=True)
        - hatted * jnp.mean(g * hatted, axis=0, keepdims=True)
    )


def loop(count, body, start=0):
    def step(k, carry):
        body(k)
        return carry

    lax.fori_loop(start, count, step, 0)


def me_index():
    return lax.axis_index("dap")


def greet():
    me = me_index()
    sem = pltpu.get_barrier_semaphore()
    loop(
        N,
        lambda k: pl.semaphore_signal(
            sem, inc=1, device_id={"dap": lax.rem(me + k, N)}, device_id_type=MESH
        ),
        1,
    )


def all_here():
    pl.semaphore_wait(pltpu.get_barrier_semaphore(), N - 1)


def remote(src, dst, send_sem, recv_sem, to):
    return pltpu.make_async_remote_copy(
        src_ref=src,
        dst_ref=dst,
        send_sem=send_sem,
        recv_sem=recv_sem,
        device_id={"dap": to},
        device_id_type=MESH,
    )


BATCH = 3
STRIDE = 37


def ahead(k):
    return lax.rem(me_index() + k * STRIDE, N)


def behind(k):
    return lax.rem(me_index() + N * STRIDE - k * STRIDE, N)


class Exchange:
    def __init__(self, out, into, sent, got, lo, hi):
        self.out, self.into, self.sent, self.got = out, into, sent, got
        self.rows = pl.ds(lo, hi - lo)

    def copy(self, d, at):
        return remote(
            self.out.at[d, self.rows], self.into.at[at, self.rows], self.sent, self.got.at[at], d
        )

    def pack_and_send(self, rows_of):
        me = me_index()
        self.into[me, self.rows] = rows_of(me)

        def pack(first):
            for k in range(BATCH):
                d = ahead(first + k)
                self.out[d, self.rows] = rows_of(d)

        def send(first):
            for k in range(BATCH):
                self.copy(ahead(first + k), me).start()

        pack(1)

        def step(b):
            pack(1 + BATCH * b)
            send(1 + BATCH * (b - 1))

        loop((N - 1) // BATCH, step, 1)
        send(N - BATCH)

    def receive(self, use):
        use(me_index())

        def step(b):
            sources = [behind(1 + BATCH * b + k) for k in range(BATCH)]
            for s in sources:
                self.copy(s, s).wait_recv()
            for s in sources:
                use(s)

        loop((N - 1) // BATCH, step)

    def close(self):
        others = pl.ds(0, N - 1)
        remote(
            self.out.at[others, self.rows], self.into.at[others, self.rows],
            self.sent, self.got.at[0], ahead(1),
        ).wait_send()


class Gather:
    def __init__(self, own, into, sent, got, passed):
        self.own, self.into, self.sent, self.got, self.passed = own, into, sent, got, passed

    def partner(self):
        me = me_index()
        return me + 1 - 2 * lax.rem(me, 2)

    def across(self, k):
        me = me_index()
        d = lax.rem(me + 2 * k, N)
        return remote(self.own, self.into.at[me], self.sent.at[k], self.got.at[me], d)

    def handed(self, s):
        return remote(
            self.into.at[s], self.into.at[s], self.passed.at[s], self.got.at[s], self.partner()
        )

    def home(self):
        me = me_index()
        return remote(
            self.own, self.into.at[me], self.passed.at[me], self.got.at[me], self.partner()
        )

    def start(self):
        self.into[me_index()] = self.own[...]
        loop(N // 2, lambda k: self.across(k).start(), 1)
        self.home().start()

    def hand_on(self):
        me = me_index()

        def step(k):
            s = lax.rem(me + N - 2 * k, N)
            self.handed(s).wait_recv()
            self.handed(s).start()

        loop(N // 2, step, 1)

    def finish(self):
        me, other = me_index(), self.partner()

        def step(k):
            self.handed(lax.rem(other + N - 2 * k, N)).wait_recv()

        loop(N // 2, step)

    def close(self):
        me = me_index()
        loop(N // 2, lambda k: self.across(k).wait_send(), 1)
        self.home().wait_send()
        loop(N // 2, lambda k: self.handed(lax.rem(me + N - 2 * k, N)).wait_send(), 1)


def ln1(v):
    centred = v - jnp.mean(v, axis=1, keepdims=True)
    factor = lax.rsqrt(jnp.mean(centred * centred, axis=1, keepdims=True) + EPSILON)
    return centred * factor, factor


def strided(ref, start, size, stride):
    return ref[pl.ds(start, size, stride=stride), :]


def packed(flat, lo, hi):
    return lambda d: strided(flat, lo * PITCH + d, hi - lo, PITCH).astype(BF16)


def widen_into(wide, into, lo, hi, pitch):
    def use(s):
        at = pl.multiple_of(s * pitch + lo, 8)
        wide[pl.ds(at, hi - lo), :] = into[s, pl.ds(lo, hi - lo)].astype(F32)

    return use


def lanes_of(t):
    return pl.ds(pl.multiple_of(t * TILE, TILE), TILE)


def row_lanes(r):
    return slice(r * RES, (r + 1) * RES)


def pair_lanes(p):
    return pl.ds(pl.multiple_of(p * 128, 128), 128)


def scatter_hidden(flat, value, piece, t):
    for q in range(TILE // 128):
        at = pl.multiple_of((piece * GROUPS + t * (TILE // 128) + q) * PITCH, 8)
        flat[pl.ds(at, N), :] = value[:, q * 128 : (q + 1) * 128]


def gather_hidden(wide, pitch, bases, t):
    parts = []
    for base in bases:
        row = [
            strided(wide, base + t * (TILE // 128) + q, N, pitch) for q in range(TILE // 128)
        ]
        parts.append(jnp.concatenate(row, axis=1))
    return jnp.concatenate(parts, axis=0)


def scatter_rows(flat, value, piece):
    for r in range(ROWS):
        for jg in range(3):
            at = (piece * GROUPS + r * 3 + jg) * PITCH
            flat[at : at + N, :] = value[r * N : (r + 1) * N, jg * 128 : (jg + 1) * 128]


def gather_matrix(out, wide, pitch, base):
    for r in range(ROWS):
        for jg in range(3):
            out[r * N : (r + 1) * N, jg * 128 : (jg + 1) * 128] = strided(
                wide, base + r * 3 + jg, N, pitch
            ).astype(BF16)


def prepare(w, p_ref, f_ref):
    order = hidden_order()
    for b in range(4):
        block = p_ref[:, b * CH : (b + 1) * CH]
        turned = nt(order, block).astype(BF16)
        for m in range(2):
            w.turned[m, b * N : (b + 1) * N, :] = turned[m * N : (m + 1) * N]
        w.straight[:, b * CH : (b + 1) * CH] = nt(block, order).astype(BF16)
    w.gate[...] = nt(identity(CH), p_ref[:, 4 * CH :]).astype(BF16)
    w.straight[:, 4 * CH :] = p_ref[:, 4 * CH :]
    w.final[...] = nn(order, f_ref[...]).astype(BF16)
    w.final_turned[...] = nt(identity(CH), w.final[...]).astype(BF16)


def tiles(body, stop=TILES, start=0, by=3):
    def step(b):
        for k in range(by):
            body(start + by * b + k)

    loop((stop - start) // by, step)
    for t in range(start + (stop - start) // by * by, stop):
        body(t)


class Update:
    def __init__(self, c, u, w, outgoing, sums_at):
        self.c, self.u, self.w, self.outgoing, self.sums_at = c, u, w, outgoing, sums_at
        plan = (
            ("ops_a", c.out_two, u.in_ops, 0, 40),
            ("ops_b", c.out_two, u.in_ops, 40, 72),
            ("tri_a", c.out_one, u.in_tri, 0, 16),
            ("tri_b", c.out_one, u.in_tri, 16, 40),
            ("grad_a", c.out_one, u.in_grad, 0, 24),
            ("grad_b", c.out_one, u.in_grad, 24, 40),
            ("back_a", c.out_two, u.in_back, 0, 32),
            ("back_b", c.out_two, u.in_back, 32, 72),
        )
        for i, (name, out, into, lo, hi) in enumerate(plan):
            setattr(self, name, Exchange(out, into, u.sent[i], u.got[i], lo, hi))

    def gated(self, m, t, norm=None):
        norm = self.u.norm[:, lanes_of(t)] if norm is None else norm
        pre = nn(self.w.turned[m], norm)
        flat = self.c.flat
        scatter_hidden(flat, sigmoid(pre[:N]) * pre[N : 2 * N], 2 * m, t)
        scatter_hidden(flat, sigmoid(pre[2 * N : 3 * N]) * pre[3 * N :], 2 * m + 1, t)

    def enter(self, t, x):
        norm = ln0(x)[0].astype(BF16)
        self.u.norm[:, lanes_of(t)] = norm
        self.gated(0, t, norm)

    def gates(self, t):
        at = lanes_of(t)
        self.u.gate[:, at] = sigmoid(nn(self.w.gate[...], self.u.norm[:, at]))

    def arrived(self, t):
        tri = gather_hidden(self.c.wide, 40, (0, GROUPS), t)
        hatted, factor = ln0(tri)
        unit = hatted.astype(BF16)
        return tri, hatted, factor, unit, nn(self.w.final_turned[...], unit)

    def descend(self, t, gz, hatted, factor, unit, values):
        c, at = self.c, lanes_of(t)
        gate = self.u.gate[:, at]
        scaled_wide = gz * gate
        scaled = scaled_wide.astype(BF16)
        c.unit[:, at] = unit
        c.scaled[:, at] = scaled
        c.grad_proj[4 * CH :, at] = (scaled_wide * values * (1.0 - gate)).astype(BF16)
        grad = ln0_adjoint(hatted, factor, nn(self.w.final[...], scaled))
        for m in range(2):
            scatter_hidden(c.flat_one, grad[m * N : (m + 1) * N], m, t)

    def coefficients(self, t):
        c, at = self.c, lanes_of(t)
        norm = self.u.norm[:, at]
        for m in range(2):
            pre = nn(self.w.turned[m], norm)
            for side in range(2):
                opened = sigmoid(pre[2 * side * N : (2 * side + 1) * N])
                slope = pre[(2 * side + 1) * N : (2 * side + 2) * N] * opened * (1.0 - opened)
                rows = 2 * side * CH + m * N
                c.coef[rows : rows + N, at] = slope
                c.coef[rows + CH : rows + CH + N, at] = opened

    def returned(self, t, x, gz):
        c, at = self.c, lanes_of(t)
        for side in range(2):
            base = 2 * side * CH
            grad = gather_hidden(c.wide, 72, (side * GROUPS, (2 + side) * GROUPS), t)
            for half in range(2):
                rows = pl.ds(base + half * CH, CH)
                c.grad_proj[rows, at] = (grad * c.coef[rows, at]).astype(BF16)
        grad_norm = nn(self.w.straight[...], c.grad_proj[:, at])
        hatted, factor = ln0(x)
        return gz + ln0_adjoint(hatted, factor, grad_norm)

    def keep_sum(self, block, value):
        at = self.sums_at + block * CH
        self.c.mine[at : at + CH, :] = value

    def early_sums(self):
        self.keep_sum(5, nt(self.c.unit[...], self.c.scaled[...]))
        self.keep_sum(4, nt(self.u.norm[...], self.c.grad_proj[4 * CH :, :]))

    def late_sums(self):
        for b in range(4):
            self.keep_sum(b, nt(self.u.norm[...], self.c.grad_proj[b * CH : (b + 1) * CH, :]))

    def forward(self):
        c, u = self.c, self.u
        tiles(lambda t: self.gated(1, t), 2, 0, 2)
        self.ops_a.pack_and_send(packed(c.flat, 0, 40))
        tiles(lambda t: self.gated(1, t), TILES, 2)
        self.ops_b.pack_and_send(packed(c.flat, 40, 72))
        tiles(self.gates)
        for m in range(2):
            if m == 0:
                self.ops_a.receive(widen_into(c.wide, u.in_ops, 0, 40, 72))
            else:
                self.ops_b.receive(widen_into(c.wide, u.in_ops, 40, 72, 72))
            for op in range(2):
                gather_matrix(u.kept.at[2 * op + m], c.wide, 72, (2 * m + op) * GROUPS)
            left, right = u.kept[m], u.kept[2 + m]
            product = nt(left, right) if self.outgoing else nn(left.T, right)
            scatter_rows(c.flat_one, product, m)
            if m == 0:
                self.tri_a.pack_and_send(packed(c.flat_one, 0, 16))
            else:
                self.tri_b.pack_and_send(packed(c.flat_one, 16, 40))
        self.ops_a.close()
        self.ops_b.close()
        self.tri_a.receive(widen_into(c.wide, u.in_tri, 0, 16, 40))
        self.tri_b.receive(widen_into(c.wide, u.in_tri, 16, 40, 40))
        self.tri_a.close()
        self.tri_b.close()

    def backward(self, between):
        c, u = self.c, self.u
        self.grad_a.pack_and_send(packed(c.flat_one, 0, 24))
        self.grad_b.pack_and_send(packed(c.flat_one, 24, 40))
        between()
        tiles(self.coefficients)
        self.early_sums()
        for m in range(2):
            if m == 0:
                self.grad_a.receive(widen_into(c.wide, u.in_grad, 0, 24, 40))
            else:
                self.grad_b.receive(widen_into(c.wide, u.in_grad, 24, 40, 40))
            gather_matrix(c.grad_m, c.wide, 40, m * GROUPS)
            grad = c.grad_m[...]
            left, right = u.kept[m], u.kept[2 + m]
            if self.outgoing:
                grad_left, grad_right = nn(grad, right), nn(grad.T, left)
            else:
                grad_left, grad_right = nt(right, grad), nn(left, grad)
            scatter_rows(c.flat, grad_left, 2 * m)
            scatter_rows(c.flat, grad_right, 2 * m + 1)
            if m == 0:
                self.back_a.pack_and_send(packed(c.flat, 0, 32))
            else:
                self.back_b.pack_and_send(packed(c.flat, 32, 72))
        self.grad_a.close()
        self.grad_b.close()
        self.back_a.receive(widen_into(c.wide, u.in_back, 0, 32, 72))
        self.back_b.receive(widen_into(c.wide, u.in_back, 32, 72, 72))
        self.back_a.close()
        self.back_b.close()


class Total:
    def __init__(self, mine, theirs, blocks, landed, own, full, sems_of):
        self.mine, self.theirs, self.blocks, self.landed = mine, theirs, blocks, landed
        self.own, self.half = own, theirs.shape[0]
        self.share = self.half // (N // 2)
        self.sent0, self.got0, self.sent1, self.got1, *rest = sems_of
        self.gather = Gather(own, full, *rest)

    def swap(self):
        core = lax.rem(me_index(), 2)
        other = pl.ds(pl.multiple_of((1 - core) * self.half, 8), self.half)
        return remote(
            self.mine.at[other], self.theirs, self.sent0, self.got0, self.gather.partner()
        )

    def to(self, k):
        me = me_index()
        chip, core = me // 2, lax.rem(me, 2)
        j = lax.rem(chip + k, N // 2)
        return remote(
            self.blocks.at[j], self.landed.at[chip], self.sent1.at[j], self.got1.at[chip],
            2 * j + core,
        )

    def back(self, k):
        me = me_index()
        chip, core = me // 2, lax.rem(me, 2)
        j = lax.rem(chip + N // 2 - k, N // 2)
        return remote(
            self.blocks.at[j], self.landed.at[j], self.sent1.at[j], self.got1.at[j], 2 * j + core
        )

    def scatter(self):
        core, chip = lax.rem(me_index(), 2), me_index() // 2
        self.swap().wait_recv()
        mine = self.mine[pl.ds(pl.multiple_of(core * self.half, 8), self.half), :]
        for j in range(N // 2):
            at = slice(j * self.share, (j + 1) * self.share)
            self.blocks[j] = mine[at] + self.theirs[at, :]
        loop(N // 2, lambda k: self.to(k).start(), 1)
        self.landed[chip] = self.blocks[chip]

    def spread(self):
        loop(N // 2, lambda k: self.back(k).wait_recv(), 1)
        total = lax.fori_loop(
            0, N // 2, lambda j, sofar: sofar + self.landed[j],
            jnp.zeros(self.landed.shape[1:], F32),
        )
        self.own[...] = (total * (1.0 / RES)).astype(self.own.dtype)
        self.gather.start()

    def close(self):
        self.swap().wait_send()
        loop(N // 2, lambda k: self.to(k).wait_send(), 1)
        self.gather.close()


def spread_out(all_ref, wide, into):
    loop(N, widen_into(wide, into, 0, 96, 104))
    for r in range(ROWS):
        for p in range(PAIRS):
            all_ref[r * N : (r + 1) * N, p * 128 : (p + 1) * 128] = strided(
                wide, r * PAIRS + p, N, 104
            ).astype(BF16)


def cells_of(c, ref, out):
    for r in range(ROWS):
        c.cells_wide[:RES, :] = ref[row_lanes(r), :].astype(F32)
        parts = [strided(c.cells_wide, q, N, ROWS) for q in range(ROWS)]
        out[:, row_lanes(r)] = jnp.concatenate(parts, 0).T.astype(BF16)


def outer_sums(c, weights, of_row, all_ref, acc, by_rows):
    for r in range(ROWS):
        block = (nt if by_rows else nn)(weights[...], of_row(r))
        for p in range(PAIRS):
            c.outer_grad[p, r * 64 : (r + 1) * 64, :] = block[p * 64 : (p + 1) * 64].astype(BF16)
    acc[...] = jnp.zeros_like(acc)

    def add(b):
        part = None
        for k in range(4):
            here = nn(c.outer_grad[4 * b + k], all_ref[:, pair_lanes(4 * b + k)])
            part = here if part is None else part + here
        acc[...] += part

    loop(PAIRS // 4, add)


def matched(acc, r):
    return acc[r * 64 : r * 64 + 32, :] + pltpu.roll(acc[r * 64 + 32 : (r + 1) * 64, :], 64, 1)


def whole_kernel(names, *refs):
    c = SimpleNamespace(**dict(zip(names, refs)))
    greet()
    phases = []
    for kind in ("out", "in"):
        part = lambda name: getattr(c, name + "_" + kind)
        phases.append(
            SimpleNamespace(
                norm=part("norm"), gate=part("gate"), tri=part("tri"), kept=part("kept"),
                in_ops=part("in_ops"), in_tri=part("in_tri"),
                in_grad=part("in_grad"), in_back=part("in_back"),
                sent=[part("sent%d" % i) for i in range(8)],
                got=[part("got%d" % i) for i in range(8)],
                weights=SimpleNamespace(
                    turned=part("turned"), straight=part("straight"), gate=part("w_gate"),
                    final=part("final"), final_turned=part("final_turned"),
                ),
            )
        )
    out, into = phases

    flank_turned = c.flank[...]
    split = lambda first: one_hot(
        HIDDEN, 2 * HIDDEN, lambda r: first + jnp.where(r < PAIRS, 2 * r, 2 * r - (HIDDEN - 1))
    )
    split_left = nn(split(0), flank_turned).astype(BF16)
    split_right = nn(split(HIDDEN), flank_turned).astype(BF16)
    plain_left = flank_turned[:HIDDEN]
    none = jnp.zeros((SEQ, FEATURES), BF16)
    for r in range(ROWS):
        hatted, _ = ln1(c.alignment[r].astype(F32))
        norm = hatted.astype(BF16)
        halves = (jnp.concatenate([norm, none], 0), jnp.concatenate([none, norm], 0))
        here = pl.ds(r * PAIRS, PAIRS)
        for block, weights in ((c.own_right, split_right), (c.own_left, split_left)):
            block[here, :] = (
                nt(weights[:PAIRS], halves[0]) + nt(weights[PAIRS:], halves[1])
            ).astype(BF16)
        for h in range(2):
            at = (2 * r + h) * HIDDEN
            c.own_outer[at : at + HIDDEN, :] = nt(plain_left, halves[h]).astype(BF16)
    all_here()
    right = Gather(c.own_right, c.in_right, c.sent_r, c.got_r, c.pass_r)
    left = Gather(c.own_left, c.in_left, c.sent_l, c.got_l, c.pass_l)
    right.start()
    cells_of(c, c.edge, c.x_one)
    cells_of(c, c.seed, c.seed_cells)
    prepare(out.weights, c.p_out, c.f_out)
    prepare(into.weights, c.p_in, c.f_in)
    c.fin_wide[...] = c.fin[...].astype(F32)
    for d in range(HIDDEN):
        c.fin_split[d * HIDDEN : (d + 1) * HIDDEN, :] = strided(
            c.fin_wide, d, HIDDEN, HIDDEN
        ).astype(BF16)
    c.fin_turned[...] = nt(identity(CH), c.fin_split[...]).astype(BF16)
    c.flat_one[2 * GROUPS * PITCH :, :] = jnp.zeros((4 * PITCH, 128), F32)
    right.hand_on()
    right.finish()
    spread_out(c.right_all, c.wide, c.in_right)

    def outer_pair(p):
        block = nt(c.own_outer[...], c.right_all[:, pair_lanes(p)]) * (1.0 / SEQ)
        for r in range(ROWS):
            c.outer[r, pl.ds(pl.multiple_of(p * 64, 64), 64), :] = block[
                r * 64 : (r + 1) * 64
            ].astype(BF16)

    tiles(outer_pair, PAIRS, 0, 4)
    for r in range(ROWS):
        at = row_lanes(r)
        c.x_one[:, at] = (c.x_one[:, at].astype(F32) + nn(c.fin_turned[...], c.outer[r])).astype(
            BF16
        )
    right.close()

    one = Update(c, out, out.weights, True, 1024)
    two = Update(c, into, into.weights, False, 1792)
    tiles(lambda t: one.enter(t, c.x_one[:, lanes_of(t)].astype(F32)))
    one.forward()

    def between_updates(t):
        at = lanes_of(t)
        tri, _, _, _, values = one.arrived(t)
        out.tri[:, at] = tri.astype(BF16)
        new = (c.x_one[:, at].astype(F32) + out.gate[:, at] * values).astype(BF16)
        c.x_two[:, at] = new
        two.enter(t, new.astype(F32))

    tiles(between_updates)
    two.forward()
    left.start()

    def turn_round(t):
        at = lanes_of(t)
        _, hatted, factor, unit, values = two.arrived(t)
        c.new_cells[:, at] = (
            c.x_two[:, at].astype(F32) + into.gate[:, at] * values
        ).astype(BF16)
        two.descend(t, c.seed_cells[:, at].astype(F32), hatted, factor, unit, values)

    tiles(turn_round)
    two.backward(left.hand_on)

    def between_backs(t):
        at = lanes_of(t)
        grad = two.returned(t, c.x_two[:, at].astype(F32), c.seed_cells[:, at].astype(F32))
        c.grad_two[:, at] = grad
        hatted, factor = ln0(out.tri[:, at].astype(F32))
        unit = hatted.astype(BF16)
        one.descend(t, grad, hatted, factor, unit, nn(out.weights.final_turned[...], unit))

    tiles(between_backs)

    def meanwhile():
        two.late_sums()
        left.finish()
        left.close()

    one.backward(meanwhile)

    def last(t):
        at = lanes_of(t)
        c.adjoint[:, at] = one.returned(
            t, c.x_one[:, at].astype(F32), c.grad_two[:, at]
        ).astype(BF16)

    tiles(last)

    for r in range(ROWS):
        turned = c.adjoint[:, row_lanes(r)].astype(F32).T
        for q in range(ROWS):
            at = (r * ROWS + q) * PITCH
            c.flat_one[at : at + N, :] = turned[q * N : (q + 1) * N]
    pair = Exchange(c.out_one, c.in_pair, c.sent_p, c.got_p, 0, 40)
    pair.pack_and_send(packed(c.flat_one, 0, 40))
    one.late_sums()
    total = None
    for r in range(ROWS):
        part = nt(c.outer[r], c.adjoint[:, row_lanes(r)])
        total = part if total is None else total + part
    c.fin_wide[...] = total
    for k in range(HIDDEN):
        c.mine[k * HIDDEN : (k + 1) * HIDDEN, :] = strided(c.fin_wide, k, HIDDEN, HIDDEN)
    large = Total(
        c.mine, c.theirs, c.blocks, c.landed, c.own_sum, c.full,
        (c.swap_a0, c.swap_a1, c.sent_a, c.got_a, c.sent_ag, c.got_ag, c.pass_ag),
    )
    small = Total(
        c.flank_sum, c.flank_theirs, c.flank_blocks, c.flank_landed, c.flank_own, c.flank_full,
        (c.swap_b0, c.swap_b1, c.sent_b, c.got_b, c.sent_bg, c.got_bg, c.pass_bg),
    )
    large.swap().start()
    spread_out(c.left_all, c.wide, c.in_left)
    large.scatter()
    outer_sums(
        c, c.fin_split, lambda r: c.adjoint[:, row_lanes(r)], c.right_all, c.acc_left, False
    )
    pair.receive(widen_into(c.wide, c.in_pair, 0, 40, 40))
    for q in range(ROWS):
        for r in range(ROWS):
            c.columns[q, r * N : (r + 1) * N, :] = strided(c.wide, r * ROWS + q, N, 40).astype(
                BF16
            )
    large.spread()
    outer_sums(c, c.fin, lambda q: c.columns[q], c.left_all, c.acc_right, True)
    large.gather.hand_on()
    lane = lax.broadcasted_iota(jnp.int32, (2 * HIDDEN, 2 * SEQ), 1)
    flank_sum = jnp.zeros((2 * HIDDEN, FEATURES), F32)
    grads = []
    for r in range(ROWS):
        both = jnp.concatenate([matched(c.acc_left, r), matched(c.acc_right, r)], 0)
        both = jnp.where(lane < SEQ, both * (1.0 / SEQ), 0.0)
        c.flank_grad[r] = both
        hatted, _ = ln1(c.alignment[r].astype(F32))
        norm = jnp.concatenate([hatted.astype(BF16), none], 0)
        flank_sum = flank_sum + nn(both.astype(BF16), norm)
    c.flank_sum[: 2 * HIDDEN, :] = flank_sum[:, :128]
    c.flank_sum[2 * HIDDEN :, :] = flank_sum[:, 128:]
    small.swap().start()
    small.scatter()
    for r in range(ROWS):
        grad = nn(c.flank_grad[r].T[:SEQ].astype(BF16), flank_turned)
        hatted, factor = ln1(c.alignment[r].astype(F32))
        c.align_grad[r] = (
            factor
            * (
                grad
                - jnp.mean(grad, axis=1, keepdims=True)
                - hatted * jnp.mean(grad * hatted, axis=1, keepdims=True)
            )
        ).astype(BF16)
    small.spread()
    pair.close()
    small.gather.hand_on()
    large.gather.finish()
    small.gather.finish()
    large.close()
    small.close()


def vmem(count):
    return [pl.BlockSpec(memory_space=pltpu.VMEM)] * count


def shaped(shape, dtype):
    return jax.ShapeDtypeStruct(shape, dtype)


INPUTS = ("edge", "alignment", "flank", "fin", "p_out", "f_out", "p_in", "f_in", "seed")
OUTPUTS = dict(
    new_cells=((CH, CELLS), BF16),
    adjoint=((CH, CELLS), BF16),
    align_grad=((ROWS, SEQ, FEATURES), BF16),
    full=((N, 40, 128), BF16),
    flank_full=((N, 2, 128), F32),
)


def scratch():
    shapes = dict(
        x_one=((CH, CELLS), BF16),
        x_two=((CH, CELLS), BF16),
        seed_cells=((CH, CELLS), BF16),
        grad_two=((CH, CELLS), F32),
        flat=((72 * PITCH, 128), F32),
        flat_one=((40 * PITCH, 128), F32),
        wide=((104 * N, 128), F32),
        out_two=((N, 72, 128), BF16),
        out_one=((N, 40, 128), BF16),
        unit=((CH, CELLS), BF16),
        scaled=((CH, CELLS), BF16),
        coef=((4 * CH, CELLS), F32),
        grad_proj=((5 * CH, CELLS), BF16),
        grad_m=((RES, RES), BF16),
        mine=((2560, 128), F32),
        theirs=((1280, 128), F32),
        blocks=((N // 2, 40, 128), F32),
        landed=((N // 2, 40, 128), F32),
        own_sum=((40, 128), BF16),
        flank_sum=((128, 128), F32),
        flank_theirs=((64, 128), F32),
        flank_blocks=((N // 2, 2, 128), F32),
        flank_landed=((N // 2, 2, 128), F32),
        flank_own=((2, 128), F32),
        flank_grad=((ROWS, 2 * HIDDEN, 128), F32),
        own_right=((96, 128), BF16),
        own_left=((96, 128), BF16),
        own_outer=((2 * ROWS * HIDDEN, 2 * SEQ), BF16),
        in_right=((N, 96, 128), BF16),
        in_left=((N, 96, 128), BF16),
        right_all=((RES, HIDDEN * SEQ), BF16),
        left_all=((RES, HIDDEN * SEQ), BF16),
        cells_wide=((RES, 128), F32),
        fin_wide=((HIDDEN * HIDDEN, CH), F32),
        fin_split=((HIDDEN * HIDDEN, CH), BF16),
        fin_turned=((CH, HIDDEN * HIDDEN), BF16),
        outer=((ROWS, HIDDEN * HIDDEN, RES), BF16),
        outer_grad=((PAIRS, RES, RES), BF16),
        acc_left=((RES, 128), F32),
        acc_right=((RES, 128), F32),
        columns=((ROWS, RES, CH), BF16),
        in_pair=((N, 40, 128), BF16),
    )
    each = dict(
        norm=((CH, CELLS), BF16),
        gate=((CH, CELLS), F32),
        tri=((CH, CELLS), BF16),
        kept=((4, RES, RES), BF16),
        in_ops=((N, 72, 128), BF16),
        in_tri=((N, 40, 128), BF16),
        in_grad=((N, 40, 128), BF16),
        in_back=((N, 72, 128), BF16),
        turned=((2, 4 * N, CH), BF16),
        straight=((CH, 5 * CH), BF16),
        w_gate=((CH, CH), BF16),
        final=((CH, CH), BF16),
        final_turned=((CH, CH), BF16),
    )
    for kind in ("out", "in"):
        shapes.update({name + "_" + kind: value for name, value in each.items()})
    made = {name: pltpu.VMEM(*value) for name, value in shapes.items()}
    flags = {}
    for kind in ("out", "in"):
        for i in range(8):
            flags["sent%d_%s" % (i, kind)] = ()
            flags["got%d_%s" % (i, kind)] = (N,)
    for tail in ("r", "l", "ag", "bg"):
        for name in ("sent_", "got_", "pass_"):
            flags[name + tail] = (N,)
    flags["sent_p"], flags["got_p"] = (), (N,)
    for tail in ("a", "b"):
        flags["sent_" + tail] = flags["got_" + tail] = (N // 2,)
        flags["swap_%s0" % tail] = flags["swap_%s1" % tail] = ()
    made.update({name: pltpu.SemaphoreType.DMA(shape) for name, shape in flags.items()})
    return made


def whole(*arrays):
    made = scratch()
    names = INPUTS + tuple(OUTPUTS) + tuple(made)
    return pl.pallas_call(
        lambda *refs: whole_kernel(names, *refs),
        out_shape=tuple(shaped(*value) for value in OUTPUTS.values()),
        in_specs=vmem(len(INPUTS)),
        out_specs=tuple(vmem(len(OUTPUTS))),
        scratch_shapes=list(made.values()),
        compiler_params=pltpu.CompilerParams(
            collective_id=1, has_side_effects=True, vmem_limit_bytes=67_043_328
        ),
        name="window",
    )(*arrays)


def finish_kernel(
    new_ref, adj_ref, align_ref, full_ref, flank_ref,
    new_out, adj_out, align_out, flank_out, fin_out, proj_out, final_out, proj_in, final_in,
    cells, sums, flank_rows,
):
    for ref, out in ((new_ref, new_out), (adj_ref, adj_out)):
        for r in range(ROWS):
            turned = ref[:, row_lanes(r)].astype(F32).T
            for q in range(ROWS):
                cells[pl.ds(q, N, stride=ROWS), :] = turned[q * N : (q + 1) * N]
            out[row_lanes(r), :] = cells[...].astype(BF16)
    align_out[...] = align_ref[...]
    order = hidden_order()

    def place(s):
        at = pl.multiple_of((lax.rem(s, 2) * (N // 2) + s // 2) * 40, 8)
        sums[pl.ds(at, 40), :] = full_ref[s].astype(F32)

    loop(N, place)
    fin_out[...] = sums[:1024, :]
    for base, proj, final in ((1024, proj_out, final_out), (1792, proj_in, final_in)):
        for b in range(5):
            block = sums[base + b * CH : base + (b + 1) * CH, :]
            proj[:, b * CH : (b + 1) * CH] = nn(block.astype(BF16), order) if b < 4 else block
        block = sums[base + 5 * CH : base + 6 * CH, :]
        final[...] = nn(order.T, block.astype(BF16))
    for j in range(N // 2):
        for core in range(2):
            flank_rows[core * 64 + 2 * j : core * 64 + 2 * j + 2, :] = flank_ref[2 * j + core]
    flank_out[:, :128] = flank_rows[:64, :]
    flank_out[:, 128:] = flank_rows[64:, :]


def shards(
    edge_embedding,
    alignment_embedding,
    tensor_flank_matrix,
    tensor_final_matrix,
    outward_sigmoid_matrix,
    outward_final_matrix,
    inward_sigmoid_matrix,
    inward_final_matrix,
    adjoint_seed,
):
    results = whole(
        edge_embedding.reshape(CELLS, CH),
        alignment_embedding.transpose(1, 0, 2),
        tensor_flank_matrix.T,
        tensor_final_matrix,
        outward_sigmoid_matrix,
        outward_final_matrix,
        inward_sigmoid_matrix,
        inward_final_matrix,
        adjoint_seed.reshape(CELLS, CH),
    )
    outs = pl.pallas_call(
        finish_kernel,
        out_shape=(
            shaped((CELLS, CH), BF16),
            shaped((CELLS, CH), BF16),
            shaped((ROWS, SEQ, FEATURES), BF16),
            shaped((2 * HIDDEN, FEATURES), F32),
            shaped((HIDDEN * HIDDEN, CH), F32),
            shaped((CH, 5 * CH), F32),
            shaped((CH, CH), F32),
            shaped((CH, 5 * CH), F32),
            shaped((CH, CH), F32),
        ),
        in_specs=vmem(5),
        out_specs=tuple(vmem(9)),
        scratch_shapes=[
            pltpu.VMEM((RES, 128), F32),
            pltpu.VMEM((2560, 128), F32),
            pltpu.VMEM((128, 128), F32),
        ],
        compiler_params=pltpu.CompilerParams(vmem_limit_bytes=VMEM_LIMIT),
        name="finish",
    )(*results)
    return (
        outs[0].reshape(ROWS, RES, CH),
        outs[1].reshape(ROWS, RES, CH),
        outs[2].transpose(1, 0, 2),
        outs[3].T,
        *outs[4:],
    )


def solution(mesh):
    placed = (
        P(("dp", "dap"), None, None),
        P("dp", "dap", None),
        P(),
        P(),
        P(),
        P(),
        P(),
        P(),
        P(("dp", "dap"), None, None),
    )
    return jax.shard_map(
        shards,
        mesh=mesh,
        in_specs=placed,
        out_specs=(
            P(("dp", "dap"), None, None),
            P(("dp", "dap"), None, None),
            P("dp", "dap", None),
            P("dp", None),
            P("dp", None),
            P("dp", None),
            P("dp", None),
            P("dp", None),
            P("dp", None),
        ),
        check_vma=False,
    )
```

```python
from types import SimpleNamespace

import jax
import jax.numpy as jnp
from jax import lax
from jax.experimental import pallas as pl
from jax.experimental.pallas import tpu as pltpu
from jax.sharding import PartitionSpec as P

EPSILON = 1e-05
F32, BF16 = jnp.float32, jnp.bfloat16
MESH = pl.DeviceIdType.MESH
N = 64
ROWS = 6
RES = 384
CELLS = ROWS * RES
CH = 128
GROUPS = CELLS // 128
PITCH = 72
HIDDEN = 32
PAIRS = HIDDEN // 2
SEQ = 64
FEATURES = 256
TILE = 256
TILES = CELLS // TILE
VMEM_LIMIT = 60 * 1024 * 1024


def nn(a, b):
    return lax.dot_general(a, b, (((1,), (0,)), ((), ())), preferred_element_type=F32)


def nt(a, b):
    return lax.dot_general(a, b, (((1,), (1,)), ((), ())), preferred_element_type=F32)


def one_hot(rows, columns, pick, dtype=BF16):
    row = lax.broadcasted_iota(jnp.int32, (rows, columns), 0)
    column = lax.broadcasted_iota(jnp.int32, (rows, columns), 1)
    return jnp.where(pick(row) == column, 1.0, 0.0).astype(dtype)


def identity(size):
    return one_hot(size, size, lambda r: r)


def hidden_order(dtype=BF16):
    return one_hot(CH, CH, lambda r: jnp.where(r < N, 2 * r, 2 * r - (CH - 1)), dtype)


def sigmoid(v):
    return 1.0 / (1.0 + jnp.exp(-v))


def ln0(v):
    centred = v - jnp.mean(v, axis=0, keepdims=True)
    factor = lax.rsqrt(jnp.mean(centred * centred, axis=0, keepdims=True) + EPSILON)
    return centred * factor, factor


def ln0_adjoint(hatted, factor, g):
    return factor * (
        g
        - jnp.mean(g, axis=0, keepdims=True)
        - hatted * jnp.mean(g * hatted, axis=0, keepdims=True)
    )


def loop(count, body, start=0):
    def step(k, carry):
        body(k)
        return carry

    lax.fori_loop(start, count, step, 0)


def me_index():
    return lax.axis_index("dap")


def greet():
    me = me_index()
    sem = pltpu.get_barrier_semaphore()
    loop(
        N,
        lambda k: pl.semaphore_signal(
            sem, inc=1, device_id={"dap": lax.rem(me + k, N)}, device_id_type=MESH
        ),
        1,
    )


def all_here():
    pl.semaphore_wait(pltpu.get_barrier_semaphore(), N - 1)


def remote(src, dst, send_sem, recv_sem, to):
    return pltpu.make_async_remote_copy(
        src_ref=src,
        dst_ref=dst,
        send_sem=send_sem,
        recv_sem=recv_sem,
        device_id={"dap": to},
        device_id_type=MESH,
    )


BATCH = 3
CHIPS = N // 2
CHIP_STRIDE = 13
STRIDE = 37


def ahead(k):
    return lax.rem(me_index() + k * STRIDE, N)


def tiles(body, stop=TILES, start=0, by=3):
    def step(b):
        for k in range(by):
            body(start + by * b + k)

    loop((stop - start) // by, step)
    for t in range(start + (stop - start) // by * by, stop):
        body(t)


class Exchange:
    def __init__(self, out, into, sent, got, lo, hi):
        self.out, self.into, self.sent, self.got = out, into, sent, got
        self.rows = pl.ds(lo, hi - lo)

    def copy(self, d, at):
        return remote(
            self.out.at[d, self.rows], self.into.at[at, self.rows], self.sent, self.got, d
        )

    def pack_and_send(self, rows_of):
        me = me_index()
        self.into[me, self.rows] = rows_of(me)

        def pack(first):
            for k in range(BATCH):
                d = ahead(first + k)
                self.out[d, self.rows] = rows_of(d)

        def send(first):
            for k in range(BATCH):
                self.copy(ahead(first + k), me).start()

        pack(1)

        def step(b):
            pack(1 + BATCH * b)
            send(1 + BATCH * (b - 1))

        loop((N - 1) // BATCH, step, 1)
        send(N - BATCH)

    def all_others(self):
        others = pl.ds(0, N - 1)
        return remote(
            self.out.at[others, self.rows], self.into.at[others, self.rows],
            self.sent, self.got, ahead(1),
        )

    def receive(self, use):
        self.all_others().wait_recv()
        tiles(use, N, 0, 4)

    def close(self):
        self.all_others().wait_send()


class Gather:
    def __init__(self, own, into, sent, got, passed, heard):
        self.own, self.into = own, into
        self.sent, self.got, self.passed, self.heard = sent, got, passed, heard
        me = me_index()
        self.core, self.chip = lax.rem(me, 2), me // 2
        self.partner = me + 1 - 2 * self.core

    def across(self, k):
        j = lax.rem(self.chip + k * CHIP_STRIDE, CHIPS)
        return remote(
            self.own, self.into.at[self.core, self.chip], self.sent, self.got, 2 * j + self.core
        )

    def all_across(self):
        blocks = self.into.at[self.core, pl.ds(0, CHIPS - 1)]
        return remote(blocks, blocks, self.sent, self.got, self.partner)

    def handed(self, core):
        half = self.into.at[core]
        return remote(half, half, self.passed, self.heard, self.partner)

    def start(self):
        self.into[self.core, self.chip] = self.own[...]
        loop(CHIPS, lambda k: self.across(k).start(), 1)

    def hand_on(self):
        self.all_across().wait_recv()
        self.handed(self.core).start()

    def finish(self):
        self.handed(1 - self.core).wait_recv()

    def close(self):
        self.all_across().wait_send()
        self.handed(self.core).wait_send()


def ln1(v):
    centred = v - jnp.mean(v, axis=1, keepdims=True)
    factor = lax.rsqrt(jnp.mean(centred * centred, axis=1, keepdims=True) + EPSILON)
    return centred * factor, factor


def strided(ref, start, size, stride):
    return ref[pl.ds(start, size, stride=stride), :]


def packed(flat, lo, hi):
    return lambda d: strided(flat, lo * PITCH + d, hi - lo, PITCH).astype(BF16)


def widen_into(wide, into, lo, hi, pitch):
    def use(s):
        at = pl.multiple_of(s * pitch + lo, 8)
        wide[pl.ds(at, hi - lo), :] = into[s, pl.ds(lo, hi - lo)].astype(F32)

    return use


def lanes_of(t):
    return pl.ds(pl.multiple_of(t * TILE, TILE), TILE)


def row_lanes(r):
    return slice(r * RES, (r + 1) * RES)


def pair_lanes(p):
    return pl.ds(pl.multiple_of(p * 128, 128), 128)


def scatter_hidden(flat, value, piece, t):
    for q in range(TILE // 128):
        at = pl.multiple_of((piece * GROUPS + t * (TILE // 128) + q) * PITCH, 8)
        flat[pl.ds(at, N), :] = value[:, q * 128 : (q + 1) * 128]


def gather_hidden(wide, pitch, bases, t):
    parts = []
    for base in bases:
        row = [
            strided(wide, base + t * (TILE // 128) + q, N, pitch) for q in range(TILE // 128)
        ]
        parts.append(jnp.concatenate(row, axis=1))
    return jnp.concatenate(parts, axis=0)


def scatter_rows(flat, value, piece):
    for r in range(ROWS):
        for jg in range(3):
            at = (piece * GROUPS + r * 3 + jg) * PITCH
            flat[at : at + N, :] = value[r * N : (r + 1) * N, jg * 128 : (jg + 1) * 128]


def gather_matrix(out, wide, pitch, base):
    for r in range(ROWS):
        for jg in range(3):
            out[r * N : (r + 1) * N, jg * 128 : (jg + 1) * 128] = strided(
                wide, base + r * 3 + jg, N, pitch
            ).astype(BF16)


def prepare(w, p_ref, f_ref):
    order = hidden_order()
    for b in range(4):
        block = p_ref[:, b * CH : (b + 1) * CH]
        turned = nt(order, block).astype(BF16)
        for m in range(2):
            w.turned[m, b * N : (b + 1) * N, :] = turned[m * N : (m + 1) * N]
        w.straight[:, b * CH : (b + 1) * CH] = nt(block, order).astype(BF16)
    w.gate[...] = nt(identity(CH), p_ref[:, 4 * CH :]).astype(BF16)
    w.straight[:, 4 * CH :] = p_ref[:, 4 * CH :]
    w.final[...] = nn(order, f_ref[...]).astype(BF16)
    w.final_turned[...] = nt(identity(CH), w.final[...]).astype(BF16)


class Update:
    def __init__(self, c, u, w, outgoing, sums_at):
        self.c, self.u, self.w, self.outgoing, self.sums_at = c, u, w, outgoing, sums_at
        plan = (
            ("ops_a", c.out_two, u.in_ops, 0, 40),
            ("ops_b", c.out_two, u.in_ops, 40, 72),
            ("tri_a", c.out_one, u.in_tri, 0, 16),
            ("tri_b", c.out_one, u.in_tri, 16, 40),
            ("grad_a", c.out_one, u.in_grad, 0, 24),
            ("grad_b", c.out_one, u.in_grad, 24, 40),
            ("back_a", c.out_two, u.in_back, 0, 32),
            ("back_b", c.out_two, u.in_back, 32, 72),
        )
        for i, (name, out, into, lo, hi) in enumerate(plan):
            setattr(self, name, Exchange(out, into, u.sent[i], u.got[i], lo, hi))

    def gated(self, m, t, norm=None):
        norm = self.u.norm[:, lanes_of(t)] if norm is None else norm
        pre = nn(self.w.turned[m], norm)
        flat = self.c.flat
        scatter_hidden(flat, sigmoid(pre[:N]) * pre[N : 2 * N], 2 * m, t)
        scatter_hidden(flat, sigmoid(pre[2 * N : 3 * N]) * pre[3 * N :], 2 * m + 1, t)

    def enter(self, t, x):
        norm = ln0(x)[0].astype(BF16)
        self.u.norm[:, lanes_of(t)] = norm
        self.gated(0, t, norm)

    def gates(self, t):
        at = lanes_of(t)
        self.u.gate[:, at] = sigmoid(nn(self.w.gate[...], self.u.norm[:, at]))

    def arrived(self, t):
        tri = gather_hidden(self.c.wide, 40, (0, GROUPS), t)
        hatted, factor = ln0(tri)
        unit = hatted.astype(BF16)
        return tri, hatted, factor, unit, nn(self.w.final_turned[...], unit)

    def descend(self, t, gz, hatted, factor, unit, values):
        c, at = self.c, lanes_of(t)
        gate = self.u.gate[:, at]
        scaled_wide = gz * gate
        scaled = scaled_wide.astype(BF16)
        c.unit[:, at] = unit
        c.scaled[:, at] = scaled
        c.grad_proj[4 * CH :, at] = (scaled_wide * values * (1.0 - gate)).astype(BF16)
        grad = ln0_adjoint(hatted, factor, nn(self.w.final[...], scaled))
        for m in range(2):
            scatter_hidden(c.flat_one, grad[m * N : (m + 1) * N], m, t)

    def coefficients(self, t):
        c, at = self.c, lanes_of(t)
        norm = self.u.norm[:, at]
        for m in range(2):
            pre = nn(self.w.turned[m], norm)
            for side in range(2):
                opened = sigmoid(pre[2 * side * N : (2 * side + 1) * N])
                slope = pre[(2 * side + 1) * N : (2 * side + 2) * N] * opened * (1.0 - opened)
                rows = 2 * side * CH + m * N
                c.coef[rows : rows + N, at] = slope
                c.coef[rows + CH : rows + CH + N, at] = opened

    def returned(self, t, x, gz):
        c, at = self.c, lanes_of(t)
        for side in range(2):
            base = 2 * side * CH
            grad = gather_hidden(c.wide, 72, (side * GROUPS, (2 + side) * GROUPS), t)
            for half in range(2):
                rows = pl.ds(base + half * CH, CH)
                c.grad_proj[rows, at] = (grad * c.coef[rows, at]).astype(BF16)
        grad_norm = nn(self.w.straight[...], c.grad_proj[:, at])
        hatted, factor = ln0(x)
        return gz + ln0_adjoint(hatted, factor, grad_norm)

    def keep_sum(self, block, value):
        at = self.sums_at + block * CH
        self.c.mine[at : at + CH, :] = value

    def early_sums(self):
        self.keep_sum(5, nt(self.c.unit[...], self.c.scaled[...]))
        self.keep_sum(4, nt(self.u.norm[...], self.c.grad_proj[4 * CH :, :]))

    def late_sums(self):
        for b in range(4):
            self.keep_sum(b, nt(self.u.norm[...], self.c.grad_proj[b * CH : (b + 1) * CH, :]))

    def forward(self):
        c, u = self.c, self.u
        tiles(lambda t: self.gated(1, t), 2, 0, 2)
        self.ops_a.pack_and_send(packed(c.flat, 0, 40))
        tiles(lambda t: self.gated(1, t), TILES, 2)
        self.ops_b.pack_and_send(packed(c.flat, 40, 72))
        tiles(self.gates)
        for m in range(2):
            if m == 0:
                self.ops_a.receive(widen_into(c.wide, u.in_ops, 0, 40, 72))
            else:
                self.ops_b.receive(widen_into(c.wide, u.in_ops, 40, 72, 72))
            for op in range(2):
                gather_matrix(u.kept.at[2 * op + m], c.wide, 72, (2 * m + op) * GROUPS)
            left, right = u.kept[m], u.kept[2 + m]
            product = nt(left, right) if self.outgoing else nn(left.T, right)
            scatter_rows(c.flat_one, product, m)
            if m == 0:
                self.tri_a.pack_and_send(packed(c.flat_one, 0, 16))
            else:
                self.tri_b.pack_and_send(packed(c.flat_one, 16, 40))
        self.ops_a.close()
        self.ops_b.close()
        self.tri_a.receive(widen_into(c.wide, u.in_tri, 0, 16, 40))
        self.tri_b.receive(widen_into(c.wide, u.in_tri, 16, 40, 40))
        self.tri_a.close()
        self.tri_b.close()

    def backward(self, between):
        c, u = self.c, self.u
        self.grad_a.pack_and_send(packed(c.flat_one, 0, 24))
        self.grad_b.pack_and_send(packed(c.flat_one, 24, 40))
        between()
        tiles(self.coefficients)
        self.early_sums()
        for m in range(2):
            if m == 0:
                self.grad_a.receive(widen_into(c.wide, u.in_grad, 0, 24, 40))
            else:
                self.grad_b.receive(widen_into(c.wide, u.in_grad, 24, 40, 40))
            gather_matrix(c.grad_m, c.wide, 40, m * GROUPS)
            grad = c.grad_m[...]
            left, right = u.kept[m], u.kept[2 + m]
            if self.outgoing:
                grad_left, grad_right = nn(grad, right), nn(grad.T, left)
            else:
                grad_left, grad_right = nt(right, grad), nn(left, grad)
            scatter_rows(c.flat, grad_left, 2 * m)
            scatter_rows(c.flat, grad_right, 2 * m + 1)
            if m == 0:
                self.back_a.pack_and_send(packed(c.flat, 0, 32))
            else:
                self.back_b.pack_and_send(packed(c.flat, 32, 72))
        self.grad_a.close()
        self.grad_b.close()
        self.back_a.receive(widen_into(c.wide, u.in_back, 0, 32, 72))
        self.back_b.receive(widen_into(c.wide, u.in_back, 32, 72, 72))
        self.back_a.close()
        self.back_b.close()


class Total:
    def __init__(self, mine, theirs, blocks, landed, own, full, sems_of):
        self.mine, self.theirs, self.blocks, self.landed = mine, theirs, blocks, landed
        self.own, self.half = own, theirs.shape[0]
        self.share = self.half // (N // 2)
        self.sent0, self.got0, self.sent1, self.got1, *rest = sems_of
        self.gather = Gather(own, full, *rest)

    def swap(self):
        core = lax.rem(me_index(), 2)
        other = pl.ds(pl.multiple_of((1 - core) * self.half, 8), self.half)
        return remote(
            self.mine.at[other], self.theirs, self.sent0, self.got0, self.gather.partner
        )

    def to(self, k):
        g = self.gather
        j = lax.rem(g.chip + k * CHIP_STRIDE, CHIPS)
        return remote(
            self.blocks.at[j], self.landed.at[g.chip], self.sent1, self.got1, 2 * j + g.core
        )

    def all_others(self):
        others = pl.ds(0, CHIPS - 1)
        return remote(
            self.blocks.at[others], self.landed.at[others], self.sent1, self.got1,
            self.gather.partner,
        )

    def scatter(self):
        g = self.gather
        self.swap().wait_recv()
        mine = self.mine[pl.ds(pl.multiple_of(g.core * self.half, 8), self.half), :]
        for j in range(CHIPS):
            at = slice(j * self.share, (j + 1) * self.share)
            self.blocks[j] = (mine[at] + self.theirs[at, :]).astype(self.blocks.dtype)
        loop(CHIPS, lambda k: self.to(k).start(), 1)
        self.landed[g.chip] = self.blocks[g.chip]

    def spread(self):
        self.all_others().wait_recv()
        total = self.landed[0].astype(F32)
        for j in range(1, CHIPS):
            total = total + self.landed[j].astype(F32)
        self.own[...] = (total * (1.0 / RES)).astype(self.own.dtype)
        self.gather.start()

    def close(self):
        self.swap().wait_send()
        self.all_others().wait_send()
        self.gather.close()


def spread_out(all_ref, wide, into):
    def widen(s):
        wide[pl.ds(pl.multiple_of(s * 104, 8), 96), :] = into[lax.rem(s, 2), s // 2].astype(F32)

    tiles(widen, N, 0, 4)
    for r in range(ROWS):
        for p in range(PAIRS):
            all_ref[r * N : (r + 1) * N, p * 128 : (p + 1) * 128] = strided(
                wide, r * PAIRS + p, N, 104
            ).astype(BF16)


def cells_of(c, ref, out):
    for r in range(ROWS):
        c.cells_wide[:RES, :] = ref[row_lanes(r), :].astype(F32)
        parts = [strided(c.cells_wide, q, N, ROWS) for q in range(ROWS)]
        out[:, row_lanes(r)] = jnp.concatenate(parts, 0).T.astype(BF16)


def outer_sums(c, weights, of_row, all_ref, acc, by_rows):
    for r in range(ROWS):
        block = (nt if by_rows else nn)(weights[...], of_row(r))
        for p in range(PAIRS):
            c.outer_grad[p, r * 64 : (r + 1) * 64, :] = block[p * 64 : (p + 1) * 64].astype(BF16)
    acc[...] = jnp.zeros_like(acc)

    def add(b):
        part = None
        for k in range(4):
            here = nn(c.outer_grad[4 * b + k], all_ref[:, pair_lanes(4 * b + k)])
            part = here if part is None else part + here
        acc[...] += part

    loop(PAIRS // 4, add)


def matched(acc, r):
    return acc[r * 64 : r * 64 + 32, :] + pltpu.roll(acc[r * 64 + 32 : (r + 1) * 64, :], 64, 1)


def whole_kernel(names, *refs):
    c = SimpleNamespace(**dict(zip(names, refs)))
    greet()
    phases = []
    for kind in ("out", "in"):
        part = lambda name: getattr(c, name + "_" + kind)
        phases.append(
            SimpleNamespace(
                norm=part("norm"), gate=part("gate"), tri=part("tri"), kept=part("kept"),
                in_ops=part("in_ops"), in_tri=part("in_tri"),
                in_grad=part("in_grad"), in_back=part("in_back"),
                sent=[part("sent%d" % i) for i in range(8)],
                got=[part("got%d" % i) for i in range(8)],
                weights=SimpleNamespace(
                    turned=part("turned"), straight=part("straight"), gate=part("w_gate"),
                    final=part("final"), final_turned=part("final_turned"),
                ),
            )
        )
    out, into = phases

    flank_turned = c.flank[...]
    split = lambda first: one_hot(
        HIDDEN, 2 * HIDDEN, lambda r: first + jnp.where(r < PAIRS, 2 * r, 2 * r - (HIDDEN - 1))
    )
    split_left = nn(split(0), flank_turned).astype(BF16)
    split_right = nn(split(HIDDEN), flank_turned).astype(BF16)
    plain_left = flank_turned[:HIDDEN]
    none = jnp.zeros((SEQ, FEATURES), BF16)
    for r in range(ROWS):
        hatted, _ = ln1(c.alignment[r].astype(F32))
        norm = hatted.astype(BF16)
        halves = (jnp.concatenate([norm, none], 0), jnp.concatenate([none, norm], 0))
        here = pl.ds(r * PAIRS, PAIRS)
        for block, weights in ((c.own_right, split_right), (c.own_left, split_left)):
            block[here, :] = (
                nt(weights[:PAIRS], halves[0]) + nt(weights[PAIRS:], halves[1])
            ).astype(BF16)
        for h in range(2):
            at = (2 * r + h) * HIDDEN
            c.own_outer[at : at + HIDDEN, :] = nt(plain_left, halves[h]).astype(BF16)
    all_here()
    right = Gather(c.own_right, c.in_right, c.sent_r, c.got_r, c.pass_r, c.heard_r)
    left = Gather(c.own_left, c.in_left, c.sent_l, c.got_l, c.pass_l, c.heard_l)
    right.start()
    cells_of(c, c.edge, c.x_one)
    cells_of(c, c.seed, c.seed_cells)
    prepare(out.weights, c.p_out, c.f_out)
    prepare(into.weights, c.p_in, c.f_in)
    c.fin_wide[...] = c.fin[...].astype(F32)
    for d in range(HIDDEN):
        c.fin_split[d * HIDDEN : (d + 1) * HIDDEN, :] = strided(
            c.fin_wide, d, HIDDEN, HIDDEN
        ).astype(BF16)
    c.fin_turned[...] = nt(identity(CH), c.fin_split[...]).astype(BF16)
    c.flat_one[2 * GROUPS * PITCH :, :] = jnp.zeros((4 * PITCH, 128), F32)
    right.hand_on()
    right.finish()
    spread_out(c.right_all, c.wide, c.in_right)

    def outer_pair(p):
        block = nt(c.own_outer[...], c.right_all[:, pair_lanes(p)]) * (1.0 / SEQ)
        for r in range(ROWS):
            c.outer[r, pl.ds(pl.multiple_of(p * 64, 64), 64), :] = block[
                r * 64 : (r + 1) * 64
            ].astype(BF16)

    tiles(outer_pair, PAIRS, 0, 4)
    for r in range(ROWS):
        at = row_lanes(r)
        c.x_one[:, at] = (c.x_one[:, at].astype(F32) + nn(c.fin_turned[...], c.outer[r])).astype(
            BF16
        )
    right.close()

    one = Update(c, out, out.weights, True, 1024)
    two = Update(c, into, into.weights, False, 1792)
    tiles(lambda t: one.enter(t, c.x_one[:, lanes_of(t)].astype(F32)))
    one.forward()

    def between_updates(t):
        at = lanes_of(t)
        tri, _, _, _, values = one.arrived(t)
        out.tri[:, at] = tri.astype(BF16)
        new = (c.x_one[:, at].astype(F32) + out.gate[:, at] * values).astype(BF16)
        c.x_two[:, at] = new
        two.enter(t, new.astype(F32))

    tiles(between_updates)
    two.forward()
    left.start()

    def turn_round(t):
        at = lanes_of(t)
        _, hatted, factor, unit, values = two.arrived(t)
        c.new_cells[:, at] = (
            c.x_two[:, at].astype(F32) + into.gate[:, at] * values
        ).astype(BF16)
        two.descend(t, c.seed_cells[:, at].astype(F32), hatted, factor, unit, values)

    tiles(turn_round)
    two.backward(left.hand_on)

    def between_backs(t):
        at = lanes_of(t)
        grad = two.returned(t, c.x_two[:, at].astype(F32), c.seed_cells[:, at].astype(F32))
        c.grad_two[:, at] = grad
        hatted, factor = ln0(out.tri[:, at].astype(F32))
        unit = hatted.astype(BF16)
        one.descend(t, grad, hatted, factor, unit, nn(out.weights.final_turned[...], unit))

    tiles(between_backs)

    def meanwhile():
        two.late_sums()
        left.finish()
        left.close()

    one.backward(meanwhile)

    def last(t):
        at = lanes_of(t)
        c.adjoint[:, at] = one.returned(
            t, c.x_one[:, at].astype(F32), c.grad_two[:, at]
        ).astype(BF16)

    tiles(last)

    for r in range(ROWS):
        turned = c.adjoint[:, row_lanes(r)].astype(F32).T
        for q in range(ROWS):
            at = (r * ROWS + q) * PITCH
            c.flat_one[at : at + N, :] = turned[q * N : (q + 1) * N]
    pair = Exchange(c.out_one, c.in_pair, c.sent_p, c.got_p, 0, 40)
    pair.pack_and_send(packed(c.flat_one, 0, 40))
    one.late_sums()
    total = None
    for r in range(ROWS):
        part = nt(c.outer[r], c.adjoint[:, row_lanes(r)])
        total = part if total is None else total + part
    c.fin_wide[...] = total
    for k in range(HIDDEN):
        c.mine[k * HIDDEN : (k + 1) * HIDDEN, :] = strided(c.fin_wide, k, HIDDEN, HIDDEN)
    large = Total(
        c.mine, c.theirs, c.blocks, c.landed, c.own_sum, c.full,
        (c.swap_a0, c.swap_a1, c.sent_a, c.got_a, c.sent_ag, c.got_ag, c.pass_ag, c.heard_ag),
    )
    small = Total(
        c.flank_sum, c.flank_theirs, c.flank_blocks, c.flank_landed, c.flank_own, c.flank_full,
        (c.swap_b0, c.swap_b1, c.sent_b, c.got_b, c.sent_bg, c.got_bg, c.pass_bg, c.heard_bg),
    )
    large.swap().start()
    spread_out(c.left_all, c.wide, c.in_left)
    large.scatter()
    outer_sums(
        c, c.fin_split, lambda r: c.adjoint[:, row_lanes(r)], c.right_all, c.acc_left, False
    )
    pair.receive(widen_into(c.wide, c.in_pair, 0, 40, 40))
    for q in range(ROWS):
        for r in range(ROWS):
            c.columns[q, r * N : (r + 1) * N, :] = strided(c.wide, r * ROWS + q, N, 40).astype(
                BF16
            )
    outer_sums(c, c.fin, lambda q: c.columns[q], c.left_all, c.acc_right, True)
    lane = lax.broadcasted_iota(jnp.int32, (2 * HIDDEN, 2 * SEQ), 1)
    flank_sum = jnp.zeros((2 * HIDDEN, FEATURES), F32)
    grads = []
    for r in range(ROWS):
        both = jnp.concatenate([matched(c.acc_left, r), matched(c.acc_right, r)], 0)
        both = jnp.where(lane < SEQ, both * (1.0 / SEQ), 0.0)
        c.flank_grad[r] = both
        hatted, _ = ln1(c.alignment[r].astype(F32))
        norm = jnp.concatenate([hatted.astype(BF16), none], 0)
        flank_sum = flank_sum + nn(both.astype(BF16), norm)
    c.flank_sum[: 2 * HIDDEN, :] = flank_sum[:, :128]
    c.flank_sum[2 * HIDDEN :, :] = flank_sum[:, 128:]
    small.swap().start()
    large.spread()
    small.scatter()
    for r in range(ROWS):
        grad = nn(c.flank_grad[r].T[:SEQ].astype(BF16), flank_turned)
        hatted, factor = ln1(c.alignment[r].astype(F32))
        c.align_grad[r] = (
            factor
            * (
                grad
                - jnp.mean(grad, axis=1, keepdims=True)
                - hatted * jnp.mean(grad * hatted, axis=1, keepdims=True)
            )
        ).astype(BF16)
    small.spread()
    pair.close()
    large.gather.hand_on()
    small.gather.hand_on()
    large.gather.finish()
    small.gather.finish()
    large.close()
    small.close()


def vmem(count):
    return [pl.BlockSpec(memory_space=pltpu.VMEM)] * count


def shaped(shape, dtype):
    return jax.ShapeDtypeStruct(shape, dtype)


INPUTS = ("edge", "alignment", "flank", "fin", "p_out", "f_out", "p_in", "f_in", "seed")
OUTPUTS = dict(
    new_cells=((CH, CELLS), BF16),
    adjoint=((CH, CELLS), BF16),
    align_grad=((ROWS, SEQ, FEATURES), BF16),
    full=((2, CHIPS, 40, 128), BF16),
    flank_full=((2, CHIPS, 2, 128), F32),
)


def scratch():
    shapes = dict(
        x_one=((CH, CELLS), BF16),
        x_two=((CH, CELLS), BF16),
        seed_cells=((CH, CELLS), BF16),
        grad_two=((CH, CELLS), F32),
        flat=((72 * PITCH, 128), F32),
        flat_one=((40 * PITCH, 128), F32),
        wide=((104 * N, 128), F32),
        out_two=((N, 72, 128), BF16),
        out_one=((N, 40, 128), BF16),
        unit=((CH, CELLS), BF16),
        scaled=((CH, CELLS), BF16),
        coef=((4 * CH, CELLS), F32),
        grad_proj=((5 * CH, CELLS), BF16),
        grad_m=((RES, RES), BF16),
        mine=((2560, 128), F32),
        theirs=((1280, 128), F32),
        blocks=((CHIPS, 40, 128), BF16),
        landed=((CHIPS, 40, 128), BF16),
        own_sum=((40, 128), BF16),
        flank_sum=((128, 128), F32),
        flank_theirs=((64, 128), F32),
        flank_blocks=((N // 2, 2, 128), F32),
        flank_landed=((N // 2, 2, 128), F32),
        flank_own=((2, 128), F32),
        flank_grad=((ROWS, 2 * HIDDEN, 128), F32),
        own_right=((96, 128), BF16),
        own_left=((96, 128), BF16),
        own_outer=((2 * ROWS * HIDDEN, 2 * SEQ), BF16),
        in_right=((2, CHIPS, 96, 128), BF16),
        in_left=((2, CHIPS, 96, 128), BF16),
        right_all=((RES, HIDDEN * SEQ), BF16),
        left_all=((RES, HIDDEN * SEQ), BF16),
        cells_wide=((RES, 128), F32),
        fin_wide=((HIDDEN * HIDDEN, CH), F32),
        fin_split=((HIDDEN * HIDDEN, CH), BF16),
        fin_turned=((CH, HIDDEN * HIDDEN), BF16),
        outer=((ROWS, HIDDEN * HIDDEN, RES), BF16),
        outer_grad=((PAIRS, RES, RES), BF16),
        acc_left=((RES, 128), F32),
        acc_right=((RES, 128), F32),
        columns=((ROWS, RES, CH), BF16),
        in_pair=((N, 40, 128), BF16),
    )
    each = dict(
        norm=((CH, CELLS), BF16),
        gate=((CH, CELLS), F32),
        tri=((CH, CELLS), BF16),
        kept=((4, RES, RES), BF16),
        in_ops=((N, 72, 128), BF16),
        in_tri=((N, 40, 128), BF16),
        in_grad=((N, 40, 128), BF16),
        in_back=((N, 72, 128), BF16),
        turned=((2, 4 * N, CH), BF16),
        straight=((CH, 5 * CH), BF16),
        w_gate=((CH, CH), BF16),
        final=((CH, CH), BF16),
        final_turned=((CH, CH), BF16),
    )
    for kind in ("out", "in"):
        shapes.update({name + "_" + kind: value for name, value in each.items()})
    made = {name: pltpu.VMEM(*value) for name, value in shapes.items()}
    flags = []
    for kind in ("out", "in"):
        for i in range(8):
            flags += ["sent%d_%s" % (i, kind), "got%d_%s" % (i, kind)]
    for tail in ("r", "l", "ag", "bg"):
        flags += [name + tail for name in ("sent_", "got_", "pass_", "heard_")]
    flags += ["sent_p", "got_p"]
    for tail in ("a", "b"):
        flags += ["sent_" + tail, "got_" + tail, "swap_%s0" % tail, "swap_%s1" % tail]
    made.update({name: pltpu.SemaphoreType.DMA(()) for name in flags})
    return made


def whole(*arrays):
    made = scratch()
    names = INPUTS + tuple(OUTPUTS) + tuple(made)
    return pl.pallas_call(
        lambda *refs: whole_kernel(names, *refs),
        out_shape=tuple(shaped(*value) for value in OUTPUTS.values()),
        in_specs=vmem(len(INPUTS)),
        out_specs=tuple(vmem(len(OUTPUTS))),
        scratch_shapes=list(made.values()),
        compiler_params=pltpu.CompilerParams(
            collective_id=1, has_side_effects=True, vmem_limit_bytes=67_043_328
        ),
        name="window",
    )(*arrays)


def finish_kernel(
    new_ref, adj_ref, align_ref, full_ref, flank_ref,
    new_out, adj_out, align_out, flank_out, fin_out, proj_out, final_out, proj_in, final_in,
    cells, sums, flank_rows,
):
    for ref, out in ((new_ref, new_out), (adj_ref, adj_out)):
        for r in range(ROWS):
            turned = ref[:, row_lanes(r)].astype(F32).T
            for q in range(ROWS):
                cells[pl.ds(q, N, stride=ROWS), :] = turned[q * N : (q + 1) * N]
            out[row_lanes(r), :] = cells[...].astype(BF16)
    align_out[...] = align_ref[...]
    order = hidden_order()

    def place(s):
        at = pl.multiple_of(s * 40, 8)
        sums[pl.ds(at, 40), :] = full_ref[s // CHIPS, lax.rem(s, CHIPS)].astype(F32)

    tiles(place, N, 0, 4)
    fin_out[...] = sums[:1024, :]
    for base, proj, final in ((1024, proj_out, final_out), (1792, proj_in, final_in)):
        for b in range(5):
            block = sums[base + b * CH : base + (b + 1) * CH, :]
            proj[:, b * CH : (b + 1) * CH] = nn(block.astype(BF16), order) if b < 4 else block
        block = sums[base + 5 * CH : base + 6 * CH, :]
        final[...] = nn(order.T, block.astype(BF16))
    for j in range(N // 2):
        for core in range(2):
            flank_rows[core * 64 + 2 * j : core * 64 + 2 * j + 2, :] = flank_ref[core, j]
    flank_out[:, :128] = flank_rows[:64, :]
    flank_out[:, 128:] = flank_rows[64:, :]


def shards(
    edge_embedding,
    alignment_embedding,
    tensor_flank_matrix,
    tensor_final_matrix,
    outward_sigmoid_matrix,
    outward_final_matrix,
    inward_sigmoid_matrix,
    inward_final_matrix,
    adjoint_seed,
):
    results = whole(
        edge_embedding.reshape(CELLS, CH),
        alignment_embedding.transpose(1, 0, 2),
        tensor_flank_matrix.T,
        tensor_final_matrix,
        outward_sigmoid_matrix,
        outward_final_matrix,
        inward_sigmoid_matrix,
        inward_final_matrix,
        adjoint_seed.reshape(CELLS, CH),
    )
    outs = pl.pallas_call(
        finish_kernel,
        out_shape=(
            shaped((CELLS, CH), BF16),
            shaped((CELLS, CH), BF16),
            shaped((ROWS, SEQ, FEATURES), BF16),
            shaped((2 * HIDDEN, FEATURES), F32),
            shaped((HIDDEN * HIDDEN, CH), F32),
            shaped((CH, 5 * CH), F32),
            shaped((CH, CH), F32),
            shaped((CH, 5 * CH), F32),
            shaped((CH, CH), F32),
        ),
        in_specs=vmem(5),
        out_specs=tuple(vmem(9)),
        scratch_shapes=[
            pltpu.VMEM((RES, 128), F32),
            pltpu.VMEM((2560, 128), F32),
            pltpu.VMEM((128, 128), F32),
        ],
        compiler_params=pltpu.CompilerParams(vmem_limit_bytes=VMEM_LIMIT),
        name="finish",
    )(*results)
    return (
        outs[0].reshape(ROWS, RES, CH),
        outs[1].reshape(ROWS, RES, CH),
        outs[2].transpose(1, 0, 2),
        outs[3].T,
        *outs[4:],
    )


def solution(mesh):
    placed = (
        P(("dp", "dap"), None, None),
        P("dp", "dap", None),
        P(),
        P(),
        P(),
        P(),
        P(),
        P(),
        P(("dp", "dap"), None, None),
    )
    return jax.shard_map(
        shards,
        mesh=mesh,
        in_specs=placed,
        out_specs=(
            P(("dp", "dap"), None, None),
            P(("dp", "dap"), None, None),
            P("dp", "dap", None),
            P("dp", None),
            P("dp", None),
            P("dp", None),
            P("dp", None),
            P("dp", None),
            P("dp", None),
        ),
        check_vma=False,
    )
```

```python
from types import SimpleNamespace

import jax
import jax.numpy as jnp
from jax import lax
from jax.experimental import pallas as pl
from jax.experimental.pallas import tpu as pltpu
from jax.sharding import PartitionSpec as P

EPSILON = 1e-05
F32, BF16 = jnp.float32, jnp.bfloat16
MESH = pl.DeviceIdType.MESH
N = 64
ROWS = 6
RES = 384
CELLS = ROWS * RES
CH = 128
GROUPS = CELLS // 128
PITCH = 72
HIDDEN = 32
PAIRS = HIDDEN // 2
SEQ = 64
FEATURES = 256
TILE = 256
TILES = CELLS // TILE
VMEM_LIMIT = 60 * 1024 * 1024


def nn(a, b):
    return lax.dot_general(a, b, (((1,), (0,)), ((), ())), preferred_element_type=F32)


def nt(a, b):
    return lax.dot_general(a, b, (((1,), (1,)), ((), ())), preferred_element_type=F32)


def one_hot(rows, columns, pick, dtype=BF16):
    row = lax.broadcasted_iota(jnp.int32, (rows, columns), 0)
    column = lax.broadcasted_iota(jnp.int32, (rows, columns), 1)
    return jnp.where(pick(row) == column, 1.0, 0.0).astype(dtype)


def identity(size):
    return one_hot(size, size, lambda r: r)


def hidden_order(dtype=BF16):
    return one_hot(CH, CH, lambda r: jnp.where(r < N, 2 * r, 2 * r - (CH - 1)), dtype)


def sigmoid(v):
    return 1.0 / (1.0 + jnp.exp(-v))


def ln0(v):
    centred = v - jnp.mean(v, axis=0, keepdims=True)
    factor = lax.rsqrt(jnp.mean(centred * centred, axis=0, keepdims=True) + EPSILON)
    return centred * factor, factor


def ln0_adjoint(hatted, factor, g):
    return factor * (
        g
        - jnp.mean(g, axis=0, keepdims=True)
        - hatted * jnp.mean(g * hatted, axis=0, keepdims=True)
    )


def loop(count, body, start=0):
    def step(k, carry):
        body(k)
        return carry

    lax.fori_loop(start, count, step, 0)


def me_index():
    return lax.axis_index("dap")


def greet():
    me = me_index()
    sem = pltpu.get_barrier_semaphore()
    loop(
        N,
        lambda k: pl.semaphore_signal(
            sem, inc=1, device_id={"dap": lax.rem(me + k, N)}, device_id_type=MESH
        ),
        1,
    )


def all_here():
    pl.semaphore_wait(pltpu.get_barrier_semaphore(), N - 1)


def remote(src, dst, send_sem, recv_sem, to):
    return pltpu.make_async_remote_copy(
        src_ref=src,
        dst_ref=dst,
        send_sem=send_sem,
        recv_sem=recv_sem,
        device_id={"dap": to},
        device_id_type=MESH,
    )


BATCH = 3
CHIPS = N // 2
CHIP_STRIDE = 13
STRIDE = 37


def ahead(k):
    return lax.rem(me_index() + k * STRIDE, N)


def tiles(body, stop=TILES, start=0, by=3):
    def step(b):
        for k in range(by):
            body(start + by * b + k)

    loop((stop - start) // by, step)
    for t in range(start + (stop - start) // by * by, stop):
        body(t)


class Exchange:
    def __init__(self, out, into, sent, got, lo, hi):
        self.out, self.into, self.sent, self.got = out, into, sent, got
        self.rows = pl.ds(lo, hi - lo)

    def copy(self, d, at):
        return remote(
            self.out.at[d, self.rows], self.into.at[at, self.rows], self.sent, self.got, d
        )

    def pack_and_send(self, rows_of):
        me = me_index()
        self.into[me, self.rows] = rows_of(me)

        def pack(first):
            for k in range(BATCH):
                d = ahead(first + k)
                self.out[d, self.rows] = rows_of(d)

        def send(first):
            for k in range(BATCH):
                self.copy(ahead(first + k), me).start()

        pack(1)

        def step(b):
            pack(1 + BATCH * b)
            send(1 + BATCH * (b - 1))

        loop((N - 1) // BATCH, step, 1)
        send(N - BATCH)

    def send_all(self):
        me = me_index()
        self.into[me, self.rows] = self.out[me, self.rows]
        loop(N, lambda k: self.copy(ahead(k), me).start(), 1)

    def all_others(self):
        others = pl.ds(0, N - 1)
        return remote(
            self.out.at[others, self.rows], self.into.at[others, self.rows],
            self.sent, self.got, ahead(1),
        )

    def receive(self, use):
        self.all_others().wait_recv()
        tiles(use, N, 0, 4)

    def close(self):
        self.all_others().wait_send()


class Gather:
    def __init__(self, own, into, sent, got, passed, heard):
        self.own, self.into = own, into
        self.sent, self.got, self.passed, self.heard = sent, got, passed, heard
        me = me_index()
        self.core, self.chip = lax.rem(me, 2), me // 2
        self.partner = me + 1 - 2 * self.core

    def across(self, k):
        j = lax.rem(self.chip + k * CHIP_STRIDE, CHIPS)
        return remote(
            self.own, self.into.at[self.core, self.chip], self.sent, self.got, 2 * j + self.core
        )

    def all_across(self):
        blocks = self.into.at[self.core, pl.ds(0, CHIPS - 1)]
        return remote(blocks, blocks, self.sent, self.got, self.partner)

    def handed(self, core):
        half = self.into.at[core]
        return remote(half, half, self.passed, self.heard, self.partner)

    def start(self):
        self.into[self.core, self.chip] = self.own[...]
        loop(CHIPS, lambda k: self.across(k).start(), 1)

    def hand_on(self):
        self.all_across().wait_recv()
        self.handed(self.core).start()

    def finish(self):
        self.handed(1 - self.core).wait_recv()

    def close(self):
        self.all_across().wait_send()
        self.handed(self.core).wait_send()


def ln1(v):
    centred = v - jnp.mean(v, axis=1, keepdims=True)
    factor = lax.rsqrt(jnp.mean(centred * centred, axis=1, keepdims=True) + EPSILON)
    return centred * factor, factor


def strided(ref, start, size, stride):
    return ref[pl.ds(start, size, stride=stride), :]


def packed(flat, lo, hi):
    return lambda d: strided(flat, lo * PITCH + d, hi - lo, PITCH).astype(BF16)


def widen_into(wide, into, lo, hi, pitch):
    def use(s):
        at = pl.multiple_of(s * pitch + lo, 8)
        wide[pl.ds(at, hi - lo), :] = into[s, pl.ds(lo, hi - lo)].astype(F32)

    return use


def lanes_of(t):
    return pl.ds(pl.multiple_of(t * TILE, TILE), TILE)


def row_lanes(r):
    return slice(r * RES, (r + 1) * RES)


def pair_lanes(p):
    return pl.ds(pl.multiple_of(p * 128, 128), 128)


def scatter_hidden(flat, value, piece, t):
    for q in range(TILE // 128):
        at = pl.multiple_of((piece * GROUPS + t * (TILE // 128) + q) * PITCH, 8)
        flat[pl.ds(at, N), :] = value[:, q * 128 : (q + 1) * 128]


def gather_hidden(wide, pitch, bases, t):
    parts = []
    for base in bases:
        row = [
            strided(wide, base + t * (TILE // 128) + q, N, pitch) for q in range(TILE // 128)
        ]
        parts.append(jnp.concatenate(row, axis=1))
    return jnp.concatenate(parts, axis=0)


def scatter_rows(flat, value, piece):
    for r in range(ROWS):
        for jg in range(3):
            at = (piece * GROUPS + r * 3 + jg) * PITCH
            flat[at : at + N, :] = value[r * N : (r + 1) * N, jg * 128 : (jg + 1) * 128]


def gather_matrix(out, wide, pitch, base):
    for r in range(ROWS):
        for jg in range(3):
            out[r * N : (r + 1) * N, jg * 128 : (jg + 1) * 128] = strided(
                wide, base + r * 3 + jg, N, pitch
            ).astype(BF16)


def prepare(w, p_ref, f_ref):
    order = hidden_order()
    for b in range(4):
        block = p_ref[:, b * CH : (b + 1) * CH]
        turned = nt(order, block).astype(BF16)
        for m in range(2):
            w.turned[m, b * N : (b + 1) * N, :] = turned[m * N : (m + 1) * N]
        w.straight[:, b * CH : (b + 1) * CH] = nt(block, order).astype(BF16)
    w.gate[...] = nt(identity(CH), p_ref[:, 4 * CH :]).astype(BF16)
    w.straight[:, 4 * CH :] = p_ref[:, 4 * CH :]
    w.final[...] = nn(order, f_ref[...]).astype(BF16)
    w.final_turned[...] = nt(identity(CH), w.final[...]).astype(BF16)


class Update:
    def __init__(self, c, u, w, outgoing, sums_at):
        self.c, self.u, self.w, self.outgoing, self.sums_at = c, u, w, outgoing, sums_at
        plan = (
            ("ops_a", c.out_two, u.in_ops, 0, 40),
            ("ops_b", c.out_two, u.in_ops, 40, 72),
            ("tri_a", c.out_one, u.in_tri, 0, 16),
            ("tri_b", c.out_one, u.in_tri, 16, 40),
            ("grad_a", c.out_one, u.in_grad, 0, 24),
            ("grad_b", c.out_one, u.in_grad, 24, 40),
            ("back_a", c.out_two, u.in_back, 0, 32),
            ("back_b", c.out_two, u.in_back, 32, 72),
        )
        for i, (name, out, into, lo, hi) in enumerate(plan):
            setattr(self, name, Exchange(out, into, u.sent[i], u.got[i], lo, hi))

    def gated(self, m, t, norm=None):
        norm = self.u.norm[:, lanes_of(t)] if norm is None else norm
        pre = nn(self.w.turned[m], norm)
        flat = self.c.flat
        scatter_hidden(flat, sigmoid(pre[:N]) * pre[N : 2 * N], 2 * m, t)
        scatter_hidden(flat, sigmoid(pre[2 * N : 3 * N]) * pre[3 * N :], 2 * m + 1, t)

    def enter(self, t, x):
        norm = ln0(x)[0].astype(BF16)
        self.u.norm[:, lanes_of(t)] = norm
        self.gated(0, t, norm)

    def gates(self, t):
        at = lanes_of(t)
        self.u.gate[:, at] = sigmoid(nn(self.w.gate[...], self.u.norm[:, at]))

    def arrived(self, t):
        tri = gather_hidden(self.c.wide, 40, (0, GROUPS), t)
        hatted, factor = ln0(tri)
        unit = hatted.astype(BF16)
        return tri, hatted, factor, unit, nn(self.w.final_turned[...], unit)

    def descend(self, t, gz, hatted, factor, unit, values):
        c, at = self.c, lanes_of(t)
        gate = self.u.gate[:, at]
        scaled_wide = gz * gate
        scaled = scaled_wide.astype(BF16)
        c.unit[:, at] = unit
        c.scaled[:, at] = scaled
        c.grad_proj[4 * CH :, at] = (scaled_wide * values * (1.0 - gate)).astype(BF16)
        grad = ln0_adjoint(hatted, factor, nn(self.w.final[...], scaled))
        for m in range(2):
            scatter_hidden(c.flat_one, grad[m * N : (m + 1) * N], m, t)

    def coefficients(self, t):
        c, at = self.c, lanes_of(t)
        norm = self.u.norm[:, at]
        for m in range(2):
            pre = nn(self.w.turned[m], norm)
            for side in range(2):
                opened = sigmoid(pre[2 * side * N : (2 * side + 1) * N])
                slope = pre[(2 * side + 1) * N : (2 * side + 2) * N] * opened * (1.0 - opened)
                rows = 2 * side * CH + m * N
                c.coef[rows : rows + N, at] = slope
                c.coef[rows + CH : rows + CH + N, at] = opened

    def returned(self, t, x, gz):
        c, at = self.c, lanes_of(t)
        for side in range(2):
            base = 2 * side * CH
            grad = gather_hidden(c.wide, 72, (side * GROUPS, (2 + side) * GROUPS), t)
            for half in range(2):
                rows = pl.ds(base + half * CH, CH)
                c.grad_proj[rows, at] = (grad * c.coef[rows, at]).astype(BF16)
        grad_norm = nn(self.w.straight[...], c.grad_proj[:, at])
        hatted, factor = ln0(x)
        return gz + ln0_adjoint(hatted, factor, grad_norm)

    def keep_sum(self, block, value):
        at = self.sums_at + block * CH
        self.c.mine[at : at + CH, :] = value

    def early_sums(self):
        self.keep_sum(5, nt(self.c.unit[...], self.c.scaled[...]))
        self.keep_sum(4, nt(self.u.norm[...], self.c.grad_proj[4 * CH :, :]))

    def late_sums(self):
        for b in range(4):
            self.keep_sum(b, nt(self.u.norm[...], self.c.grad_proj[b * CH : (b + 1) * CH, :]))

    def forward(self, between):
        c, u = self.c, self.u
        tiles(lambda t: self.gated(1, t), 2, 0, 2)
        self.ops_a.pack_and_send(packed(c.flat, 0, 40))
        tiles(lambda t: self.gated(1, t), TILES, 2)
        self.ops_b.pack_and_send(packed(c.flat, 40, 72))
        between()
        tiles(self.gates)
        for m in range(2):
            if m == 0:
                self.ops_a.receive(widen_into(c.wide, u.in_ops, 0, 40, 72))
            else:
                self.ops_b.receive(widen_into(c.wide, u.in_ops, 40, 72, 72))
            for op in range(2):
                gather_matrix(u.kept.at[2 * op + m], c.wide, 72, (2 * m + op) * GROUPS)
            left, right = u.kept[m], u.kept[2 + m]
            product = nt(left, right) if self.outgoing else nn(left.T, right)
            scatter_rows(c.flat_one, product, m)
            if m == 0:
                self.tri_a.pack_and_send(packed(c.flat_one, 0, 16))
            else:
                self.tri_b.pack_and_send(packed(c.flat_one, 16, 40))
        self.ops_a.close()
        self.ops_b.close()
        self.tri_a.receive(widen_into(c.wide, u.in_tri, 0, 16, 40))
        self.tri_b.receive(widen_into(c.wide, u.in_tri, 16, 40, 40))
        self.tri_a.close()
        self.tri_b.close()

    def backward(self, between):
        c, u = self.c, self.u
        self.grad_a.pack_and_send(packed(c.flat_one, 0, 24))
        self.grad_b.pack_and_send(packed(c.flat_one, 24, 40))
        between()
        tiles(self.coefficients)
        self.early_sums()
        for m in range(2):
            if m == 0:
                self.grad_a.receive(widen_into(c.wide, u.in_grad, 0, 24, 40))
            else:
                self.grad_b.receive(widen_into(c.wide, u.in_grad, 24, 40, 40))
            gather_matrix(c.grad_m, c.wide, 40, m * GROUPS)
            grad = c.grad_m[...]
            left, right = u.kept[m], u.kept[2 + m]
            if self.outgoing:
                grad_left, grad_right = nn(grad, right), nn(grad.T, left)
            else:
                grad_left, grad_right = nt(right, grad), nn(left, grad)
            scatter_rows(c.flat, grad_left, 2 * m)
            scatter_rows(c.flat, grad_right, 2 * m + 1)
            if m == 0:
                self.back_a.pack_and_send(packed(c.flat, 0, 32))
            else:
                self.back_b.pack_and_send(packed(c.flat, 32, 72))
        self.grad_a.close()
        self.grad_b.close()
        self.back_a.receive(widen_into(c.wide, u.in_back, 0, 32, 72))
        self.back_b.receive(widen_into(c.wide, u.in_back, 32, 72, 72))
        self.back_a.close()
        self.back_b.close()


class Total:
    def __init__(self, mine, theirs, blocks, landed, own, full, sems_of):
        self.mine, self.theirs, self.blocks, self.landed = mine, theirs, blocks, landed
        self.own, self.half = own, theirs.shape[0]
        self.share = self.half // (N // 2)
        self.sent0, self.got0, self.sent1, self.got1, *rest = sems_of
        self.gather = Gather(own, full, *rest)

    def swap(self):
        core = lax.rem(me_index(), 2)
        other = pl.ds(pl.multiple_of((1 - core) * self.half, 8), self.half)
        return remote(
            self.mine.at[other], self.theirs, self.sent0, self.got0, self.gather.partner
        )

    def to(self, k):
        g = self.gather
        j = lax.rem(g.chip + k * CHIP_STRIDE, CHIPS)
        return remote(
            self.blocks.at[j], self.landed.at[g.chip], self.sent1, self.got1, 2 * j + g.core
        )

    def all_others(self):
        others = pl.ds(0, CHIPS - 1)
        return remote(
            self.blocks.at[others], self.landed.at[others], self.sent1, self.got1,
            self.gather.partner,
        )

    def scatter(self):
        g = self.gather
        self.swap().wait_recv()
        mine = self.mine[pl.ds(pl.multiple_of(g.core * self.half, 8), self.half), :]
        for j in range(CHIPS):
            at = slice(j * self.share, (j + 1) * self.share)
            self.blocks[j] = (mine[at] + self.theirs[at, :]).astype(self.blocks.dtype)
        loop(CHIPS, lambda k: self.to(k).start(), 1)
        self.landed[g.chip] = self.blocks[g.chip]

    def spread(self):
        self.all_others().wait_recv()
        total = self.landed[0].astype(F32)
        for j in range(1, CHIPS):
            total = total + self.landed[j].astype(F32)
        self.own[...] = (total * (1.0 / RES)).astype(self.own.dtype)
        self.gather.start()

    def close(self):
        self.swap().wait_send()
        self.all_others().wait_send()
        self.gather.close()


def spread_out(all_ref, wide, into, rows, placed):
    pitch = rows if rows // 8 % 2 else rows + 8

    def widen(s):
        at = pl.ds(pl.multiple_of(s * pitch, 8), rows)
        wide[at, :] = into[lax.rem(s, 2), s // 2].astype(F32)

    tiles(widen, N, 0, 4)
    for r, p, row in placed:
        all_ref[r * N : (r + 1) * N, p * 128 : (p + 1) * 128] = strided(
            wide, row, N, pitch
        ).astype(BF16)


def cells_of(c, ref, out):
    for r in range(ROWS):
        c.cells_wide[:RES, :] = ref[row_lanes(r), :].astype(F32)
        parts = [strided(c.cells_wide, q, N, ROWS) for q in range(ROWS)]
        out[:, row_lanes(r)] = jnp.concatenate(parts, 0).T.astype(BF16)


def natural(c, cells, out):
    for r in range(ROWS):
        turned = cells[:, row_lanes(r)].astype(F32).T
        for q in range(ROWS):
            c.cells_wide[pl.ds(q, N, stride=ROWS), :] = turned[q * N : (q + 1) * N]
        out[row_lanes(r), :] = c.cells_wide[...].astype(BF16)


def outer_grads(c, block, r):
    for p in range(PAIRS):
        c.outer_grad[p, r * 64 : (r + 1) * 64, :] = block[p * 64 : (p + 1) * 64].astype(BF16)


def outer_sums(c, all_ref, acc):
    acc[...] = jnp.zeros_like(acc)

    def add(b):
        part = None
        for k in range(4):
            here = nn(c.outer_grad[4 * b + k], all_ref[:, pair_lanes(4 * b + k)])
            part = here if part is None else part + here
        acc[...] += part

    loop(PAIRS // 4, add)


def matched(acc, r):
    return acc[r * 64 : r * 64 + 32, :] + pltpu.roll(acc[r * 64 + 32 : (r + 1) * 64, :], 64, 1)


def whole_kernel(names, *refs):
    c = SimpleNamespace(**dict(zip(names, refs)))
    greet()
    phases = []
    for kind in ("out", "in"):
        part = lambda name: getattr(c, name + "_" + kind)
        phases.append(
            SimpleNamespace(
                norm=part("norm"), gate=part("gate"), tri=part("tri"), kept=part("kept"),
                in_ops=part("in_ops"), in_tri=part("in_tri"),
                in_grad=part("in_grad"), in_back=part("in_back"),
                sent=[part("sent%d" % i) for i in range(8)],
                got=[part("got%d" % i) for i in range(8)],
                weights=SimpleNamespace(
                    turned=part("turned"), straight=part("straight"), gate=part("w_gate"),
                    final=part("final"), final_turned=part("final_turned"),
                ),
            )
        )
    out, into = phases

    flank_turned = c.flank[...]
    split = lambda first: one_hot(
        HIDDEN, 2 * HIDDEN, lambda r: first + jnp.where(r < PAIRS, 2 * r, 2 * r - (HIDDEN - 1))
    )
    split_left = nn(split(0), flank_turned).astype(BF16)
    split_right = nn(split(HIDDEN), flank_turned).astype(BF16)
    plain_left = flank_turned[:HIDDEN]
    none = jnp.zeros((SEQ, FEATURES), BF16)
    for r in range(ROWS):
        hatted, _ = ln1(c.alignment[r].astype(F32))
        norm = hatted.astype(BF16)
        halves = (jnp.concatenate([norm, none], 0), jnp.concatenate([none, norm], 0))
        made = [
            (nt(weights[:PAIRS], halves[0]) + nt(weights[PAIRS:], halves[1])).astype(BF16)
            for weights in (split_right, split_left)
        ]
        for h in range(2):
            c.own_right[h, r * 8 : (r + 1) * 8, :] = made[0][h * 8 : (h + 1) * 8]
        c.own_left[r // 2, (r % 2) * PAIRS : (r % 2 + 1) * PAIRS, :] = made[1]
        for h in range(2):
            at = (2 * r + h) * HIDDEN
            c.own_outer[at : at + HIDDEN, :] = nt(plain_left, halves[h]).astype(BF16)
    all_here()
    gather = lambda own, into, tail: Gather(
        own, into, *(getattr(c, name + tail) for name in ("sent_", "got_", "pass_", "heard_"))
    )
    right = [gather(c.own_right.at[h], c.in_right.at[h], "r%d" % h) for h in range(2)]
    left = [gather(c.own_left.at[h], c.in_left.at[h], "l%d" % h) for h in range(3)]
    right[0].start()
    right[1].start()
    cells_of(c, c.edge, c.x_one)
    cells_of(c, c.seed, c.seed_cells)
    prepare(out.weights, c.p_out, c.f_out)
    prepare(into.weights, c.p_in, c.f_in)
    c.fin_wide[...] = c.fin[...].astype(F32)
    for d in range(HIDDEN):
        c.fin_split[d * HIDDEN : (d + 1) * HIDDEN, :] = strided(
            c.fin_wide, d, HIDDEN, HIDDEN
        ).astype(BF16)
    c.fin_turned[...] = nt(identity(CH), c.fin_split[...]).astype(BF16)
    c.flat_one[2 * GROUPS * PITCH :, :] = jnp.zeros((4 * PITCH, 128), F32)
    def outer_pair(p):
        block = nt(c.own_outer[...], c.right_all[:, pair_lanes(p)]) * (1.0 / SEQ)
        for r in range(ROWS):
            c.outer[r, pl.ds(pl.multiple_of(p * 64, 64), 64), :] = block[
                r * 64 : (r + 1) * 64
            ].astype(BF16)

    for h in range(2):
        right[h].hand_on()
        right[h].finish()
        if h == 1:
            left[0].start()
        spread_out(
            c.right_all, c.wide, c.in_right.at[h], 48,
            [(r, 8 * h + p, r * 8 + p) for r in range(ROWS) for p in range(8)],
        )
        tiles(outer_pair, 8 * h + 8, 8 * h, 4)
    for r in range(ROWS):
        at = row_lanes(r)
        c.x_one[:, at] = (c.x_one[:, at].astype(F32) + nn(c.fin_turned[...], c.outer[r])).astype(
            BF16
        )
    right[0].close()
    right[1].close()

    one = Update(c, out, out.weights, True, 1024)
    two = Update(c, into, into.weights, False, 1792)
    tiles(lambda t: one.enter(t, c.x_one[:, lanes_of(t)].astype(F32)))
    one.forward(left[0].hand_on)
    left[1].start()

    def between_updates(t):
        at = lanes_of(t)
        tri, _, _, _, values = one.arrived(t)
        out.tri[:, at] = tri.astype(BF16)
        new = (c.x_one[:, at].astype(F32) + out.gate[:, at] * values).astype(BF16)
        c.x_two[:, at] = new
        two.enter(t, new.astype(F32))

    tiles(between_updates)
    two.forward(left[1].hand_on)
    left[2].start()

    def turn_round(t):
        at = lanes_of(t)
        _, hatted, factor, unit, values = two.arrived(t)
        c.new_cells[:, at] = (
            c.x_two[:, at].astype(F32) + into.gate[:, at] * values
        ).astype(BF16)
        two.descend(t, c.seed_cells[:, at].astype(F32), hatted, factor, unit, values)

    def after_turn():
        left[2].hand_on()
        natural(c, c.new_cells, c.new_pair)

    tiles(turn_round)
    two.backward(after_turn)

    def between_backs(t):
        at = lanes_of(t)
        grad = two.returned(t, c.x_two[:, at].astype(F32), c.seed_cells[:, at].astype(F32))
        c.grad_two[:, at] = grad
        hatted, factor = ln0(out.tri[:, at].astype(F32))
        unit = hatted.astype(BF16)
        one.descend(t, grad, hatted, factor, unit, nn(out.weights.final_turned[...], unit))

    tiles(between_backs)

    def meanwhile():
        two.late_sums()
        for h in range(3):
            left[h].finish()
            left[h].close()
            spread_out(
                c.left_all, c.wide, c.in_left.at[h], 32,
                [(2 * h + r, p, r * PAIRS + p) for r in range(2) for p in range(PAIRS)],
            )

    one.backward(meanwhile)

    def last(t):
        at = lanes_of(t)
        c.adjoint[:, at] = one.returned(
            t, c.x_one[:, at].astype(F32), c.grad_two[:, at]
        ).astype(BF16)

    tiles(last)

    for r in range(ROWS):
        turned = c.adjoint[:, row_lanes(r)].astype(F32).T
        for q in range(ROWS):
            at = (q * ROWS + r) * PITCH
            c.flat_one[at : at + N, :] = turned[q * N : (q + 1) * N]
    pair_a = Exchange(c.out_one, c.in_pair, c.sent_pa, c.got_pa, 0, 24)
    pair_b = Exchange(c.out_one, c.in_pair, c.sent_pb, c.got_pb, 24, 40)
    pair_a.pack_and_send(packed(c.flat_one, 0, 24))
    pair_b.pack_and_send(packed(c.flat_one, 24, 40))
    one.late_sums()
    total = None
    for r in range(ROWS):
        part = nt(c.outer[r], c.adjoint[:, row_lanes(r)])
        total = part if total is None else total + part
    c.fin_wide[...] = total
    for k in range(HIDDEN):
        c.mine[k * HIDDEN : (k + 1) * HIDDEN, :] = strided(c.fin_wide, k, HIDDEN, HIDDEN)
    large = Total(
        c.mine, c.theirs, c.blocks, c.landed, c.own_sum, c.full,
        (c.swap_a0, c.swap_a1, c.sent_a, c.got_a, c.sent_ag, c.got_ag, c.pass_ag, c.heard_ag),
    )
    small = Exchange(c.flank_blocks, c.flank_landed, c.sent_b, c.got_b, 0, 2)
    large.swap().start()
    large.scatter()
    for r in range(ROWS):
        outer_grads(c, nn(c.fin_split[...], c.adjoint[:, row_lanes(r)]), r)
    outer_sums(c, c.right_all, c.acc_left)
    for part, lo, hi in ((pair_a, 0, 4), (pair_b, 4, ROWS)):
        part.receive(widen_into(c.wide, c.in_pair, 6 * lo, 24 if lo == 0 else 40, 40))
        for q in range(lo, hi):
            for r in range(ROWS):
                c.columns[q, r * N : (r + 1) * N, :] = strided(
                    c.wide, q * ROWS + r, N, 40
                ).astype(BF16)
            outer_grads(c, nt(c.fin[...], c.columns[q]), q)
    outer_sums(c, c.left_all, c.acc_right)
    lane = lax.broadcasted_iota(jnp.int32, (2 * HIDDEN, 2 * SEQ), 1)
    flank_sum = jnp.zeros((2 * HIDDEN, FEATURES), F32)
    grads = []
    for r in range(ROWS):
        both = jnp.concatenate([matched(c.acc_left, r), matched(c.acc_right, r)], 0)
        both = jnp.where(lane < SEQ, both * (1.0 / SEQ), 0.0)
        c.flank_grad[r] = both
        hatted, _ = ln1(c.alignment[r].astype(F32))
        norm = jnp.concatenate([hatted.astype(BF16), none], 0)
        flank_sum = flank_sum + nn(both.astype(BF16), norm)
    for half in range(2):
        for d in range(N // 2):
            c.flank_blocks[half * (N // 2) + d] = flank_sum[
                2 * d : 2 * d + 2, half * 128 : (half + 1) * 128
            ]
    small.send_all()
    large.spread()
    for r in range(ROWS):
        grad = nn(c.flank_grad[r].T[:SEQ].astype(BF16), flank_turned)
        hatted, factor = ln1(c.alignment[r].astype(F32))
        c.align_grad[r] = (
            factor
            * (
                grad
                - jnp.mean(grad, axis=1, keepdims=True)
                - hatted * jnp.mean(grad * hatted, axis=1, keepdims=True)
            )
        ).astype(BF16)
    small.all_others().wait_recv()
    total = c.flank_landed[0]
    for d in range(1, N):
        total = total + c.flank_landed[d]
    c.flank_own[...] = total * (1.0 / RES)
    me = me_index()
    c.flank_full[me] = c.flank_own[...]

    def to_all(k):
        d = ahead(k)
        return remote(c.flank_own, c.flank_full.at[me], c.sent_bg, c.got_bg, d)

    loop(N, lambda k: to_all(k).start(), 1)
    large.gather.hand_on()
    natural(c, c.adjoint, c.adjoint_pair)
    others = c.flank_full.at[pl.ds(0, N - 1)]
    summed = remote(others, others, c.sent_bg, c.got_bg, ahead(1))
    large.gather.finish()
    summed.wait_recv()
    pair_a.close()
    pair_b.close()
    small.close()
    summed.wait_send()
    large.close()


def vmem(count):
    return [pl.BlockSpec(memory_space=pltpu.VMEM)] * count


def shaped(shape, dtype):
    return jax.ShapeDtypeStruct(shape, dtype)


INPUTS = ("edge", "alignment", "flank", "fin", "p_out", "f_out", "p_in", "f_in", "seed")
OUTPUTS = dict(
    new_pair=((CELLS, CH), BF16),
    adjoint_pair=((CELLS, CH), BF16),
    align_grad=((ROWS, SEQ, FEATURES), BF16),
    full=((2, CHIPS, 40, 128), BF16),
    flank_full=((N, 2, 128), F32),
)


def scratch():
    shapes = dict(
        x_one=((CH, CELLS), BF16),
        x_two=((CH, CELLS), BF16),
        new_cells=((CH, CELLS), BF16),
        adjoint=((CH, CELLS), BF16),
        seed_cells=((CH, CELLS), BF16),
        grad_two=((CH, CELLS), F32),
        flat=((72 * PITCH, 128), F32),
        flat_one=((40 * PITCH, 128), F32),
        wide=((104 * N, 128), F32),
        out_two=((N, 72, 128), BF16),
        out_one=((N, 40, 128), BF16),
        unit=((CH, CELLS), BF16),
        scaled=((CH, CELLS), BF16),
        coef=((4 * CH, CELLS), F32),
        grad_proj=((5 * CH, CELLS), BF16),
        grad_m=((RES, RES), BF16),
        mine=((2560, 128), F32),
        theirs=((1280, 128), F32),
        blocks=((CHIPS, 40, 128), BF16),
        landed=((CHIPS, 40, 128), BF16),
        own_sum=((40, 128), BF16),
        flank_blocks=((N, 2, 128), F32),
        flank_landed=((N, 2, 128), F32),
        flank_own=((2, 128), F32),
        flank_grad=((ROWS, 2 * HIDDEN, 128), F32),
        own_right=((2, 48, 128), BF16),
        own_left=((3, 32, 128), BF16),
        own_outer=((2 * ROWS * HIDDEN, 2 * SEQ), BF16),
        in_right=((2, 2, CHIPS, 48, 128), BF16),
        in_left=((3, 2, CHIPS, 32, 128), BF16),
        right_all=((RES, HIDDEN * SEQ), BF16),
        left_all=((RES, HIDDEN * SEQ), BF16),
        cells_wide=((RES, 128), F32),
        fin_wide=((HIDDEN * HIDDEN, CH), F32),
        fin_split=((HIDDEN * HIDDEN, CH), BF16),
        fin_turned=((CH, HIDDEN * HIDDEN), BF16),
        outer=((ROWS, HIDDEN * HIDDEN, RES), BF16),
        outer_grad=((PAIRS, RES, RES), BF16),
        acc_left=((RES, 128), F32),
        acc_right=((RES, 128), F32),
        columns=((ROWS, RES, CH), BF16),
        in_pair=((N, 40, 128), BF16),
    )
    each = dict(
        norm=((CH, CELLS), BF16),
        gate=((CH, CELLS), F32),
        tri=((CH, CELLS), BF16),
        kept=((4, RES, RES), BF16),
        in_ops=((N, 72, 128), BF16),
        in_tri=((N, 40, 128), BF16),
        in_grad=((N, 40, 128), BF16),
        in_back=((N, 72, 128), BF16),
        turned=((2, 4 * N, CH), BF16),
        straight=((CH, 5 * CH), BF16),
        w_gate=((CH, CH), BF16),
        final=((CH, CH), BF16),
        final_turned=((CH, CH), BF16),
    )
    for kind in ("out", "in"):
        shapes.update({name + "_" + kind: value for name, value in each.items()})
    made = {name: pltpu.VMEM(*value) for name, value in shapes.items()}
    flags = []
    for kind in ("out", "in"):
        for i in range(8):
            flags += ["sent%d_%s" % (i, kind), "got%d_%s" % (i, kind)]
    for tail in ("r0", "r1", "l0", "l1", "l2", "ag"):
        flags += [name + tail for name in ("sent_", "got_", "pass_", "heard_")]
    for tail in ("pa", "pb", "a", "b", "bg"):
        flags += ["sent_" + tail, "got_" + tail]
    flags += ["swap_a0", "swap_a1"]
    made.update({name: pltpu.SemaphoreType.DMA(()) for name in flags})
    return made


def whole(*arrays):
    made = scratch()
    names = INPUTS + tuple(OUTPUTS) + tuple(made)
    return pl.pallas_call(
        lambda *refs: whole_kernel(names, *refs),
        out_shape=tuple(shaped(*value) for value in OUTPUTS.values()),
        in_specs=vmem(len(INPUTS)),
        out_specs=tuple(vmem(len(OUTPUTS))),
        scratch_shapes=list(made.values()),
        compiler_params=pltpu.CompilerParams(
            collective_id=1, has_side_effects=True, vmem_limit_bytes=67_043_328
        ),
        name="window",
    )(*arrays)


def finish_kernel(
    new_ref, adj_ref, align_ref, full_ref, flank_ref,
    new_out, adj_out, align_out, flank_out, fin_out, proj_out, final_out, proj_in, final_in,
    sums,
):
    new_out[...] = new_ref[...]
    adj_out[...] = adj_ref[...]
    align_out[...] = align_ref[...]
    order = hidden_order()

    def place(s):
        at = pl.multiple_of(s * 40, 8)
        sums[pl.ds(at, 40), :] = full_ref[s // CHIPS, lax.rem(s, CHIPS)].astype(F32)

    tiles(place, N, 0, 4)
    fin_out[...] = sums[:1024, :]
    for base, proj, final in ((1024, proj_out, final_out), (1792, proj_in, final_in)):
        for b in range(5):
            block = sums[base + b * CH : base + (b + 1) * CH, :]
            proj[:, b * CH : (b + 1) * CH] = nn(block.astype(BF16), order) if b < 4 else block
        block = sums[base + 5 * CH : base + 6 * CH, :]
        final[...] = nn(order.T, block.astype(BF16))
    for half in range(2):
        for d in range(N // 2):
            flank_out[2 * d : 2 * d + 2, half * 128 : (half + 1) * 128] = flank_ref[
                half * (N // 2) + d
            ]


def shards(
    edge_embedding,
    alignment_embedding,
    tensor_flank_matrix,
    tensor_final_matrix,
    outward_sigmoid_matrix,
    outward_final_matrix,
    inward_sigmoid_matrix,
    inward_final_matrix,
    adjoint_seed,
):
    results = whole(
        edge_embedding.reshape(CELLS, CH),
        alignment_embedding.transpose(1, 0, 2),
        tensor_flank_matrix.T,
        tensor_final_matrix,
        outward_sigmoid_matrix,
        outward_final_matrix,
        inward_sigmoid_matrix,
        inward_final_matrix,
        adjoint_seed.reshape(CELLS, CH),
    )
    outs = pl.pallas_call(
        finish_kernel,
        out_shape=(
            shaped((CELLS, CH), BF16),
            shaped((CELLS, CH), BF16),
            shaped((ROWS, SEQ, FEATURES), BF16),
            shaped((2 * HIDDEN, FEATURES), F32),
            shaped((HIDDEN * HIDDEN, CH), F32),
            shaped((CH, 5 * CH), F32),
            shaped((CH, CH), F32),
            shaped((CH, 5 * CH), F32),
            shaped((CH, CH), F32),
        ),
        in_specs=vmem(5),
        out_specs=tuple(vmem(9)),
        scratch_shapes=[
            pltpu.VMEM((2560, 128), F32),
        ],
        compiler_params=pltpu.CompilerParams(vmem_limit_bytes=VMEM_LIMIT),
        name="finish",
    )(*results)
    return (
        outs[0].reshape(ROWS, RES, CH),
        outs[1].reshape(ROWS, RES, CH),
        outs[2].transpose(1, 0, 2),
        outs[3].T,
        *outs[4:],
    )


def solution(mesh):
    placed = (
        P(("dp", "dap"), None, None),
        P("dp", "dap", None),
        P(),
        P(),
        P(),
        P(),
        P(),
        P(),
        P(("dp", "dap"), None, None),
    )
    return jax.shard_map(
        shards,
        mesh=mesh,
        in_specs=placed,
        out_specs=(
            P(("dp", "dap"), None, None),
            P(("dp", "dap"), None, None),
            P("dp", "dap", None),
            P("dp", None),
            P("dp", None),
            P("dp", None),
            P("dp", None),
            P("dp", None),
            P("dp", None),
        ),
        check_vma=False,
    )
```

```python
from types import SimpleNamespace

import jax
import jax.numpy as jnp
from jax import lax
from jax.experimental import pallas as pl
from jax.experimental.pallas import tpu as pltpu
from jax.sharding import PartitionSpec as P

EPSILON = 1e-05
F32, BF16 = jnp.float32, jnp.bfloat16
MESH = pl.DeviceIdType.MESH
N = 64
ROWS = 6
RES = 384
CELLS = ROWS * RES
CH = 128
GROUPS = CELLS // 128
PITCH = 72
HIDDEN = 32
PAIRS = HIDDEN // 2
SEQ = 64
FEATURES = 256
TILE = 256
TILES = CELLS // TILE
VMEM_LIMIT = 60 * 1024 * 1024


def nn(a, b):
    return lax.dot_general(a, b, (((1,), (0,)), ((), ())), preferred_element_type=F32)


def nt(a, b):
    return lax.dot_general(a, b, (((1,), (1,)), ((), ())), preferred_element_type=F32)


def one_hot(rows, columns, pick, dtype=BF16):
    row = lax.broadcasted_iota(jnp.int32, (rows, columns), 0)
    column = lax.broadcasted_iota(jnp.int32, (rows, columns), 1)
    return jnp.where(pick(row) == column, 1.0, 0.0).astype(dtype)


def identity(size):
    return one_hot(size, size, lambda r: r)


def hidden_order(dtype=BF16):
    return one_hot(CH, CH, lambda r: jnp.where(r < N, 2 * r, 2 * r - (CH - 1)), dtype)


def sigmoid(v):
    return 1.0 / (1.0 + jnp.exp(-v))


def ln0(v):
    centred = v - jnp.mean(v, axis=0, keepdims=True)
    factor = lax.rsqrt(jnp.mean(centred * centred, axis=0, keepdims=True) + EPSILON)
    return centred * factor, factor


def ln0_adjoint(hatted, factor, g):
    return factor * (
        g
        - jnp.mean(g, axis=0, keepdims=True)
        - hatted * jnp.mean(g * hatted, axis=0, keepdims=True)
    )


def loop(count, body, start=0):
    def step(k, carry):
        body(k)
        return carry

    lax.fori_loop(start, count, step, 0)


def me_index():
    return lax.axis_index("dap")


def greet():
    me = me_index()
    sem = pltpu.get_barrier_semaphore()
    tiles(
        lambda k: pl.semaphore_signal(
            sem, inc=1, device_id={"dap": lax.rem(me + k, N)}, device_id_type=MESH
        ),
        N,
        1,
    )


def all_here():
    pl.semaphore_wait(pltpu.get_barrier_semaphore(), N - 1)


def remote(src, dst, send_sem, recv_sem, to):
    return pltpu.make_async_remote_copy(
        src_ref=src,
        dst_ref=dst,
        send_sem=send_sem,
        recv_sem=recv_sem,
        device_id={"dap": to},
        device_id_type=MESH,
    )


BATCH = 3
CHIPS = N // 2
CHIP_STRIDE = 13
STRIDE = 37


def ahead(k):
    return lax.rem(me_index() + k * STRIDE, N)


def tiles(body, stop=TILES, start=0, by=3):
    def step(b):
        for k in range(by):
            body(start + by * b + k)

    loop((stop - start) // by, step)
    for t in range(start + (stop - start) // by * by, stop):
        body(t)


class Exchange:
    def __init__(self, out, into, sent, got, lo, hi):
        self.out, self.into, self.sent, self.got = out, into, sent, got
        self.folded = len(out.shape) == 4
        self.rows = pl.ds(lo // 4, (hi - lo) // 4) if self.folded else pl.ds(lo, hi - lo)

    def fold(self, value):
        return value.reshape(-1, 4, 128) if self.folded else value

    def copy(self, d, at):
        return remote(
            self.out.at[d, self.rows], self.into.at[at, self.rows], self.sent, self.got, d
        )

    def pack_and_send(self, rows_of):
        me = me_index()
        self.into[me, self.rows] = self.fold(rows_of(me))

        def pack(first):
            for k in range(BATCH):
                d = ahead(first + k)
                self.out[d, self.rows] = self.fold(rows_of(d))

        def send(first):
            for k in range(BATCH):
                self.copy(ahead(first + k), me).start()

        pack(1)

        def step(b):
            pack(1 + BATCH * b)
            send(1 + BATCH * (b - 1))

        loop((N - 1) // BATCH, step, 1)
        send(N - BATCH)

    def send_all(self):
        me = me_index()
        self.into[me, self.rows] = self.out[me, self.rows]
        tiles(lambda k: self.copy(ahead(k), me).start(), N, 1)

    def all_others(self):
        others = pl.ds(0, N - 1)
        return remote(
            self.out.at[others, self.rows], self.into.at[others, self.rows],
            self.sent, self.got, ahead(1),
        )

    def receive(self, use):
        self.all_others().wait_recv()
        tiles(use, N, 0, 4)

    def close(self):
        self.all_others().wait_send()


class Gather:
    def __init__(self, own, into, sent, got, passed, heard):
        self.own, self.into = own, into
        self.sent, self.got, self.passed, self.heard = sent, got, passed, heard
        me = me_index()
        self.core, self.chip = lax.rem(me, 2), me // 2
        self.partner = me + 1 - 2 * self.core

    def across(self, k):
        j = lax.rem(self.chip + k * CHIP_STRIDE, CHIPS)
        return remote(
            self.own, self.into.at[self.core, self.chip], self.sent, self.got, 2 * j + self.core
        )

    def all_across(self):
        blocks = self.into.at[self.core, pl.ds(0, CHIPS - 1)]
        return remote(blocks, blocks, self.sent, self.got, self.partner)

    def handed(self, core):
        half = self.into.at[core]
        return remote(half, half, self.passed, self.heard, self.partner)

    def start(self):
        self.into[self.core, self.chip] = self.own[...]
        tiles(lambda k: self.across(k).start(), CHIPS, 1)

    def hand_on(self):
        self.all_across().wait_recv()
        self.handed(self.core).start()

    def finish(self):
        self.handed(1 - self.core).wait_recv()

    def close(self):
        self.all_across().wait_send()
        self.handed(self.core).wait_send()


def ln1(v):
    centred = v - jnp.mean(v, axis=1, keepdims=True)
    factor = lax.rsqrt(jnp.mean(centred * centred, axis=1, keepdims=True) + EPSILON)
    return centred * factor, factor


def strided(ref, start, size, stride):
    return ref[pl.ds(start, size, stride=stride), :]


def packed(flat, lo, hi):
    return lambda d: strided(flat, lo * PITCH + d, hi - lo, PITCH).astype(BF16)


def widen_into(wide, into, lo, hi, pitch):
    def use(s):
        at = pl.multiple_of(s * pitch + lo, 8)
        if len(into.shape) == 4:
            rows = into[s, pl.ds(lo // 4, (hi - lo) // 4)].astype(F32).reshape(hi - lo, 128)
        else:
            rows = into[s, pl.ds(lo, hi - lo)].astype(F32)
        wide[pl.ds(at, hi - lo), :] = rows

    return use


def lanes_of(t):
    return pl.ds(pl.multiple_of(t * TILE, TILE), TILE)


def row_lanes(r):
    return slice(r * RES, (r + 1) * RES)


def pair_lanes(p):
    return pl.ds(pl.multiple_of(p * 128, 128), 128)


def scatter_hidden(flat, value, piece, t):
    for q in range(TILE // 128):
        at = pl.multiple_of((piece * GROUPS + t * (TILE // 128) + q) * PITCH, 8)
        flat[pl.ds(at, N), :] = value[:, q * 128 : (q + 1) * 128]


def gather_hidden(wide, pitch, bases, t):
    parts = []
    for base in bases:
        row = [
            strided(wide, base + t * (TILE // 128) + q, N, pitch) for q in range(TILE // 128)
        ]
        parts.append(jnp.concatenate(row, axis=1))
    return jnp.concatenate(parts, axis=0)


def scatter_rows(flat, value, piece):
    for r in range(ROWS):
        for jg in range(3):
            at = (piece * GROUPS + r * 3 + jg) * PITCH
            flat[at : at + N, :] = value[r * N : (r + 1) * N, jg * 128 : (jg + 1) * 128]


def gather_matrix(out, wide, pitch, base):
    for r in range(ROWS):
        for jg in range(3):
            out[r * N : (r + 1) * N, jg * 128 : (jg + 1) * 128] = strided(
                wide, base + r * 3 + jg, N, pitch
            ).astype(BF16)


def prepare(w, p_ref, f_ref):
    order = hidden_order()
    for b in range(4):
        block = p_ref[:, b * CH : (b + 1) * CH]
        turned = nt(order, block).astype(BF16)
        for m in range(2):
            w.turned[m, b * N : (b + 1) * N, :] = turned[m * N : (m + 1) * N]
        w.straight[:, b * CH : (b + 1) * CH] = nt(block, order).astype(BF16)
    w.gate[...] = nt(identity(CH), p_ref[:, 4 * CH :]).astype(BF16)
    w.straight[:, 4 * CH :] = p_ref[:, 4 * CH :]
    w.final[...] = nn(order, f_ref[...]).astype(BF16)
    w.final_turned[...] = nt(identity(CH), w.final[...]).astype(BF16)


class Update:
    def __init__(self, c, u, w, outgoing, sums_at):
        self.c, self.u, self.w, self.outgoing, self.sums_at = c, u, w, outgoing, sums_at
        plan = (
            ("ops_a", c.out_two, u.in_ops, 0, 40),
            ("ops_b", c.out_two, u.in_ops, 40, 72),
            ("tri_a", c.out_one, u.in_tri, 0, 16),
            ("tri_b", c.out_one, u.in_tri, 16, 36),
            ("grad_a", c.out_one, u.in_grad, 0, 24),
            ("grad_b", c.out_one, u.in_grad, 24, 36),
            ("back_a", c.out_two, u.in_back, 0, 32),
            ("back_b", c.out_two, u.in_back, 32, 72),
        )
        for i, (name, out, into, lo, hi) in enumerate(plan):
            setattr(self, name, Exchange(out, into, u.sent[i], u.got[i], lo, hi))

    def gated(self, m, t, norm=None):
        norm = self.u.norm[:, lanes_of(t)] if norm is None else norm
        pre = nn(self.w.turned[m], norm)
        flat = self.c.flat
        scatter_hidden(flat, sigmoid(pre[:N]) * pre[N : 2 * N], 2 * m, t)
        scatter_hidden(flat, sigmoid(pre[2 * N : 3 * N]) * pre[3 * N :], 2 * m + 1, t)

    def enter(self, t, x):
        norm = ln0(x)[0].astype(BF16)
        self.u.norm[:, lanes_of(t)] = norm
        self.gated(0, t, norm)

    def gates(self, t):
        at = lanes_of(t)
        self.u.gate[:, at] = sigmoid(nn(self.w.gate[...], self.u.norm[:, at]))

    def arrived(self, t):
        tri = gather_hidden(self.c.wide, 40, (0, GROUPS), t)
        hatted, factor = ln0(tri)
        unit = hatted.astype(BF16)
        return tri, hatted, factor, unit, nn(self.w.final_turned[...], unit)

    def descend(self, t, gz, hatted, factor, unit, values):
        c, at = self.c, lanes_of(t)
        gate = self.u.gate[:, at]
        scaled_wide = gz * gate
        scaled = scaled_wide.astype(BF16)
        c.unit[:, at] = unit
        c.scaled[:, at] = scaled
        c.grad_proj[4 * CH :, at] = (scaled_wide * values * (1.0 - gate)).astype(BF16)
        grad = ln0_adjoint(hatted, factor, nn(self.w.final[...], scaled))
        for m in range(2):
            scatter_hidden(c.flat_one, grad[m * N : (m + 1) * N], m, t)

    def coefficients(self, t):
        c, at = self.c, lanes_of(t)
        norm = self.u.norm[:, at]
        for m in range(2):
            pre = nn(self.w.turned[m], norm)
            for side in range(2):
                opened = sigmoid(pre[2 * side * N : (2 * side + 1) * N])
                slope = pre[(2 * side + 1) * N : (2 * side + 2) * N] * opened * (1.0 - opened)
                rows = 2 * side * CH + m * N
                c.coef[rows : rows + N, at] = slope
                c.coef[rows + CH : rows + CH + N, at] = opened

    def returned(self, t, x, gz):
        c, at = self.c, lanes_of(t)
        for side in range(2):
            base = 2 * side * CH
            grad = gather_hidden(c.wide, 72, (side * GROUPS, (2 + side) * GROUPS), t)
            for half in range(2):
                rows = pl.ds(base + half * CH, CH)
                c.grad_proj[rows, at] = (grad * c.coef[rows, at]).astype(BF16)
        grad_norm = nn(self.w.straight[...], c.grad_proj[:, at])
        hatted, factor = ln0(x)
        return gz + ln0_adjoint(hatted, factor, grad_norm)

    def keep_sum(self, block, value):
        at = self.sums_at + block * CH
        self.c.mine[at : at + CH, :] = value

    def early_sums(self):
        self.keep_sum(5, nt(self.c.unit[...], self.c.scaled[...]))
        self.keep_sum(4, nt(self.u.norm[...], self.c.grad_proj[4 * CH :, :]))

    def late_sums(self):
        for b in range(4):
            self.keep_sum(b, nt(self.u.norm[...], self.c.grad_proj[b * CH : (b + 1) * CH, :]))

    def forward(self, between):
        c, u = self.c, self.u
        tiles(lambda t: self.gated(1, t), 2, 0, 2)
        self.ops_a.pack_and_send(packed(c.flat, 0, 40))
        tiles(lambda t: self.gated(1, t), TILES, 2)
        self.ops_b.pack_and_send(packed(c.flat, 40, 72))
        between()
        tiles(self.gates)
        for m in range(2):
            if m == 0:
                self.ops_a.receive(widen_into(c.wide, u.in_ops, 0, 40, 72))
            else:
                self.ops_b.receive(widen_into(c.wide, u.in_ops, 40, 72, 72))
            for op in range(2):
                gather_matrix(u.kept.at[2 * op + m], c.wide, 72, (2 * m + op) * GROUPS)
            left, right = u.kept[m], u.kept[2 + m]
            product = nt(left, right) if self.outgoing else nn(left.T, right)
            scatter_rows(c.flat_one, product, m)
            if m == 0:
                self.tri_a.pack_and_send(packed(c.flat_one, 0, 16))
            else:
                self.tri_b.pack_and_send(packed(c.flat_one, 16, 36))
        self.ops_a.close()
        self.ops_b.close()
        self.tri_a.receive(widen_into(c.wide, u.in_tri, 0, 16, 40))
        self.tri_b.receive(widen_into(c.wide, u.in_tri, 16, 36, 40))
        self.tri_a.close()
        self.tri_b.close()

    def backward(self, between):
        c, u = self.c, self.u
        self.grad_a.pack_and_send(packed(c.flat_one, 0, 24))
        self.grad_b.pack_and_send(packed(c.flat_one, 24, 36))
        between()
        tiles(self.coefficients)
        self.early_sums()
        for m in range(2):
            if m == 0:
                self.grad_a.receive(widen_into(c.wide, u.in_grad, 0, 24, 40))
            else:
                self.grad_b.receive(widen_into(c.wide, u.in_grad, 24, 36, 40))
            gather_matrix(c.grad_m, c.wide, 40, m * GROUPS)
            grad = c.grad_m[...]
            left, right = u.kept[m], u.kept[2 + m]
            if self.outgoing:
                grad_left, grad_right = nn(grad, right), nn(grad.T, left)
            else:
                grad_left, grad_right = nt(right, grad), nn(left, grad)
            scatter_rows(c.flat, grad_left, 2 * m)
            scatter_rows(c.flat, grad_right, 2 * m + 1)
            if m == 0:
                self.back_a.pack_and_send(packed(c.flat, 0, 32))
            else:
                self.back_b.pack_and_send(packed(c.flat, 32, 72))
        self.grad_a.close()
        self.grad_b.close()
        self.back_a.receive(widen_into(c.wide, u.in_back, 0, 32, 72))
        self.back_b.receive(widen_into(c.wide, u.in_back, 32, 72, 72))
        self.back_a.close()
        self.back_b.close()


class Total:
    def __init__(self, mine, theirs, blocks, landed, own, full, sems_of):
        self.mine, self.theirs, self.blocks, self.landed = mine, theirs, blocks, landed
        self.own, self.half = own, theirs.shape[0]
        self.share = self.half // (N // 2)
        self.sent0, self.got0, self.sent1, self.got1, *rest = sems_of
        self.gather = Gather(own, full, *rest)

    def swap(self):
        core = lax.rem(me_index(), 2)
        other = pl.ds(pl.multiple_of((1 - core) * self.half, 8), self.half)
        return remote(
            self.mine.at[other], self.theirs, self.sent0, self.got0, self.gather.partner
        )

    def to(self, k):
        g = self.gather
        j = lax.rem(g.chip + k * CHIP_STRIDE, CHIPS)
        return remote(
            self.blocks.at[j], self.landed.at[g.chip], self.sent1, self.got1, 2 * j + g.core
        )

    def all_others(self):
        others = pl.ds(0, CHIPS - 1)
        return remote(
            self.blocks.at[others], self.landed.at[others], self.sent1, self.got1,
            self.gather.partner,
        )

    def scatter(self):
        g = self.gather
        self.swap().wait_recv()
        mine = self.mine[pl.ds(pl.multiple_of(g.core * self.half, 8), self.half), :]
        for j in range(CHIPS):
            at = slice(j * self.share, (j + 1) * self.share)
            self.blocks[j] = (mine[at] + self.theirs[at, :]).astype(self.blocks.dtype)
        loop(CHIPS, lambda k: self.to(k).start(), 1)
        self.landed[g.chip] = self.blocks[g.chip]

    def spread(self):
        self.all_others().wait_recv()
        total = self.landed[0].astype(F32)
        for j in range(1, CHIPS):
            total = total + self.landed[j].astype(F32)
        self.own[...] = (total * (1.0 / RES)).astype(self.own.dtype)
        self.gather.start()

    def close(self):
        self.swap().wait_send()
        self.all_others().wait_send()
        self.gather.close()


def spread_out(all_ref, wide, into, rows, placed):
    pitch = rows if rows // 8 % 2 else rows + 8

    def widen(s):
        at = pl.ds(pl.multiple_of(s * pitch, 8), rows)
        wide[at, :] = into[lax.rem(s, 2), s // 2].astype(F32)

    tiles(widen, N, 0, 4)
    for r, p, row in placed:
        all_ref[r * N : (r + 1) * N, p * 128 : (p + 1) * 128] = strided(
            wide, row, N, pitch
        ).astype(BF16)


def cells_of(c, ref, out):
    for r in range(ROWS):
        c.cells_wide[:RES, :] = ref[row_lanes(r), :].astype(F32)
        parts = [strided(c.cells_wide, q, N, ROWS) for q in range(ROWS)]
        out[:, row_lanes(r)] = jnp.concatenate(parts, 0).T.astype(BF16)


def natural(c, cells, out):
    for r in range(ROWS):
        turned = cells[:, row_lanes(r)].astype(F32).T
        for q in range(ROWS):
            c.cells_wide[pl.ds(q, N, stride=ROWS), :] = turned[q * N : (q + 1) * N]
        out[row_lanes(r), :] = c.cells_wide[...].astype(BF16)


def outer_grads(c, block, r):
    for p in range(PAIRS):
        c.outer_grad[p, r * 64 : (r + 1) * 64, :] = block[p * 64 : (p + 1) * 64].astype(BF16)


def outer_sums(c, all_ref, acc):
    acc[...] = jnp.zeros_like(acc)

    def add(b):
        part = None
        for k in range(4):
            here = nn(c.outer_grad[4 * b + k], all_ref[:, pair_lanes(4 * b + k)])
            part = here if part is None else part + here
        acc[...] += part

    loop(PAIRS // 4, add)


def matched(acc, r):
    return acc[r * 64 : r * 64 + 32, :] + pltpu.roll(acc[r * 64 + 32 : (r + 1) * 64, :], 64, 1)


def whole_kernel(names, *refs):
    c = SimpleNamespace(**dict(zip(names, refs)))
    greet()
    phases = []
    for kind in ("out", "in"):
        part = lambda name: getattr(c, name + "_" + kind)
        phases.append(
            SimpleNamespace(
                norm=part("norm"), gate=part("gate"), tri=part("tri"), kept=part("kept"),
                in_ops=part("in_ops"), in_tri=part("in_tri"),
                in_grad=part("in_grad"), in_back=part("in_back"),
                sent=[part("sent%d" % i) for i in range(8)],
                got=[part("got%d" % i) for i in range(8)],
                weights=SimpleNamespace(
                    turned=part("turned"), straight=part("straight"), gate=part("w_gate"),
                    final=part("final"), final_turned=part("final_turned"),
                ),
            )
        )
    out, into = phases

    flank_turned = c.flank[...]
    split = lambda first: one_hot(
        HIDDEN, 2 * HIDDEN, lambda r: first + jnp.where(r < PAIRS, 2 * r, 2 * r - (HIDDEN - 1))
    )
    split_left = nn(split(0), flank_turned).astype(BF16)
    split_right = nn(split(HIDDEN), flank_turned).astype(BF16)
    plain_left = flank_turned[:HIDDEN]
    none = jnp.zeros((SEQ, FEATURES), BF16)
    for r in range(ROWS):
        hatted, _ = ln1(c.alignment[r].astype(F32))
        norm = hatted.astype(BF16)
        halves = (jnp.concatenate([norm, none], 0), jnp.concatenate([none, norm], 0))
        made = [
            (nt(weights[:PAIRS], halves[0]) + nt(weights[PAIRS:], halves[1])).astype(BF16)
            for weights in (split_right, split_left)
        ]
        for h in range(2):
            c.own_right[h, r * 8 : (r + 1) * 8, :] = made[0][h * 8 : (h + 1) * 8]
        c.own_left[r // 2, (r % 2) * PAIRS : (r % 2 + 1) * PAIRS, :] = made[1]
        for h in range(2):
            at = (2 * r + h) * HIDDEN
            c.own_outer[at : at + HIDDEN, :] = nt(plain_left, halves[h]).astype(BF16)
    all_here()
    gather = lambda own, into, tail: Gather(
        own, into, *(getattr(c, name + tail) for name in ("sent_", "got_", "pass_", "heard_"))
    )
    right = [gather(c.own_right.at[h], c.in_right.at[h], "r%d" % h) for h in range(2)]
    left = [gather(c.own_left.at[h], c.in_left.at[h], "l%d" % h) for h in range(3)]
    right[0].start()
    right[1].start()
    cells_of(c, c.edge, c.x_one)
    cells_of(c, c.seed, c.seed_cells)
    prepare(out.weights, c.p_out, c.f_out)
    prepare(into.weights, c.p_in, c.f_in)
    c.fin_wide[...] = c.fin[...].astype(F32)
    for d in range(HIDDEN):
        c.fin_split[d * HIDDEN : (d + 1) * HIDDEN, :] = strided(
            c.fin_wide, d, HIDDEN, HIDDEN
        ).astype(BF16)
    c.fin_turned[...] = nt(identity(CH), c.fin_split[...]).astype(BF16)
    def outer_pair(p):
        block = nt(c.own_outer[...], c.right_all[:, pair_lanes(p)]) * (1.0 / SEQ)
        for r in range(ROWS):
            c.outer[r, pl.ds(pl.multiple_of(p * 64, 64), 64), :] = block[
                r * 64 : (r + 1) * 64
            ].astype(BF16)

    for h in range(2):
        right[h].hand_on()
        right[h].finish()
        if h == 1:
            left[0].start()
        spread_out(
            c.right_all, c.wide, c.in_right.at[h], 48,
            [(r, 8 * h + p, r * 8 + p) for r in range(ROWS) for p in range(8)],
        )
        tiles(outer_pair, 8 * h + 8, 8 * h, 4)
    for r in range(ROWS):
        at = row_lanes(r)
        c.x_one[:, at] = (c.x_one[:, at].astype(F32) + nn(c.fin_turned[...], c.outer[r])).astype(
            BF16
        )
    right[0].close()
    right[1].close()

    one = Update(c, out, out.weights, True, 1024)
    two = Update(c, into, into.weights, False, 1792)
    tiles(lambda t: one.enter(t, c.x_one[:, lanes_of(t)].astype(F32)))
    one.forward(left[0].hand_on)
    left[1].start()

    def between_updates(t):
        at = lanes_of(t)
        tri, _, _, _, values = one.arrived(t)
        out.tri[:, at] = tri.astype(BF16)
        new = (c.x_one[:, at].astype(F32) + out.gate[:, at] * values).astype(BF16)
        c.x_two[:, at] = new
        two.enter(t, new.astype(F32))

    tiles(between_updates)
    two.forward(left[1].hand_on)
    left[2].start()

    def turn_round(t):
        at = lanes_of(t)
        _, hatted, factor, unit, values = two.arrived(t)
        c.new_cells[:, at] = (
            c.x_two[:, at].astype(F32) + into.gate[:, at] * values
        ).astype(BF16)
        two.descend(t, c.seed_cells[:, at].astype(F32), hatted, factor, unit, values)

    def after_turn():
        left[2].hand_on()
        natural(c, c.new_cells, c.new_pair)

        def ahead_of_back(t):
            at = lanes_of(t)
            unit = ln0(out.tri[:, at].astype(F32))[0].astype(BF16)
            c.values[:, at] = nn(out.weights.final_turned[...], unit)

        tiles(ahead_of_back)

    tiles(turn_round)
    two.backward(after_turn)

    def between_backs(t):
        at = lanes_of(t)
        c.grad_two[:, at] = two.returned(
            t, c.x_two[:, at].astype(F32), c.seed_cells[:, at].astype(F32)
        )

    def below(t):
        at = lanes_of(t)
        hatted, factor = ln0(out.tri[:, at].astype(F32))
        one.descend(
            t, c.grad_two[:, at], hatted, factor, hatted.astype(BF16), c.values[:, at]
        )

    tiles(between_backs)
    tiles(below)

    def meanwhile():
        two.late_sums()
        for h in range(3):
            left[h].finish()
            left[h].close()
            spread_out(
                c.left_all, c.wide, c.in_left.at[h], 32,
                [(2 * h + r, p, r * PAIRS + p) for r in range(2) for p in range(PAIRS)],
            )

    one.backward(meanwhile)

    def last(t):
        at = lanes_of(t)
        c.adjoint[:, at] = one.returned(
            t, c.x_one[:, at].astype(F32), c.grad_two[:, at]
        ).astype(BF16)

    tiles(last)

    for r in range(ROWS):
        turned = c.adjoint[:, row_lanes(r)].astype(F32).T
        for q in range(ROWS):
            at = (q * ROWS + r) * PITCH
            c.flat_one[at : at + N, :] = turned[q * N : (q + 1) * N]
    pair_a = Exchange(c.out_one, c.in_pair, c.sent_pa, c.got_pa, 0, 24)
    pair_b = Exchange(c.out_one, c.in_pair, c.sent_pb, c.got_pb, 24, 36)
    pair_a.pack_and_send(packed(c.flat_one, 0, 24))
    pair_b.pack_and_send(packed(c.flat_one, 24, 36))
    one.late_sums()
    total = None
    for r in range(ROWS):
        part = nt(c.outer[r], c.adjoint[:, row_lanes(r)])
        total = part if total is None else total + part
    c.fin_wide[...] = total
    for k in range(HIDDEN):
        c.mine[k * HIDDEN : (k + 1) * HIDDEN, :] = strided(c.fin_wide, k, HIDDEN, HIDDEN)
    large = Total(
        c.mine, c.theirs, c.blocks, c.landed, c.own_sum, c.full,
        (c.swap_a0, c.swap_a1, c.sent_a, c.got_a, c.sent_ag, c.got_ag, c.pass_ag, c.heard_ag),
    )
    small = Exchange(c.flank_blocks, c.flank_landed, c.sent_b, c.got_b, 0, 2)
    large.swap().start()
    large.scatter()
    for r in range(ROWS):
        outer_grads(c, nn(c.fin_split[...], c.adjoint[:, row_lanes(r)]), r)
    outer_sums(c, c.right_all, c.acc_left)
    for part, lo, hi in ((pair_a, 0, 4), (pair_b, 4, ROWS)):
        part.receive(widen_into(c.wide, c.in_pair, 6 * lo, 24 if lo == 0 else 36, 40))
        for q in range(lo, hi):
            for r in range(ROWS):
                c.columns[q, r * N : (r + 1) * N, :] = strided(
                    c.wide, q * ROWS + r, N, 40
                ).astype(BF16)
            outer_grads(c, nt(c.fin[...], c.columns[q]), q)
    outer_sums(c, c.left_all, c.acc_right)
    lane = lax.broadcasted_iota(jnp.int32, (2 * HIDDEN, 2 * SEQ), 1)
    flank_sum = jnp.zeros((2 * HIDDEN, FEATURES), F32)
    grads = []
    for r in range(ROWS):
        both = jnp.concatenate([matched(c.acc_left, r), matched(c.acc_right, r)], 0)
        both = jnp.where(lane < SEQ, both * (1.0 / SEQ), 0.0)
        c.flank_grad[r] = both
        hatted, _ = ln1(c.alignment[r].astype(F32))
        norm = jnp.concatenate([hatted.astype(BF16), none], 0)
        flank_sum = flank_sum + nn(both.astype(BF16), norm)
    for half in range(2):
        for d in range(N // 2):
            c.flank_blocks[half * (N // 2) + d] = flank_sum[
                2 * d : 2 * d + 2, half * 128 : (half + 1) * 128
            ]
    small.send_all()
    large.spread()
    for r in range(ROWS):
        grad = nn(c.flank_grad[r].T[:SEQ].astype(BF16), flank_turned)
        hatted, factor = ln1(c.alignment[r].astype(F32))
        c.align_grad[r] = (
            factor
            * (
                grad
                - jnp.mean(grad, axis=1, keepdims=True)
                - hatted * jnp.mean(grad * hatted, axis=1, keepdims=True)
            )
        ).astype(BF16)
    small.all_others().wait_recv()
    total = c.flank_landed[0]
    for d in range(1, N):
        total = total + c.flank_landed[d]
    c.flank_own[...] = total * (1.0 / RES)
    me = me_index()
    c.flank_full[me] = c.flank_own[...]

    def to_all(k):
        d = ahead(k)
        return remote(c.flank_own, c.flank_full.at[me], c.sent_bg, c.got_bg, d)

    tiles(lambda k: to_all(k).start(), N, 1)
    large.gather.hand_on()
    natural(c, c.adjoint, c.adjoint_pair)
    others = c.flank_full.at[pl.ds(0, N - 1)]
    summed = remote(others, others, c.sent_bg, c.got_bg, ahead(1))
    large.gather.finish()
    summed.wait_recv()
    pair_a.close()
    pair_b.close()
    small.close()
    summed.wait_send()
    large.close()


def vmem(count):
    return [pl.BlockSpec(memory_space=pltpu.VMEM)] * count


def shaped(shape, dtype):
    return jax.ShapeDtypeStruct(shape, dtype)


INPUTS = ("edge", "alignment", "flank", "fin", "p_out", "f_out", "p_in", "f_in", "seed")
OUTPUTS = dict(
    new_pair=((CELLS, CH), BF16),
    adjoint_pair=((CELLS, CH), BF16),
    align_grad=((ROWS, SEQ, FEATURES), BF16),
    full=((2, CHIPS, 40, 128), BF16),
    flank_full=((N, 2, 128), F32),
)


def scratch():
    shapes = dict(
        x_one=((CH, CELLS), BF16),
        x_two=((CH, CELLS), BF16),
        new_cells=((CH, CELLS), BF16),
        adjoint=((CH, CELLS), BF16),
        seed_cells=((CH, CELLS), BF16),
        grad_two=((CH, CELLS), F32),
        values=((CH, CELLS), F32),
        flat=((72 * PITCH, 128), F32),
        flat_one=((36 * PITCH, 128), F32),
        wide=((104 * N, 128), F32),
        out_two=((N, 72, 128), BF16),
        out_one=((N, 9, 4, 128), BF16),
        unit=((CH, CELLS), BF16),
        scaled=((CH, CELLS), BF16),
        coef=((4 * CH, CELLS), F32),
        grad_proj=((5 * CH, CELLS), BF16),
        grad_m=((RES, RES), BF16),
        mine=((2560, 128), F32),
        theirs=((1280, 128), F32),
        blocks=((CHIPS, 40, 128), BF16),
        landed=((CHIPS, 40, 128), BF16),
        own_sum=((40, 128), BF16),
        flank_blocks=((N, 2, 128), F32),
        flank_landed=((N, 2, 128), F32),
        flank_own=((2, 128), F32),
        flank_grad=((ROWS, 2 * HIDDEN, 128), F32),
        own_right=((2, 48, 128), BF16),
        own_left=((3, 32, 128), BF16),
        own_outer=((2 * ROWS * HIDDEN, 2 * SEQ), BF16),
        in_right=((2, 2, CHIPS, 48, 128), BF16),
        in_left=((3, 2, CHIPS, 32, 128), BF16),
        right_all=((RES, HIDDEN * SEQ), BF16),
        left_all=((RES, HIDDEN * SEQ), BF16),
        cells_wide=((RES, 128), F32),
        fin_wide=((HIDDEN * HIDDEN, CH), F32),
        fin_split=((HIDDEN * HIDDEN, CH), BF16),
        fin_turned=((CH, HIDDEN * HIDDEN), BF16),
        outer=((ROWS, HIDDEN * HIDDEN, RES), BF16),
        outer_grad=((PAIRS, RES, RES), BF16),
        acc_left=((RES, 128), F32),
        acc_right=((RES, 128), F32),
        columns=((ROWS, RES, CH), BF16),
        in_pair=((N, 9, 4, 128), BF16),
    )
    each = dict(
        norm=((CH, CELLS), BF16),
        gate=((CH, CELLS), F32),
        tri=((CH, CELLS), BF16),
        kept=((4, RES, RES), BF16),
        in_ops=((N, 72, 128), BF16),
        in_tri=((N, 9, 4, 128), BF16),
        in_grad=((N, 9, 4, 128), BF16),
        in_back=((N, 72, 128), BF16),
        turned=((2, 4 * N, CH), BF16),
        straight=((CH, 5 * CH), BF16),
        w_gate=((CH, CH), BF16),
        final=((CH, CH), BF16),
        final_turned=((CH, CH), BF16),
    )
    for kind in ("out", "in"):
        shapes.update({name + "_" + kind: value for name, value in each.items()})
    made = {name: pltpu.VMEM(*value) for name, value in shapes.items()}
    flags = []
    for kind in ("out", "in"):
        for i in range(8):
            flags += ["sent%d_%s" % (i, kind), "got%d_%s" % (i, kind)]
    for tail in ("r0", "r1", "l0", "l1", "l2", "ag"):
        flags += [name + tail for name in ("sent_", "got_", "pass_", "heard_")]
    for tail in ("pa", "pb", "a", "b", "bg"):
        flags += ["sent_" + tail, "got_" + tail]
    flags += ["swap_a0", "swap_a1"]
    made.update({name: pltpu.SemaphoreType.DMA(()) for name in flags})
    return made


def whole(*arrays):
    made = scratch()
    names = INPUTS + tuple(OUTPUTS) + tuple(made)
    return pl.pallas_call(
        lambda *refs: whole_kernel(names, *refs),
        out_shape=tuple(shaped(*value) for value in OUTPUTS.values()),
        in_specs=vmem(len(INPUTS)),
        out_specs=tuple(vmem(len(OUTPUTS))),
        scratch_shapes=list(made.values()),
        compiler_params=pltpu.CompilerParams(
            collective_id=1, has_side_effects=True, vmem_limit_bytes=67_043_328
        ),
        name="window",
    )(*arrays)


def finish_kernel(
    new_ref, adj_ref, align_ref, full_ref, flank_ref,
    new_out, adj_out, align_out, flank_out, fin_out, proj_out, final_out, proj_in, final_in,
    sums,
):
    new_out[...] = new_ref[...]
    adj_out[...] = adj_ref[...]
    align_out[...] = align_ref[...]
    order = hidden_order()

    def place(s):
        at = pl.multiple_of(s * 40, 8)
        sums[pl.ds(at, 40), :] = full_ref[s // CHIPS, lax.rem(s, CHIPS)].astype(F32)

    tiles(place, N, 0, 4)
    fin_out[...] = sums[:1024, :]
    for base, proj, final in ((1024, proj_out, final_out), (1792, proj_in, final_in)):
        for b in range(5):
            block = sums[base + b * CH : base + (b + 1) * CH, :]
            proj[:, b * CH : (b + 1) * CH] = nn(block.astype(BF16), order) if b < 4 else block
        block = sums[base + 5 * CH : base + 6 * CH, :]
        final[...] = nn(order.T, block.astype(BF16))
    for half in range(2):
        for d in range(N // 2):
            flank_out[2 * d : 2 * d + 2, half * 128 : (half + 1) * 128] = flank_ref[
                half * (N // 2) + d
            ]


def shards(
    edge_embedding,
    alignment_embedding,
    tensor_flank_matrix,
    tensor_final_matrix,
    outward_sigmoid_matrix,
    outward_final_matrix,
    inward_sigmoid_matrix,
    inward_final_matrix,
    adjoint_seed,
):
    results = whole(
        edge_embedding.reshape(CELLS, CH),
        alignment_embedding.transpose(1, 0, 2),
        tensor_flank_matrix.T,
        tensor_final_matrix,
        outward_sigmoid_matrix,
        outward_final_matrix,
        inward_sigmoid_matrix,
        inward_final_matrix,
        adjoint_seed.reshape(CELLS, CH),
    )
    outs = pl.pallas_call(
        finish_kernel,
        out_shape=(
            shaped((CELLS, CH), BF16),
            shaped((CELLS, CH), BF16),
            shaped((ROWS, SEQ, FEATURES), BF16),
            shaped((2 * HIDDEN, FEATURES), F32),
            shaped((HIDDEN * HIDDEN, CH), F32),
            shaped((CH, 5 * CH), F32),
            shaped((CH, CH), F32),
            shaped((CH, 5 * CH), F32),
            shaped((CH, CH), F32),
        ),
        in_specs=vmem(5),
        out_specs=tuple(vmem(9)),
        scratch_shapes=[
            pltpu.VMEM((2560, 128), F32),
        ],
        compiler_params=pltpu.CompilerParams(vmem_limit_bytes=VMEM_LIMIT),
        name="finish",
    )(*results)
    return (
        outs[0].reshape(ROWS, RES, CH),
        outs[1].reshape(ROWS, RES, CH),
        outs[2].transpose(1, 0, 2),
        outs[3].T,
        *outs[4:],
    )


def solution(mesh):
    placed = (
        P(("dp", "dap"), None, None),
        P("dp", "dap", None),
        P(),
        P(),
        P(),
        P(),
        P(),
        P(),
        P(("dp", "dap"), None, None),
    )
    return jax.shard_map(
        shards,
        mesh=mesh,
        in_specs=placed,
        out_specs=(
            P(("dp", "dap"), None, None),
            P(("dp", "dap"), None, None),
            P("dp", "dap", None),
            P("dp", None),
            P("dp", None),
            P("dp", None),
            P("dp", None),
            P("dp", None),
            P("dp", None),
        ),
        check_vma=False,
    )
```

```python
from types import SimpleNamespace

import jax
import jax.numpy as jnp
from jax import lax
from jax.experimental import pallas as pl
from jax.experimental.pallas import tpu as pltpu
from jax.sharding import PartitionSpec as P

EPSILON = 1e-05
F32, BF16 = jnp.float32, jnp.bfloat16
MESH = pl.DeviceIdType.MESH
N = 64
ROWS = 6
RES = 384
CELLS = ROWS * RES
CH = 128
GROUPS = CELLS // 128
PITCH = 72
HIDDEN = 32
PAIRS = HIDDEN // 2
SEQ = 64
FEATURES = 256
TILE = 256
TILES = CELLS // TILE
VMEM_LIMIT = 60 * 1024 * 1024


def nn(a, b):
    return lax.dot_general(a, b, (((1,), (0,)), ((), ())), preferred_element_type=F32)


def nt(a, b):
    return lax.dot_general(a, b, (((1,), (1,)), ((), ())), preferred_element_type=F32)


def one_hot(rows, columns, pick, dtype=BF16):
    row = lax.broadcasted_iota(jnp.int32, (rows, columns), 0)
    column = lax.broadcasted_iota(jnp.int32, (rows, columns), 1)
    return jnp.where(pick(row) == column, 1.0, 0.0).astype(dtype)


def identity(size):
    return one_hot(size, size, lambda r: r)


def hidden_order(dtype=BF16):
    return one_hot(CH, CH, lambda r: jnp.where(r < N, 2 * r, 2 * r - (CH - 1)), dtype)


def sigmoid(v):
    return 1.0 / (1.0 + jnp.exp(-v))


def ln0(v):
    centred = v - jnp.mean(v, axis=0, keepdims=True)
    factor = lax.rsqrt(jnp.mean(centred * centred, axis=0, keepdims=True) + EPSILON)
    return centred * factor, factor


def ln0_adjoint(hatted, factor, g):
    return factor * (
        g
        - jnp.mean(g, axis=0, keepdims=True)
        - hatted * jnp.mean(g * hatted, axis=0, keepdims=True)
    )


def loop(count, body, start=0):
    def step(k, carry):
        body(k)
        return carry

    lax.fori_loop(start, count, step, 0)


def me_index():
    return lax.axis_index("dap")


def greet():
    me = me_index()
    sem = pltpu.get_barrier_semaphore()
    tiles(
        lambda k: pl.semaphore_signal(
            sem, inc=1, device_id={"dap": lax.rem(me + k, N)}, device_id_type=MESH
        ),
        N,
        1,
    )


def all_here():
    pl.semaphore_wait(pltpu.get_barrier_semaphore(), N - 1)


def remote(src, dst, send_sem, recv_sem, to):
    return pltpu.make_async_remote_copy(
        src_ref=src,
        dst_ref=dst,
        send_sem=send_sem,
        recv_sem=recv_sem,
        device_id={"dap": to},
        device_id_type=MESH,
    )


BATCH = 3
CHIPS = N // 2
CHIP_STRIDE = 13
STRIDE = 37


def ahead(k):
    return lax.rem(me_index() + k * STRIDE, N)


def tiles(body, stop=TILES, start=0, by=3):
    def step(b):
        for k in range(by):
            body(start + by * b + k)

    loop((stop - start) // by, step)
    for t in range(start + (stop - start) // by * by, stop):
        body(t)


class Exchange:
    def __init__(self, out, into, sent, got, lo, hi):
        self.out, self.into, self.sent, self.got = out, into, sent, got
        self.folded = len(out.shape) == 4
        self.rows = pl.ds(lo // 4, (hi - lo) // 4) if self.folded else pl.ds(lo, hi - lo)

    def fold(self, value):
        return value.reshape(-1, 4, 128) if self.folded else value

    def copy(self, d, at):
        return remote(
            self.out.at[d, self.rows], self.into.at[at, self.rows], self.sent, self.got, d
        )

    def pack_and_send(self, rows_of):
        me = me_index()
        self.into[me, self.rows] = self.fold(rows_of(me))

        def pack(first):
            for k in range(BATCH):
                d = ahead(first + k)
                self.out[d, self.rows] = self.fold(rows_of(d))

        def send(first):
            for k in range(BATCH):
                self.copy(ahead(first + k), me).start()

        pack(1)

        def step(b):
            pack(1 + BATCH * b)
            send(1 + BATCH * (b - 1))

        loop((N - 1) // BATCH, step, 1)
        send(N - BATCH)

    def send_all(self):
        me = me_index()
        self.into[me, self.rows] = self.out[me, self.rows]
        tiles(lambda k: self.copy(ahead(k), me).start(), N, 1)

    def all_others(self):
        others = pl.ds(0, N - 1)
        return remote(
            self.out.at[others, self.rows], self.into.at[others, self.rows],
            self.sent, self.got, ahead(1),
        )

    def receive(self, use):
        self.all_others().wait_recv()
        tiles(use, N, 0, 4)

    def close(self):
        self.all_others().wait_send()


class Gather:
    def __init__(self, own, into, sent, got, passed, heard):
        self.own, self.into = own, into
        self.sent, self.got, self.passed, self.heard = sent, got, passed, heard
        me = me_index()
        self.core, self.chip = lax.rem(me, 2), me // 2
        self.partner = me + 1 - 2 * self.core

    def across(self, k):
        j = lax.rem(self.chip + k * CHIP_STRIDE, CHIPS)
        return remote(
            self.own, self.into.at[self.core, self.chip], self.sent, self.got, 2 * j + self.core
        )

    def all_across(self):
        blocks = self.into.at[self.core, pl.ds(0, CHIPS - 1)]
        return remote(blocks, blocks, self.sent, self.got, self.partner)

    def handed(self, core):
        half = self.into.at[core]
        return remote(half, half, self.passed, self.heard, self.partner)

    def start(self):
        self.into[self.core, self.chip] = self.own[...]
        tiles(lambda k: self.across(k).start(), CHIPS, 1)

    def hand_on(self):
        self.all_across().wait_recv()
        self.handed(self.core).start()

    def finish(self):
        self.handed(1 - self.core).wait_recv()

    def close(self):
        self.all_across().wait_send()
        self.handed(self.core).wait_send()


def ln1(v):
    centred = v - jnp.mean(v, axis=1, keepdims=True)
    factor = lax.rsqrt(jnp.mean(centred * centred, axis=1, keepdims=True) + EPSILON)
    return centred * factor, factor


def strided(ref, start, size, stride):
    return ref[pl.ds(start, size, stride=stride), :]


def packed(flat, lo, hi):
    return lambda d: strided(flat, lo * PITCH + d, hi - lo, PITCH).astype(BF16)


def widen_into(wide, into, lo, hi, pitch):
    def use(s):
        at = pl.multiple_of(s * pitch + lo, 8)
        if len(into.shape) == 4:
            rows = into[s, pl.ds(lo // 4, (hi - lo) // 4)].astype(F32).reshape(hi - lo, 128)
        else:
            rows = into[s, pl.ds(lo, hi - lo)].astype(F32)
        wide[pl.ds(at, hi - lo), :] = rows

    return use


def lanes_of(t):
    return pl.ds(pl.multiple_of(t * TILE, TILE), TILE)


def row_lanes(r):
    return slice(r * RES, (r + 1) * RES)


def pair_lanes(p):
    return pl.ds(pl.multiple_of(p * 128, 128), 128)


def scatter_hidden(flat, value, piece, t):
    for q in range(TILE // 128):
        at = pl.multiple_of((piece * GROUPS + t * (TILE // 128) + q) * PITCH, 8)
        flat[pl.ds(at, N), :] = value[:, q * 128 : (q + 1) * 128]


def gather_hidden(wide, pitch, bases, t):
    parts = []
    for base in bases:
        row = [
            strided(wide, base + t * (TILE // 128) + q, N, pitch) for q in range(TILE // 128)
        ]
        parts.append(jnp.concatenate(row, axis=1))
    return jnp.concatenate(parts, axis=0)


def scatter_rows(flat, value, piece):
    for r in range(ROWS):
        for jg in range(3):
            at = (piece * GROUPS + r * 3 + jg) * PITCH
            flat[at : at + N, :] = value[r * N : (r + 1) * N, jg * 128 : (jg + 1) * 128]


def gather_matrix(out, wide, pitch, base):
    for r in range(ROWS):
        for jg in range(3):
            out[r * N : (r + 1) * N, jg * 128 : (jg + 1) * 128] = strided(
                wide, base + r * 3 + jg, N, pitch
            ).astype(BF16)


def prepare(w, p_ref, f_ref):
    order = hidden_order()
    for b in range(4):
        block = p_ref[:, b * CH : (b + 1) * CH]
        turned = nt(order, block).astype(BF16)
        for m in range(2):
            w.turned[m, b * N : (b + 1) * N, :] = turned[m * N : (m + 1) * N]
        w.straight[:, b * CH : (b + 1) * CH] = nt(block, order).astype(BF16)
    w.gate[...] = nt(identity(CH), p_ref[:, 4 * CH :]).astype(BF16)
    w.straight[:, 4 * CH :] = p_ref[:, 4 * CH :]
    w.final[...] = nn(order, f_ref[...]).astype(BF16)
    w.final_turned[...] = nt(identity(CH), w.final[...]).astype(BF16)


class Update:
    def __init__(self, c, u, w, outgoing, sums_at):
        self.c, self.u, self.w, self.outgoing, self.sums_at = c, u, w, outgoing, sums_at
        plan = (
            ("ops_a", c.out_two, u.in_ops, 0, 40),
            ("ops_b", c.out_two, u.in_ops, 40, 72),
            ("tri_a", c.out_one, u.in_tri, 0, 16),
            ("tri_b", c.out_one, u.in_tri, 16, 36),
            ("grad_a", c.out_one, u.in_grad, 0, 24),
            ("grad_b", c.out_one, u.in_grad, 24, 36),
            ("back_a", c.out_two, u.in_back, 0, 32),
            ("back_b", c.out_two, u.in_back, 32, 72),
        )
        for i, (name, out, into, lo, hi) in enumerate(plan):
            setattr(self, name, Exchange(out, into, u.sent[i], u.got[i], lo, hi))

    def gated(self, m, t, norm=None):
        norm = self.u.norm[:, lanes_of(t)] if norm is None else norm
        pre = nn(self.w.turned[m], norm)
        flat = self.c.flat
        scatter_hidden(flat, sigmoid(pre[:N]) * pre[N : 2 * N], 2 * m, t)
        scatter_hidden(flat, sigmoid(pre[2 * N : 3 * N]) * pre[3 * N :], 2 * m + 1, t)

    def enter(self, t, x):
        norm = ln0(x)[0].astype(BF16)
        self.u.norm[:, lanes_of(t)] = norm
        self.gated(0, t, norm)

    def gates(self, t):
        at = lanes_of(t)
        self.u.gate[:, at] = sigmoid(nn(self.w.gate[...], self.u.norm[:, at]))

    def arrived(self, t):
        tri = gather_hidden(self.c.wide, 40, (0, GROUPS), t)
        hatted, factor = ln0(tri)
        unit = hatted.astype(BF16)
        return tri, hatted, factor, unit, nn(self.w.final_turned[...], unit)

    def descend(self, t, gz, hatted, factor, unit, values):
        c, at = self.c, lanes_of(t)
        gate = self.u.gate[:, at]
        scaled_wide = gz * gate
        scaled = scaled_wide.astype(BF16)
        c.unit[:, at] = unit
        c.scaled[:, at] = scaled
        c.grad_proj[4 * CH :, at] = (scaled_wide * values * (1.0 - gate)).astype(BF16)
        grad = ln0_adjoint(hatted, factor, nn(self.w.final[...], scaled))
        for m in range(2):
            scatter_hidden(c.flat_one, grad[m * N : (m + 1) * N], m, t)

    def coefficients(self, t):
        c, at = self.c, lanes_of(t)
        norm = self.u.norm[:, at]
        for m in range(2):
            pre = nn(self.w.turned[m], norm)
            for side in range(2):
                opened = sigmoid(pre[2 * side * N : (2 * side + 1) * N])
                slope = pre[(2 * side + 1) * N : (2 * side + 2) * N] * opened * (1.0 - opened)
                rows = 2 * side * CH + m * N
                c.coef[rows : rows + N, at] = slope
                c.coef[rows + CH : rows + CH + N, at] = opened

    def returned(self, t, x, gz):
        c, at = self.c, lanes_of(t)
        for side in range(2):
            base = 2 * side * CH
            grad = gather_hidden(c.wide, 72, (side * GROUPS, (2 + side) * GROUPS), t)
            for half in range(2):
                rows = pl.ds(base + half * CH, CH)
                c.grad_proj[rows, at] = (grad * c.coef[rows, at]).astype(BF16)
        grad_norm = nn(self.w.straight[...], c.grad_proj[:, at])
        hatted, factor = ln0(x)
        return gz + ln0_adjoint(hatted, factor, grad_norm)

    def keep_sum(self, block, value):
        at = self.sums_at + block * CH
        self.c.mine[at : at + CH, :] = value

    def early_sums(self):
        self.keep_sum(5, nt(self.c.unit[...], self.c.scaled[...]))
        self.keep_sum(4, nt(self.u.norm[...], self.c.grad_proj[4 * CH :, :]))

    def late_sums(self):
        for b in range(4):
            self.keep_sum(b, nt(self.u.norm[...], self.c.grad_proj[b * CH : (b + 1) * CH, :]))

    def forward(self, between):
        c, u = self.c, self.u
        tiles(lambda t: self.gated(1, t), 2, 0, 2)
        self.ops_a.pack_and_send(packed(c.flat, 0, 40))
        tiles(lambda t: self.gated(1, t), TILES, 2)
        self.ops_b.pack_and_send(packed(c.flat, 40, 72))
        between()
        tiles(self.gates)
        for m in range(2):
            if m == 0:
                self.ops_a.receive(widen_into(c.wide, u.in_ops, 0, 40, 72))
            else:
                self.ops_b.receive(widen_into(c.wide, u.in_ops, 40, 72, 72))
            for op in range(2):
                gather_matrix(u.kept.at[2 * op + m], c.wide, 72, (2 * m + op) * GROUPS)
            left, right = u.kept[m], u.kept[2 + m]
            product = nt(left, right) if self.outgoing else nn(left.T, right)
            scatter_rows(c.flat_one, product, m)
            if m == 0:
                self.tri_a.pack_and_send(packed(c.flat_one, 0, 16))
            else:
                self.tri_b.pack_and_send(packed(c.flat_one, 16, 36))
        self.ops_a.close()
        self.ops_b.close()
        self.tri_a.receive(widen_into(c.wide, u.in_tri, 0, 16, 40))
        self.tri_b.receive(widen_into(c.wide, u.in_tri, 16, 36, 40))
        self.tri_a.close()
        self.tri_b.close()

    def backward(self, between):
        c, u = self.c, self.u
        self.grad_a.pack_and_send(packed(c.flat_one, 0, 24))
        self.grad_b.pack_and_send(packed(c.flat_one, 24, 36))
        between()
        tiles(self.coefficients)
        self.early_sums()
        for m in range(2):
            if m == 0:
                self.grad_a.receive(widen_into(c.wide, u.in_grad, 0, 24, 40))
            else:
                self.grad_b.receive(widen_into(c.wide, u.in_grad, 24, 36, 40))
            gather_matrix(c.grad_m, c.wide, 40, m * GROUPS)
            grad = c.grad_m[...]
            left, right = u.kept[m], u.kept[2 + m]
            if self.outgoing:
                grad_left, grad_right = nn(grad, right), nn(grad.T, left)
            else:
                grad_left, grad_right = nt(right, grad), nn(left, grad)
            scatter_rows(c.flat, grad_left, 2 * m)
            scatter_rows(c.flat, grad_right, 2 * m + 1)
            if m == 0:
                self.back_a.pack_and_send(packed(c.flat, 0, 32))
            else:
                self.back_b.pack_and_send(packed(c.flat, 32, 72))
        self.grad_a.close()
        self.grad_b.close()
        self.back_a.receive(widen_into(c.wide, u.in_back, 0, 32, 72))
        self.back_b.receive(widen_into(c.wide, u.in_back, 32, 72, 72))
        self.back_a.close()
        self.back_b.close()


class Total:
    def __init__(self, mine, theirs, blocks, landed, own, full, sems_of):
        self.mine, self.theirs, self.blocks, self.landed = mine, theirs, blocks, landed
        self.own, self.half = own, theirs.shape[0]
        self.share = self.half // (N // 2)
        self.sent0, self.got0, self.sent1, self.got1, *rest = sems_of
        self.gather = Gather(own, full, *rest)

    def swap(self):
        core = lax.rem(me_index(), 2)
        other = pl.ds(pl.multiple_of((1 - core) * self.half, 8), self.half)
        return remote(
            self.mine.at[other], self.theirs, self.sent0, self.got0, self.gather.partner
        )

    def to(self, k):
        g = self.gather
        j = lax.rem(g.chip + k * CHIP_STRIDE, CHIPS)
        return remote(
            self.blocks.at[j], self.landed.at[g.chip], self.sent1, self.got1, 2 * j + g.core
        )

    def all_others(self):
        others = pl.ds(0, CHIPS - 1)
        return remote(
            self.blocks.at[others], self.landed.at[others], self.sent1, self.got1,
            self.gather.partner,
        )

    def scatter(self):
        g = self.gather
        self.swap().wait_recv()
        mine = self.mine[pl.ds(pl.multiple_of(g.core * self.half, 8), self.half), :]
        for j in range(CHIPS):
            at = slice(j * self.share, (j + 1) * self.share)
            self.blocks[j] = (mine[at] + self.theirs[at, :]).astype(self.blocks.dtype)
        loop(CHIPS, lambda k: self.to(k).start(), 1)
        self.landed[g.chip] = self.blocks[g.chip]

    def spread(self):
        self.all_others().wait_recv()
        total = self.landed[0].astype(F32)
        for j in range(1, CHIPS):
            total = total + self.landed[j].astype(F32)
        self.own[...] = (total * (1.0 / RES)).astype(self.own.dtype)
        self.gather.start()

    def close(self):
        self.swap().wait_send()
        self.all_others().wait_send()
        self.gather.close()


def spread_out(all_ref, wide, into, rows, placed):
    pitch = rows if rows // 8 % 2 else rows + 8

    def widen(s):
        at = pl.ds(pl.multiple_of(s * pitch, 8), rows)
        wide[at, :] = into[lax.rem(s, 2), s // 2].astype(F32)

    tiles(widen, N, 0, 4)
    for r, p, row in placed:
        all_ref[r * N : (r + 1) * N, p * 128 : (p + 1) * 128] = strided(
            wide, row, N, pitch
        ).astype(BF16)


def cells_of(c, ref, out):
    for r in range(ROWS):
        c.cells_wide[:RES, :] = ref[row_lanes(r), :].astype(F32)
        parts = [strided(c.cells_wide, q, N, ROWS) for q in range(ROWS)]
        out[:, row_lanes(r)] = jnp.concatenate(parts, 0).T.astype(BF16)


def natural(c, cells, out):
    for r in range(ROWS):
        turned = cells[:, row_lanes(r)].astype(F32).T
        for q in range(ROWS):
            c.cells_wide[pl.ds(q, N, stride=ROWS), :] = turned[q * N : (q + 1) * N]
        out[row_lanes(r), :] = c.cells_wide[...].astype(BF16)


def outer_grads(c, block, r):
    for p in range(PAIRS):
        c.outer_grad[p, r * 64 : (r + 1) * 64, :] = block[p * 64 : (p + 1) * 64].astype(BF16)


def outer_sums(c, all_ref, acc):
    acc[...] = jnp.zeros_like(acc)

    def add(b):
        part = None
        for k in range(4):
            here = nn(c.outer_grad[4 * b + k], all_ref[:, pair_lanes(4 * b + k)])
            part = here if part is None else part + here
        acc[...] += part

    loop(PAIRS // 4, add)


def matched(acc, r):
    return acc[r * 64 : r * 64 + 32, :] + pltpu.roll(acc[r * 64 + 32 : (r + 1) * 64, :], 64, 1)


def whole_kernel(names, *refs):
    c = SimpleNamespace(**dict(zip(names, refs)))
    greet()
    loads = []
    for name in LATE:
        held = getattr(c, "held_" + name)
        loads.append(pltpu.make_async_copy(getattr(c, name), held, getattr(c, "load_" + name)))
        loads[-1].start()
        setattr(c, name, held)
    phases = []
    for kind in ("out", "in"):
        part = lambda name: getattr(c, name + "_" + kind)
        phases.append(
            SimpleNamespace(
                norm=part("norm"), gate=part("gate"), tri=part("tri"), kept=part("kept"),
                in_ops=part("in_ops"), in_tri=part("in_tri"),
                in_grad=part("in_grad"), in_back=part("in_back"),
                sent=[part("sent%d" % i) for i in range(8)],
                got=[part("got%d" % i) for i in range(8)],
                weights=SimpleNamespace(
                    turned=part("turned"), straight=part("straight"), gate=part("w_gate"),
                    final=part("final"), final_turned=part("final_turned"),
                ),
            )
        )
    out, into = phases

    flank_turned = c.flank[...]
    split = lambda first: one_hot(
        HIDDEN, 2 * HIDDEN, lambda r: first + jnp.where(r < PAIRS, 2 * r, 2 * r - (HIDDEN - 1))
    )
    split_left = nn(split(0), flank_turned).astype(BF16)
    split_right = nn(split(HIDDEN), flank_turned).astype(BF16)
    plain_left = flank_turned[:HIDDEN]
    none = jnp.zeros((SEQ, FEATURES), BF16)
    for r in range(ROWS):
        hatted, _ = ln1(c.alignment[r].astype(F32))
        norm = hatted.astype(BF16)
        halves = (jnp.concatenate([norm, none], 0), jnp.concatenate([none, norm], 0))
        made = [
            (nt(weights[:PAIRS], halves[0]) + nt(weights[PAIRS:], halves[1])).astype(BF16)
            for weights in (split_right, split_left)
        ]
        for h in range(2):
            c.own_right[h, r * 8 : (r + 1) * 8, :] = made[0][h * 8 : (h + 1) * 8]
        c.own_left[r // 2, (r % 2) * PAIRS : (r % 2 + 1) * PAIRS, :] = made[1]
        for h in range(2):
            at = (2 * r + h) * HIDDEN
            c.own_outer[at : at + HIDDEN, :] = nt(plain_left, halves[h]).astype(BF16)
    all_here()
    gather = lambda own, into, tail: Gather(
        own, into, *(getattr(c, name + tail) for name in ("sent_", "got_", "pass_", "heard_"))
    )
    right = [gather(c.own_right.at[h], c.in_right.at[h], "r%d" % h) for h in range(2)]
    left = [gather(c.own_left.at[h], c.in_left.at[h], "l%d" % h) for h in range(3)]
    right[0].start()
    right[1].start()
    for copy in loads:
        copy.wait()
    cells_of(c, c.edge, c.x_one)
    cells_of(c, c.seed, c.seed_cells)
    prepare(out.weights, c.p_out, c.f_out)
    prepare(into.weights, c.p_in, c.f_in)
    c.fin_wide[...] = c.fin[...].astype(F32)
    for d in range(HIDDEN):
        c.fin_split[d * HIDDEN : (d + 1) * HIDDEN, :] = strided(
            c.fin_wide, d, HIDDEN, HIDDEN
        ).astype(BF16)
    c.fin_turned[...] = nt(identity(CH), c.fin_split[...]).astype(BF16)
    def outer_pair(p):
        block = nt(c.own_outer[...], c.right_all[:, pair_lanes(p)]) * (1.0 / SEQ)
        for r in range(ROWS):
            c.outer[r, pl.ds(pl.multiple_of(p * 64, 64), 64), :] = block[
                r * 64 : (r + 1) * 64
            ].astype(BF16)

    for h in range(2):
        right[h].hand_on()
        right[h].finish()
        if h == 1:
            left[0].start()
        spread_out(
            c.right_all, c.wide, c.in_right.at[h], 48,
            [(r, 8 * h + p, r * 8 + p) for r in range(ROWS) for p in range(8)],
        )
        tiles(outer_pair, 8 * h + 8, 8 * h, 4)
    for r in range(ROWS):
        at = row_lanes(r)
        c.x_one[:, at] = (c.x_one[:, at].astype(F32) + nn(c.fin_turned[...], c.outer[r])).astype(
            BF16
        )
    right[0].close()
    right[1].close()

    one = Update(c, out, out.weights, True, 1024)
    two = Update(c, into, into.weights, False, 1792)
    tiles(lambda t: one.enter(t, c.x_one[:, lanes_of(t)].astype(F32)))
    one.forward(left[0].hand_on)
    left[1].start()

    def between_updates(t):
        at = lanes_of(t)
        tri, _, _, _, values = one.arrived(t)
        out.tri[:, at] = tri.astype(BF16)
        new = (c.x_one[:, at].astype(F32) + out.gate[:, at] * values).astype(BF16)
        c.x_two[:, at] = new
        two.enter(t, new.astype(F32))

    tiles(between_updates)
    two.forward(left[1].hand_on)
    left[2].start()

    def turn_round(t):
        at = lanes_of(t)
        _, hatted, factor, unit, values = two.arrived(t)
        c.new_cells[:, at] = (
            c.x_two[:, at].astype(F32) + into.gate[:, at] * values
        ).astype(BF16)
        two.descend(t, c.seed_cells[:, at].astype(F32), hatted, factor, unit, values)

    def after_turn():
        left[2].hand_on()
        natural(c, c.new_cells, c.new_pair)

        def ahead_of_back(t):
            at = lanes_of(t)
            unit = ln0(out.tri[:, at].astype(F32))[0].astype(BF16)
            c.values[:, at] = nn(out.weights.final_turned[...], unit)

        tiles(ahead_of_back)

    tiles(turn_round)
    two.backward(after_turn)

    def between_backs(t):
        at = lanes_of(t)
        c.grad_two[:, at] = two.returned(
            t, c.x_two[:, at].astype(F32), c.seed_cells[:, at].astype(F32)
        )

    def below(t):
        at = lanes_of(t)
        hatted, factor = ln0(out.tri[:, at].astype(F32))
        one.descend(
            t, c.grad_two[:, at], hatted, factor, hatted.astype(BF16), c.values[:, at]
        )

    tiles(between_backs)
    tiles(below)

    def meanwhile():
        two.late_sums()
        for h in range(3):
            left[h].finish()
            left[h].close()
            spread_out(
                c.left_all, c.wide, c.in_left.at[h], 32,
                [(2 * h + r, p, r * PAIRS + p) for r in range(2) for p in range(PAIRS)],
            )

    one.backward(meanwhile)

    def last(t):
        at = lanes_of(t)
        c.adjoint[:, at] = one.returned(
            t, c.x_one[:, at].astype(F32), c.grad_two[:, at]
        ).astype(BF16)

    tiles(last)

    for r in range(ROWS):
        turned = c.adjoint[:, row_lanes(r)].astype(F32).T
        for q in range(ROWS):
            at = (q * ROWS + r) * PITCH
            c.flat_one[at : at + N, :] = turned[q * N : (q + 1) * N]
    pair_a = Exchange(c.out_one, c.in_pair, c.sent_pa, c.got_pa, 0, 24)
    pair_b = Exchange(c.out_one, c.in_pair, c.sent_pb, c.got_pb, 24, 36)
    pair_a.pack_and_send(packed(c.flat_one, 0, 24))
    pair_b.pack_and_send(packed(c.flat_one, 24, 36))
    one.late_sums()
    total = None
    for r in range(ROWS):
        part = nt(c.outer[r], c.adjoint[:, row_lanes(r)])
        total = part if total is None else total + part
    c.fin_wide[...] = total
    for k in range(HIDDEN):
        c.mine[k * HIDDEN : (k + 1) * HIDDEN, :] = strided(c.fin_wide, k, HIDDEN, HIDDEN)
    large = Total(
        c.mine, c.theirs, c.blocks, c.landed, c.own_sum, c.full,
        (c.swap_a0, c.swap_a1, c.sent_a, c.got_a, c.sent_ag, c.got_ag, c.pass_ag, c.heard_ag),
    )
    small = Exchange(c.flank_blocks, c.flank_landed, c.sent_b, c.got_b, 0, 2)
    large.swap().start()
    large.scatter()
    for r in range(ROWS):
        outer_grads(c, nn(c.fin_split[...], c.adjoint[:, row_lanes(r)]), r)
    outer_sums(c, c.right_all, c.acc_left)
    for part, lo, hi in ((pair_a, 0, 4), (pair_b, 4, ROWS)):
        part.receive(widen_into(c.wide, c.in_pair, 6 * lo, 24 if lo == 0 else 36, 40))
        for q in range(lo, hi):
            for r in range(ROWS):
                c.columns[q, r * N : (r + 1) * N, :] = strided(
                    c.wide, q * ROWS + r, N, 40
                ).astype(BF16)
            outer_grads(c, nt(c.fin[...], c.columns[q]), q)
    outer_sums(c, c.left_all, c.acc_right)
    lane = lax.broadcasted_iota(jnp.int32, (2 * HIDDEN, 2 * SEQ), 1)
    flank_sum = jnp.zeros((2 * HIDDEN, FEATURES), F32)
    grads = []
    for r in range(ROWS):
        both = jnp.concatenate([matched(c.acc_left, r), matched(c.acc_right, r)], 0)
        both = jnp.where(lane < SEQ, both * (1.0 / SEQ), 0.0)
        c.flank_grad[r] = both
        hatted, _ = ln1(c.alignment[r].astype(F32))
        norm = jnp.concatenate([hatted.astype(BF16), none], 0)
        flank_sum = flank_sum + nn(both.astype(BF16), norm)
    for half in range(2):
        for d in range(N // 2):
            c.flank_blocks[half * (N // 2) + d] = flank_sum[
                2 * d : 2 * d + 2, half * 128 : (half + 1) * 128
            ]
    small.send_all()
    large.spread()
    for r in range(ROWS):
        grad = nn(c.flank_grad[r].T[:SEQ].astype(BF16), flank_turned)
        hatted, factor = ln1(c.alignment[r].astype(F32))
        c.align_grad[r] = (
            factor
            * (
                grad
                - jnp.mean(grad, axis=1, keepdims=True)
                - hatted * jnp.mean(grad * hatted, axis=1, keepdims=True)
            )
        ).astype(BF16)
    small.all_others().wait_recv()
    total = c.flank_landed[0]
    for d in range(1, N):
        total = total + c.flank_landed[d]
    c.flank_own[...] = total * (1.0 / RES)
    me = me_index()
    c.flank_full[me] = c.flank_own[...]

    def to_all(k):
        d = ahead(k)
        return remote(c.flank_own, c.flank_full.at[me], c.sent_bg, c.got_bg, d)

    tiles(lambda k: to_all(k).start(), N, 1)
    large.gather.hand_on()
    natural(c, c.adjoint, c.adjoint_pair)
    others = c.flank_full.at[pl.ds(0, N - 1)]
    summed = remote(others, others, c.sent_bg, c.got_bg, ahead(1))
    large.gather.finish()
    summed.wait_recv()
    pair_a.close()
    pair_b.close()
    small.close()
    summed.wait_send()
    large.close()


def vmem(count):
    return [pl.BlockSpec(memory_space=pltpu.VMEM)] * count


def shaped(shape, dtype):
    return jax.ShapeDtypeStruct(shape, dtype)


INPUTS = ("edge", "alignment", "flank", "fin", "p_out", "f_out", "p_in", "f_in", "seed")
LATE = dict(
    edge=(CELLS, CH),
    seed=(CELLS, CH),
    fin=(HIDDEN * HIDDEN, CH),
    p_out=(CH, 5 * CH),
    f_out=(CH, CH),
    p_in=(CH, 5 * CH),
    f_in=(CH, CH),
)
OUTPUTS = dict(
    new_pair=((CELLS, CH), BF16),
    adjoint_pair=((CELLS, CH), BF16),
    align_grad=((ROWS, SEQ, FEATURES), BF16),
    full=((2, CHIPS, 40, 128), BF16),
    flank_full=((N, 2, 128), F32),
)


def scratch():
    shapes = dict(
        x_one=((CH, CELLS), BF16),
        x_two=((CH, CELLS), BF16),
        new_cells=((CH, CELLS), BF16),
        adjoint=((CH, CELLS), BF16),
        seed_cells=((CH, CELLS), BF16),
        grad_two=((CH, CELLS), F32),
        values=((CH, CELLS), F32),
        flat=((72 * PITCH, 128), F32),
        flat_one=((36 * PITCH, 128), F32),
        wide=((104 * N, 128), F32),
        out_two=((N, 72, 128), BF16),
        out_one=((N, 9, 4, 128), BF16),
        unit=((CH, CELLS), BF16),
        scaled=((CH, CELLS), BF16),
        coef=((4 * CH, CELLS), F32),
        grad_proj=((5 * CH, CELLS), BF16),
        grad_m=((RES, RES), BF16),
        mine=((2560, 128), F32),
        theirs=((1280, 128), F32),
        blocks=((CHIPS, 40, 128), BF16),
        landed=((CHIPS, 40, 128), BF16),
        own_sum=((40, 128), BF16),
        flank_blocks=((N, 2, 128), F32),
        flank_landed=((N, 2, 128), F32),
        flank_own=((2, 128), F32),
        flank_grad=((ROWS, 2 * HIDDEN, 128), F32),
        own_right=((2, 48, 128), BF16),
        own_left=((3, 32, 128), BF16),
        own_outer=((2 * ROWS * HIDDEN, 2 * SEQ), BF16),
        in_right=((2, 2, CHIPS, 48, 128), BF16),
        in_left=((3, 2, CHIPS, 32, 128), BF16),
        right_all=((RES, HIDDEN * SEQ), BF16),
        left_all=((RES, HIDDEN * SEQ), BF16),
        cells_wide=((RES, 128), F32),
        fin_wide=((HIDDEN * HIDDEN, CH), F32),
        fin_split=((HIDDEN * HIDDEN, CH), BF16),
        fin_turned=((CH, HIDDEN * HIDDEN), BF16),
        outer=((ROWS, HIDDEN * HIDDEN, RES), BF16),
        outer_grad=((PAIRS, RES, RES), BF16),
        acc_left=((RES, 128), F32),
        acc_right=((RES, 128), F32),
        columns=((ROWS, RES, CH), BF16),
        in_pair=((N, 9, 4, 128), BF16),
    )
    each = dict(
        norm=((CH, CELLS), BF16),
        gate=((CH, CELLS), F32),
        tri=((CH, CELLS), BF16),
        kept=((4, RES, RES), BF16),
        in_ops=((N, 72, 128), BF16),
        in_tri=((N, 9, 4, 128), BF16),
        in_grad=((N, 9, 4, 128), BF16),
        in_back=((N, 72, 128), BF16),
        turned=((2, 4 * N, CH), BF16),
        straight=((CH, 5 * CH), BF16),
        w_gate=((CH, CH), BF16),
        final=((CH, CH), BF16),
        final_turned=((CH, CH), BF16),
    )
    for kind in ("out", "in"):
        shapes.update({name + "_" + kind: value for name, value in each.items()})
    made = {name: pltpu.VMEM(*value) for name, value in shapes.items()}
    made.update({"held_" + name: pltpu.VMEM(shape, BF16) for name, shape in LATE.items()})
    flags = ["load_" + name for name in LATE]
    for kind in ("out", "in"):
        for i in range(8):
            flags += ["sent%d_%s" % (i, kind), "got%d_%s" % (i, kind)]
    for tail in ("r0", "r1", "l0", "l1", "l2", "ag"):
        flags += [name + tail for name in ("sent_", "got_", "pass_", "heard_")]
    for tail in ("pa", "pb", "a", "b", "bg"):
        flags += ["sent_" + tail, "got_" + tail]
    flags += ["swap_a0", "swap_a1"]
    made.update({name: pltpu.SemaphoreType.DMA(()) for name in flags})
    return made


def whole(*arrays):
    made = scratch()
    names = INPUTS + tuple(OUTPUTS) + tuple(made)
    return pl.pallas_call(
        lambda *refs: whole_kernel(names, *refs),
        out_shape=tuple(shaped(*value) for value in OUTPUTS.values()),
        in_specs=[
            pl.BlockSpec(memory_space=pl.ANY if name in LATE else pltpu.VMEM) for name in INPUTS
        ],
        out_specs=tuple(vmem(len(OUTPUTS))),
        scratch_shapes=list(made.values()),
        compiler_params=pltpu.CompilerParams(
            collective_id=1, has_side_effects=True, vmem_limit_bytes=67_043_328
        ),
        name="window",
    )(*arrays)


def finish_kernel(
    new_ref, adj_ref, align_ref, full_ref, flank_ref,
    new_out, adj_out, align_out, flank_out, fin_out, proj_out, final_out, proj_in, final_in,
    sums, held, arrived, left,
):
    pairs = ((new_ref, new_out), (adj_ref, adj_out))
    taken = [
        pltpu.make_async_copy(ref, held.at[i], arrived.at[i]) for i, (ref, _) in enumerate(pairs)
    ]
    given = [
        pltpu.make_async_copy(held.at[i], out, left.at[i]) for i, (_, out) in enumerate(pairs)
    ]
    for copy in taken:
        copy.start()
    for came, goes in zip(taken, given):
        came.wait()
        goes.start()
    align_out[...] = align_ref[...]
    order = hidden_order()

    def place(s):
        at = pl.multiple_of(s * 40, 8)
        sums[pl.ds(at, 40), :] = full_ref[s // CHIPS, lax.rem(s, CHIPS)].astype(F32)

    tiles(place, N, 0, 4)
    fin_out[...] = sums[:1024, :]
    for base, proj, final in ((1024, proj_out, final_out), (1792, proj_in, final_in)):
        for b in range(5):
            block = sums[base + b * CH : base + (b + 1) * CH, :]
            proj[:, b * CH : (b + 1) * CH] = nn(block.astype(BF16), order) if b < 4 else block
        block = sums[base + 5 * CH : base + 6 * CH, :]
        final[...] = nn(order.T, block.astype(BF16))
    for half in range(2):
        for d in range(N // 2):
            flank_out[2 * d : 2 * d + 2, half * 128 : (half + 1) * 128] = flank_ref[
                half * (N // 2) + d
            ]
    for copy in given:
        copy.wait()


def shards(
    edge_embedding,
    alignment_embedding,
    tensor_flank_matrix,
    tensor_final_matrix,
    outward_sigmoid_matrix,
    outward_final_matrix,
    inward_sigmoid_matrix,
    inward_final_matrix,
    adjoint_seed,
):
    results = whole(
        edge_embedding.reshape(CELLS, CH),
        alignment_embedding.transpose(1, 0, 2),
        tensor_flank_matrix.T,
        tensor_final_matrix,
        outward_sigmoid_matrix,
        outward_final_matrix,
        inward_sigmoid_matrix,
        inward_final_matrix,
        adjoint_seed.reshape(CELLS, CH),
    )
    outs = pl.pallas_call(
        finish_kernel,
        out_shape=(
            shaped((CELLS, CH), BF16),
            shaped((CELLS, CH), BF16),
            shaped((ROWS, SEQ, FEATURES), BF16),
            shaped((2 * HIDDEN, FEATURES), F32),
            shaped((HIDDEN * HIDDEN, CH), F32),
            shaped((CH, 5 * CH), F32),
            shaped((CH, CH), F32),
            shaped((CH, 5 * CH), F32),
            shaped((CH, CH), F32),
        ),
        in_specs=[pl.BlockSpec(memory_space=pl.ANY)] * 2 + vmem(3),
        out_specs=tuple([pl.BlockSpec(memory_space=pl.ANY)] * 2 + vmem(7)),
        scratch_shapes=[
            pltpu.VMEM((2560, 128), F32),
            pltpu.VMEM((2, CELLS, CH), BF16),
            pltpu.SemaphoreType.DMA((2,)),
            pltpu.SemaphoreType.DMA((2,)),
        ],
        compiler_params=pltpu.CompilerParams(vmem_limit_bytes=VMEM_LIMIT),
        name="finish",
    )(*results)
    return (
        outs[0].reshape(ROWS, RES, CH),
        outs[1].reshape(ROWS, RES, CH),
        outs[2].transpose(1, 0, 2),
        outs[3].T,
        *outs[4:],
    )


def solution(mesh):
    placed = (
        P(("dp", "dap"), None, None),
        P("dp", "dap", None),
        P(),
        P(),
        P(),
        P(),
        P(),
        P(),
        P(("dp", "dap"), None, None),
    )
    return jax.shard_map(
        shards,
        mesh=mesh,
        in_specs=placed,
        out_specs=(
            P(("dp", "dap"), None, None),
            P(("dp", "dap"), None, None),
            P("dp", "dap", None),
            P("dp", None),
            P("dp", None),
            P("dp", None),
            P("dp", None),
            P("dp", None),
            P("dp", None),
        ),
        check_vma=False,
    )
```
